512 devices in a mesh: dp: 16 (over z, core), rows: 32 (over y, x).
Axes of the slice: x: 4, y: 8, z: 8, core: 2. Of those that a mesh axis runs over, the one named last changes fastest.
Arguments:
- latent: bfloat16 [32, 32, 64, 640], P('dp', 'rows'), may hold values from -16.25 to 16.25
- hidden: bfloat16 [32, 32, 64, 640], P('dp', 'rows'), may hold values from -16.25 to 16.25
- cotangent: bfloat16 [32, 32, 64, 640], P('dp', 'rows'), may hold values from -6 to 6
- filter_one: bfloat16 [9, 640, 640], P(None, 'dp', 'rows'), may hold values from -0.078125 to 0.078125
- filter_two: bfloat16 [9, 640, 640], P(None, 'dp', 'rows'), may hold values from -0.078125 to 0.078125
- gain_one: float32 [640], replicated, may hold values from 0.1 to 1.9
- shift_one: float32 [640], replicated, may hold values from -2.5 to 2.5
- gain_two: float32 [640], replicated, may hold values from 0.1 to 1.9
- shift_two: float32 [640], replicated, may hold values from -2.5 to 2.5
Outputs:
- latent_grad: bfloat16 [32, 32, 64, 640], P('dp', 'rows')
The draws below stay inside these ranges and needn't reach their ends.
All inputs are finite; a program needn't handle non-finite values.
Results may differ from the reference program's by a relative error of at most 0.0027.
Values may be sent and summed in bfloat16 or wider, within the bound.
A program may use at most 128 MiB of HBM per device.

```python
import jax
import jax.numpy as jnp
from jax import lax

GROUPS = 16
GSIZE = 40
WIDTH = 64
CH = 640
IMAGES = 32
HEIGHT = 32


def draw_field(key, salt):
    key = jax.random.fold_in(key, salt)
    key_noise, key_channel = jax.random.split(key, 2)
    height_pos = jnp.arange(HEIGHT, dtype=jnp.float32) / max(HEIGHT - 1, 1)
    row_scale = jnp.exp(jnp.log(3.0) * height_pos)[None, :, None, None]
    channel_scale = jnp.exp(jax.random.uniform(key_channel, (CH,), jnp.float32, jnp.log(0.1), 0.0))
    noise = jnp.clip(jax.random.normal(key_noise, (IMAGES, HEIGHT, WIDTH, CH), jnp.float32), -5.0, 5.0)
    field = noise * row_scale * channel_scale
    return field.astype(jnp.bfloat16)


def draw_latent(key, part):
    return draw_field(key, 11)


def draw_hidden(key, part):
    return draw_field(key, 23)


def draw_cotangent(key, part):
    key = jax.random.fold_in(key, 37)
    key_noise, key_offset = jax.random.split(key, 2)
    noise = jax.random.normal(key_noise, (IMAGES, HEIGHT, WIDTH, CH), jnp.float32)
    offset = jax.random.normal(key_offset, (IMAGES, 1, 1, CH), jnp.float32)
    field = jnp.clip(noise + offset, -6.0, 6.0)
    return field.astype(jnp.bfloat16)


def levels(key, dims, cuts, low, top_value):
    factor_of, own = 1.0, jax.random.fold_in(key, 6)
    for axis_at, blocks in cuts:
        draws = jnp.exp(jax.random.uniform(jax.random.fold_in(own, axis_at), (blocks,), jnp.float32, low / len(cuts), top_value / len(cuts)))
        factor_of = factor_of * jnp.repeat(draws, dims[axis_at] // blocks).reshape([-1 if axis == axis_at else 1 for axis in range(len(dims))])
    return factor_of


def centred(stream_key, extent, scale, most, cuts=(), held_as=jnp.bfloat16):
    level = levels(stream_key, extent, cuts, -0.22, 0.18) if cuts else 1.0
    values = jax.random.normal(stream_key, extent, jnp.float32) * scale * level
    return jnp.minimum(jnp.maximum(values, -most), most).astype(held_as)


def setup_inputs(seed: int = 0) -> dict:
    seeds = jax.random.split(jax.random.key(seed), 10)
    return {
        "latent": draw_latent(jax.random.fold_in(seeds[9], 71), 0),
        "hidden": draw_hidden(jax.random.fold_in(seeds[9], 71), 0),
        "cotangent": draw_cotangent(jax.random.fold_in(seeds[9], 71), 0),
        "filter_one": centred(seeds[3], (9, CH, CH), (9 * CH) ** -0.5, 0.078125, ((1, 16), (2, 32))),
        "filter_two": centred(seeds[4], (9, CH, CH), (9 * CH) ** -0.5, 0.078125, ((1, 16), (2, 32))),
        "gain_one": jnp.clip(1.0 + 0.18 * jax.random.normal(seeds[5], (CH,), jnp.float32), 0.1, 1.9),
        "shift_one": centred(seeds[6], (CH,), 0.5, 2.5, (), jnp.float32),
        "gain_two": jnp.clip(1.0 + 0.18 * jax.random.normal(seeds[7], (CH,), jnp.float32), 0.1, 1.9),
        "shift_two": centred(seeds[8], (CH,), 0.5, 2.5, (), jnp.float32),
    }


def group_sums(values):
    per_channel = lax.optimization_barrier(jnp.sum(values, axis=(1, 2)))
    return lax.optimization_barrier(jnp.sum(per_channel.reshape(per_channel.shape[0], GROUPS, -1), axis=2))

def expand_groups(moment):
    return jnp.repeat(moment, GSIZE, axis=1)[:, None, None, :]

def finish_stats(sum_plain, sum_square, number):
    average = sum_plain / number
    variance = sum_square / number - average * average
    return (average, lax.rsqrt(variance + 1e-05))

def norm_backward(field, stats, gain, shift, incoming, number):
    average, inverse = stats
    values = field.astype(jnp.float32)
    normed = (values - expand_groups(average)) * expand_groups(inverse)
    linear = normed * gain + shift
    logistic = jax.nn.sigmoid(linear)
    scaled = incoming * logistic * (1.0 + linear * (1.0 - logistic)) * gain
    first = group_sums(scaled) / number
    second = group_sums(scaled * normed) / number
    return expand_groups(inverse) * (scaled - expand_groups(first) - normed * expand_groups(second))

def conv_backward(gradient, weights):
    images, height, breadth, channels = gradient.shape
    padded = jnp.pad(gradient, ((0, 0), (1, 1), (1, 1), (0, 0)))
    result = jnp.zeros((images * height * breadth, channels), jnp.float32)
    for tap_index in range(9):
        down_step = tap_index // 3 - 1
        side_step = tap_index % 3 - 1
        window = padded[:, 1 - down_step:1 - down_step + height, 1 - side_step:1 - side_step + breadth, :]
        window = window.reshape(images * height * breadth, channels)
        result = result + jnp.dot(window, weights[tap_index].T, preferred_element_type=jnp.float32)
    return result.reshape(images, height, breadth, channels)

def reference(latent, hidden, cotangent, filter_one, filter_two, gain_one, shift_one, gain_two, shift_two):
    number = HEIGHT * WIDTH * GSIZE
    latent_values = latent.astype(jnp.float32)
    hidden_values = hidden.astype(jnp.float32)
    stats_one = finish_stats(group_sums(latent_values), group_sums(latent_values * latent_values), number)
    stats_two = finish_stats(group_sums(hidden_values), group_sums(hidden_values * hidden_values), number)
    back_two = conv_backward(cotangent, filter_two)
    hidden_grad = norm_backward(hidden, stats_two, gain_two, shift_two, back_two, number).astype(jnp.bfloat16)
    back_one = conv_backward(hidden_grad, filter_one)
    latent_part = norm_backward(latent, stats_one, gain_one, shift_one, back_one, number)
    return (cotangent.astype(jnp.float32) + latent_part).astype(jnp.bfloat16)
```

```python
import jax
import jax.numpy as jnp
from jax import lax
from jax.experimental import pallas as pl
from jax.experimental.pallas import tpu as pltpu
from jax.sharding import PartitionSpec as P

MESH = pl.DeviceIdType.MESH
F32 = jnp.float32
BF16 = jnp.bfloat16
NX, NY, NZ = 4, 8, 8
CH = 640
BLK = 160
PX = 128
NUMBER = 32 * 64 * 40


def dev(x, y, z, c):
    return (2 * z + c, 4 * y + x)


def iota(shape, dim):
    return lax.broadcasted_iota(jnp.int32, shape, dim)


def dot(a, b, **kw):
    return jnp.dot(a, b, preferred_element_type=F32, **kw)


def group_of(lane):
    g = jnp.zeros_like(lane)
    for edge in (40, 80, 120, 160):
        g = g + (lane >= edge).astype(jnp.int32)
    return g


def kernel(
    wb, cot, hid, lat, par, out,
    W, RA, G, Gh, Hs, Hc, SS, ST, HBs, HBr, AC, BK, Os, Oc, CC,
    sA, sA0, rA, lsem, sR, rR, sP, rP, sG, rG, sGh, rGh, sH, rH, sS, rS, sB, rB, sO, rO,
):
    dp = lax.axis_index("dp")
    rr = lax.axis_index("rows")
    c = lax.rem(dp, 2)
    z = lax.div(dp, 2)
    x = lax.rem(rr, NX)
    y = lax.div(rr, NX)

    def remote(src, dst, ss, rs, target):
        return pltpu.make_async_remote_copy(
            src_ref=src, dst_ref=dst, send_sem=ss, recv_sem=rs, device_id=target,
            device_id_type=MESH,
        )

    def local_wait(ref, sem):
        pltpu.make_async_copy(ref, ref, sem).wait()

    X = lax.div(z, 2)
    slot = lax.rem(z, 2) * 4 + x
    for f in (1, 0):
        for k in range(8):
            if f == 1:
                z_, y_ = lax.rem(z + k, NZ), y
                mine = x == X
            else:
                z_, y_ = y, lax.rem(y + k, NY)
                mine = jnp.logical_and(x == X, y == z)
            target = dev(X, y_, z_, c)
            if k == 0:
                @pl.when(mine)
                def _():
                    pltpu.make_async_copy(wb.at[f], RA.at[f, slot], rA.at[f]).start()

                @pl.when(jnp.logical_not(mine))
                def _():
                    remote(wb.at[f], RA.at[f, slot], sA0.at[f], rA.at[f], target).start()
            else:
                remote(wb.at[f], RA.at[f, slot], sA.at[f], rA.at[f], target).start()

    for k in range(1, NX):
        t = lax.rem(x + k, NX)
        remote(cot, G.at[x], sG, rG, dev(t, y, z, c)).start()
    own_cot = pltpu.make_async_copy(cot, G.at[x], lsem)
    own_cot.start()

    for a, ref in enumerate((hid, lat)):
        v = ref[...].astype(F32)
        for k in range(NX):
            blk = v[:, BLK * k : BLK * k + BLK]
            blk = jnp.concatenate([blk, jnp.zeros((PX, 256 - BLK), F32)], axis=1)
            Hs[k, a] = blk.astype(BF16)
    for k in range(1, NX):
        t = lax.rem(x + k, NX)
        remote(Hs.at[t], Hc.at[x], sH, rH, dev(t, y, z, c)).start()
    Hc[x] = Hs[x]

    def region(f, cc, a, o):
        return W.at[f, cc, a, pl.ds(pl.multiple_of(80 * o, 16), 80), :]

    om = iota((80, 128), 0)
    mm_ = iota((80, 128), 1)
    hit = jnp.zeros((80, 128), jnp.bool_)
    for k in range(4):
        hit = jnp.logical_or(
            hit,
            jnp.logical_and(
                jnp.logical_and(mm_ >= 32 * k, mm_ < 32 * k + 20), om == mm_ - 12 * k
            ),
        )
    join = hit.astype(F32).astype(BF16)

    place = {1: y, 0: z}

    def at(f, p):
        return dev(x, p, z, c) if f == 1 else dev(x, y, p, c)

    def up(f, s, a):
        p = place[f]
        o = lax.rem(p - s + 8, 8)
        return remote(
            region(f, c, a, o), region(f, c, a, o), sR.at[f], rR.at[f, 0, s, a],
            at(f, lax.rem(p + 1, 8)),
        )

    def down(f, s, a):
        p = place[f]
        o = lax.rem(p + s, 8)
        return remote(
            region(f, c, a, o), region(f, c, a, o), sR.at[f], rR.at[f, 1, s, a],
            at(f, lax.rem(p + 7, 8)),
        )

    def share(f, a, o):
        o = lax.rem(o + 8, 8)
        remote(
            region(f, c, a, o), region(f, c, a, o), sP.at[f], rP.at[f], dev(x, y, z, 1 - c)
        ).start()

    for f in (1, 0):
        local_wait(RA.at[f], rA.at[f])
        for b in range(2):
            piece = dot(join, RA[f, 4 * b : 4 * b + 4].reshape(128, 384)).astype(BF16)
            for a in range(3):
                W[
                    f, c, a, pl.ds(pl.multiple_of(80 * place[f], 16), 80),
                    128 * b : 128 * b + 128,
                ] = piece[:, 128 * a : 128 * a + 128]
        for a in range(3):
            up(f, 0, a).start()
            down(f, 0, a).start()
            share(f, a, place[f])

    local_wait(Hc.at[0:3], rH)
    lane = iota((8, 256), 1)
    row8 = iota((8, 256), 0)
    sums = jnp.zeros((8, 256), F32)
    for a in range(2):
        for img in range(2):
            tot = jnp.zeros((1, 256), F32)
            sq = jnp.zeros((1, 256), F32)
            for t in range(NX):
                v = Hc[t, a, 64 * img : 64 * img + 64, :].astype(F32)
                tot = tot + jnp.sum(v, axis=0, keepdims=True)
                sq = sq + jnp.sum(v * v, axis=0, keepdims=True)
            sums = jnp.where(row8 == 4 * a + img, tot, sums)
            sums = jnp.where(row8 == 4 * a + 2 + img, sq, sums)

    def send_sums(p, value):
        SS[p] = value
        ST[p, y] = value
        for k in range(1, NY):
            remote(
                SS.at[p], ST.at[p, y], sS.at[p], rS.at[p], dev(x, lax.rem(y + k, NY), z, c)
            ).start()

    gi = group_of(iota((256, 256), 0))
    gj = group_of(iota((256, 256), 1))
    same = jnp.logical_and(gi == gj, gi < 4).astype(F32)

    def take_sums(p):
        local_wait(ST.at[p, 0:7], rS.at[p])
        tot = ST[p, 0]
        for k in range(1, NY):
            tot = tot + ST[p, k]
        return dot(tot, same, precision=lax.Precision.HIGHEST) / NUMBER

    send_sums(0, sums)

    for s in range(4):
        for f in (1, 0):
            for a in range(3):
                up(f, s, a).wait_recv()
                if s < 3:
                    up(f, s + 1, a).start()
                share(f, a, place[f] - 1 - s)
                if s < 3:
                    down(f, s, a).wait_recv()
                    if s < 2:
                        down(f, s + 1, a).start()
                    share(f, a, place[f] + 1 + s)

    mean = take_sums(0)
    stats = []
    for a in range(2):
        avg = mean[4 * a : 4 * a + 2]
        inv = lax.rsqrt(mean[4 * a + 2 : 4 * a + 4] - avg * avg + 1e-05)
        stats.append((avg, inv))

    own_cot.wait()
    local_wait(G.at[0:3], rG)
    pick = (iota((CH, 256), 0) == iota((CH, 256), 1) + BLK * x) & (iota((CH, 256), 1) < BLK)
    pick = pick.astype(F32).astype(BF16)
    for t in range(NX):
        CC[t] = dot(G[t], pick)

    def combine(accs):
        rows = accs[0].shape[0]
        q = jnp.bitwise_and(iota((rows, 128), 0), 63)
        ln = iota((rows, 128), 1)
        t0 = jnp.zeros((rows, 128), F32)
        t1 = jnp.zeros((rows, 128), F32)
        for j in range(4):
            b = j // 2
            blk = accs[j % 2][:, 128 * b : 128 * b + 128]
            low = jnp.where(q == 63, 0.0, pltpu.roll(blk, rows - 1, 0))
            mid = pltpu.roll(blk, 128 - 40, 1)
            high = jnp.where(q == 0, 0.0, pltpu.roll(pltpu.roll(blk, 128 - 80, 1), 1, 0))
            v = jnp.where(ln < 40, low + mid + high, 0.0)
            if j:
                v = pltpu.roll(v, 40 * j, 1)
            if j < 3:
                t0 = t0 + v
            else:
                t0 = t0 + jnp.where(ln >= 120, v, 0.0)
                t1 = jnp.where(ln < 32, v, 0.0)
        return jnp.concatenate([t0, t1], axis=1)

    def conv(n, f, mul):
        for e, (ai, t) in enumerate(((0, 0), (2, 3))):
            HBs[n, e] = combine([mul(f, cc, ai, t, t + 1) for cc in range(2)])

        @pl.when(y > 0)
        def _():
            remote(HBs.at[n, 0], HBr.at[n, 0], sB.at[n, 0], rB.at[n, 0], dev(x, lax.rem(y + 7, 8), z, c)).start()

        @pl.when(y < NY - 1)
        def _():
            remote(HBs.at[n, 1], HBr.at[n, 1], sB.at[n, 1], rB.at[n, 1], dev(x, lax.rem(y + 1, 8), z, c)).start()

        for cc in range(2):
            AC[cc] = mul(f, cc, 1, 0, 4)
            AC[cc, 0:384] += mul(f, cc, 0, 1, 4)
            AC[cc, 128:512] += mul(f, cc, 2, 0, 3)
        BK[...] = combine([AC[0], AC[1]])

        @pl.when(y < NY - 1)
        def _():
            local_wait(HBr.at[n, 0], rB.at[n, 0])
            BK[384:512] += HBr[n, 0]

        @pl.when(y > 0)
        def _():
            local_wait(HBr.at[n, 1], rB.at[n, 1])
            BK[0:128] += HBr[n, 1]

    def mul_cot(f, cc, ai, t0, t1):
        return dot(G[t0:t1].reshape((t1 - t0) * PX, CH), W[f, cc, ai])

    def mul_grad(f, cc, ai, t0, t1):
        acc = None
        for k in range(NX):
            v = dot(
                Gh[k, t0 * PX : t1 * PX, 0:BLK], W[f, cc, ai, BLK * k : BLK * k + BLK, :]
            )
            acc = v if acc is None else acc + v
        return acc

    def norm_sums(n, a, gain, shift):
        avg, inv = stats[a]
        first = [jnp.zeros((1, 256), F32)] * 2
        second = [jnp.zeros((1, 256), F32)] * 2
        for t in range(NX):
            for img in range(2):
                px = slice(t * PX + 64 * img, t * PX + 64 * img + 64)
                v = Hc[t, a, 64 * img : 64 * img + 64, :].astype(F32)
                normed = (v - avg[img : img + 1]) * inv[img : img + 1]
                linear = normed * gain + shift
                s = jax.nn.sigmoid(linear)
                scaled = BK[px, :] * s * (1.0 + linear * (1.0 - s)) * gain
                BK[px, :] = scaled
                first[img] = first[img] + jnp.sum(scaled, axis=0, keepdims=True)
                second[img] = second[img] + jnp.sum(scaled * normed, axis=0, keepdims=True)
        value = jnp.zeros((8, 256), F32)
        for img in range(2):
            value = jnp.where(row8 == img, first[img], value)
            value = jnp.where(row8 == 2 + img, second[img], value)
        send_sums(n, value)
        got = take_sums(n)
        return got[0:2], got[2:4]

    def norm_apply(a, t, img, first, second):
        avg, inv = stats[a]
        px = slice(t * PX + 64 * img, t * PX + 64 * img + 64)
        v = Hc[t, a, 64 * img : 64 * img + 64, :].astype(F32)
        i_ = inv[img : img + 1]
        normed = (v - avg[img : img + 1]) * i_
        return i_ * (BK[px, :] - first[img : img + 1] - normed * second[img : img + 1])

    par_x = par[x]
    local_wait(W.at[1, 1 - c], rP.at[1])
    conv(0, 1, mul_cot)
    first, second = norm_sums(1, 0, par_x[0:1], par_x[1:2])
    for t in range(NX):
        for img in range(2):
            px = slice(t * PX + 64 * img, t * PX + 64 * img + 64)
            Gh[x, px, :] = norm_apply(0, t, img, first, second).astype(BF16)
    for k in range(1, NX):
        remote(Gh.at[x], Gh.at[x], sGh, rGh, dev(lax.rem(x + k, NX), y, z, c)).start()
    local_wait(W.at[0, 1 - c], rP.at[0])
    local_wait(Gh.at[0:3], rGh)

    conv(1, 0, mul_grad)
    first, second = norm_sums(2, 1, par_x[2:3], par_x[3:4])
    for t in range(NX):
        for img in range(2):
            q = slice(64 * img, 64 * img + 64)
            v = CC[t, q, :] + norm_apply(1, t, img, first, second)
            Os[t, q, :] = v.astype(BF16)
    for k in range(1, NX):
        t = lax.rem(x + k, NX)
        remote(Os.at[t], Oc.at[x], sO, rO, dev(t, y, z, c)).start()
    Oc[x] = Os[x]

    for f in (1, 0):
        if f == 1:
            mine = x == X
        else:
            mine = jnp.logical_and(x == X, y == z)
        local_wait(RA.at[f, 0:7], sA.at[f])

        @pl.when(jnp.logical_not(mine))
        def _():
            local_wait(RA.at[f, 0], sA0.at[f])

        local_wait(W.at[f, 0, :, 0:560, :], sR.at[f])
        local_wait(W.at[f, 0], sP.at[f])
    local_wait(G.at[0:3], sG)
    local_wait(Gh.at[0:3], sGh)
    local_wait(Hc.at[0:3], sH)
    for p in range(3):
        local_wait(ST.at[p, 0:7], sS.at[p])
    for n in range(2):
        @pl.when(y > 0)
        def _():
            local_wait(HBs.at[n, 0], sB.at[n, 0])

        @pl.when(y < NY - 1)
        def _():
            local_wait(HBs.at[n, 1], sB.at[n, 1])

    local_wait(Oc.at[0:3], rO)
    local_wait(Oc.at[0:3], sO)
    out[...] = jnp.concatenate([Oc[k, :, 0:BLK].astype(F32) for k in range(NX)], axis=1).astype(
        BF16
    )


def body(latent, hidden, cotangent, filter_one, filter_two, gain_one, shift_one, gain_two, shift_two):
    both = jnp.stack([filter_one, filter_two]).reshape(2, 3, 120, 20)
    wb = jnp.transpose(both, (0, 3, 1, 2))
    wb = jnp.pad(wb, ((0, 0), (0, 12), (0, 0), (0, 8))).reshape(2, 32, 384)
    par = jnp.stack([gain_two, shift_two, gain_one, shift_one]).reshape(4, NX, BLK)
    par = jnp.pad(jnp.transpose(par, (1, 0, 2)), ((0, 0), (0, 4), (0, 256 - BLK)))
    rows = [a.reshape(PX, CH) for a in (cotangent, hidden, latent)]
    vmem = pl.BlockSpec(memory_space=pltpu.VMEM)
    dma = pltpu.SemaphoreType.DMA
    out = pl.pallas_call(
        kernel,
        out_shape=jax.ShapeDtypeStruct((PX, CH), BF16),
        in_specs=[vmem] * 5,
        out_specs=vmem,
        scratch_shapes=[
            pltpu.VMEM((2, 2, 3, CH, 256), BF16),
            pltpu.VMEM((2, 8, 32, 384), BF16),
            pltpu.VMEM((NX, PX, CH), BF16),
            pltpu.VMEM((NX, NX * PX, 256), BF16),
            pltpu.VMEM((NX, 2, PX, 256), BF16),
            pltpu.VMEM((NX, 2, PX, 256), BF16),
            pltpu.VMEM((3, 8, 256), F32),
            pltpu.VMEM((3, NY, 8, 256), F32),
            pltpu.VMEM((2, 2, PX, 256), F32),
            pltpu.VMEM((2, 2, PX, 256), F32),
            pltpu.VMEM((2, NX * PX, 256), F32),
            pltpu.VMEM((NX * PX, 256), F32),
            pltpu.VMEM((NX, PX, 256), BF16),
            pltpu.VMEM((NX, PX, 256), BF16),
            pltpu.VMEM((NX, PX, 256), F32),
            dma((2,)), dma((2,)), dma((2,)), dma,
            dma((2,)), dma((2, 2, 4, 3)),
            dma((2,)), dma((2,)),
            dma, dma, dma, dma, dma, dma,
            dma((3,)), dma((3,)),
            dma((2, 2)), dma((2, 2)),
            dma, dma,
        ],
        compiler_params=pltpu.CompilerParams(
            has_side_effects=True, vmem_limit_bytes=48 * 1024 * 1024
        ),
        name="block_backward",
    )(wb, *rows, par)
    return out.reshape(latent.shape)


def solution(mesh):
    in_specs = (
        P("dp", "rows", None, None),
        P("dp", "rows", None, None),
        P("dp", "rows", None, None),
        P(None, "dp", "rows"),
        P(None, "dp", "rows"),
        P(),
        P(),
        P(),
        P(),
    )
    out_specs = P("dp", "rows", None, None)
    return jax.shard_map(body, mesh=mesh, in_specs=in_specs, out_specs=out_specs, check_vma=False)
```

```python
import jax
import jax.numpy as jnp
from jax import lax
from jax.experimental import pallas as pl
from jax.experimental.pallas import tpu as pltpu
from jax.sharding import PartitionSpec as P

MESH = pl.DeviceIdType.MESH
F32 = jnp.float32
BF16 = jnp.bfloat16
NX, NY, NZ = 4, 8, 8
CH = 640
BLK = 160
PX = 128
NUMBER = 32 * 64 * 40


def dev(x, y, z, c):
    return (2 * z + c, 4 * y + x)


def iota(shape, dim):
    return lax.broadcasted_iota(jnp.int32, shape, dim)


def dot(a, b, **kw):
    return jnp.dot(a, b, preferred_element_type=F32, **kw)


def group_of(lane):
    g = jnp.zeros_like(lane)
    for edge in (40, 80, 120, 160):
        g = g + (lane >= edge).astype(jnp.int32)
    return g


def kernel(
    f1, f2, cot, hid, lat, g2, s2, g1, s1, out,
    FV, PV, HV, WB, W, W1, RA, G, Gh, L, Hs, Hc, Hx, SS, ST, HBs, HBr, AC, BK, Os, Oc, CC,
    lF, lP, lH, lC, sA, sA0, rA, sR, rR, sP, rP, sG, rG, sGh, rGh, sH, rH, sS, rS, sB, rB, sO, rO,
):
    dp = lax.axis_index("dp")
    rr = lax.axis_index("rows")
    c = lax.rem(dp, 2)
    z = lax.div(dp, 2)
    x = lax.rem(rr, NX)
    y = lax.div(rr, NX)
    X = lax.div(z, 2)
    mine_y = x == X
    mine_z = jnp.logical_and(x == X, y == z)

    def remote(src, dst, ss, rs, target):
        return pltpu.make_async_remote_copy(
            src_ref=src, dst_ref=dst, send_sem=ss, recv_sem=rs, device_id=target,
            device_id_type=MESH,
        )

    def local_wait(ref, sem):
        pltpu.make_async_copy(ref, ref, sem).wait()

    bar = pltpu.get_barrier_semaphore()

    def here(target):
        pl.semaphore_signal(bar, inc=1, device_id=target, device_id_type=MESH)

    for b in range(2):
        zs = 2 * x + lax.rem(z + b, 2)
        for k in range(NX):
            xs = lax.rem(x + k, NX)
            if b == 0 and k == 0:
                @pl.when(jnp.logical_not(mine_y))
                def _():
                    here(dev(xs, y, zs, c))

                @pl.when(jnp.logical_not(mine_z))
                def _():
                    here(dev(xs, z, zs, c))
            else:
                here(dev(xs, y, zs, c))
                here(dev(xs, z, zs, c))
    for k in range(1, NX):
        here(dev(lax.rem(x + k, NX), y, z, c))
    for k in range(1, NY):
        here(dev(x, lax.rem(y + k, NY), z, c))
    for k in (1, NZ - 1):
        here(dev(x, y, lax.rem(z + k, NZ), c))
    here(dev(x, y, z, 1 - c))

    loads = [pltpu.make_async_copy(r, FV.at[f], lF.at[f]) for f, r in enumerate((f1, f2))]
    loads += [pltpu.make_async_copy(r, HV.at[a], lH.at[a]) for a, r in enumerate((hid, lat))]
    loads += [
        pltpu.make_async_copy(r, PV[a], lP.at[a]) for a, r in enumerate((g2, s2, g1, s1))
    ]
    own_cot = pltpu.make_async_copy(cot, G.at[x], lC)
    for load in loads[1::-1] + loads[2:]:
        load.start()
    own_cot.start()
    WB[...] = jnp.zeros_like(WB)
    for f in (1, 0):
        loads[f].wait()
        for a in range(3):
            taps = [FV[f, 3 * a + b].astype(F32) for b in range(3)]
            WB[f, 0:20, 128 * a : 128 * a + 128] = jnp.concatenate(
                taps + [jnp.zeros((20, 8), F32)], axis=1
            ).astype(BF16)
    for a in range(2):
        loads[2 + a].wait()
    v = [HV[a].astype(F32) for a in range(2)]
    for k in range(NX):
        Hs[k] = jnp.concatenate(
            [v[a][:, BLK * k : BLK * k + BLK] for a in range(2)] + [jnp.zeros((PX, 64), F32)],
            axis=1,
        ).astype(BF16)
    params = []
    for a in range(4):
        loads[4 + a].wait()
        whole = PV[a][...].reshape(1, CH)
        p = jnp.zeros((1, BLK), F32)
        for k in range(NX):
            p = jnp.where(x == k, whole[:, BLK * k : BLK * k + BLK], p)
        params.append(jnp.concatenate([p, jnp.zeros((1, 256 - BLK), F32)], axis=1))
    own_cot.wait()

    pl.semaphore_wait(
        bar, 29 - mine_y.astype(jnp.int32) - mine_z.astype(jnp.int32)
    )

    slot = lax.rem(z, 2) * 4 + x
    for f in (1, 0):
        for k in range(8):
            if f == 1:
                z_, y_, mine = lax.rem(z + k, NZ), y, mine_y
            else:
                z_, y_, mine = y, lax.rem(y + k, NY), mine_z
            target = dev(X, y_, z_, c)
            if k == 0:
                @pl.when(mine)
                def _():
                    pltpu.make_async_copy(WB.at[f], RA.at[f, slot], rA.at[f]).start()

                @pl.when(jnp.logical_not(mine))
                def _():
                    remote(WB.at[f], RA.at[f, slot], sA0.at[f], rA.at[f], target).start()
            else:
                remote(WB.at[f], RA.at[f, slot], sA.at[f], rA.at[f], target).start()

    def region(f, cc, a, o):
        return W.at[f, cc, a, pl.ds(pl.multiple_of(80 * o, 16), 80), :]

    om = iota((80, 128), 0)
    mm_ = iota((80, 128), 1)
    hit = jnp.zeros((80, 128), jnp.bool_)
    for k in range(4):
        hit = jnp.logical_or(
            hit,
            jnp.logical_and(
                jnp.logical_and(mm_ >= 32 * k, mm_ < 32 * k + 20), om == mm_ - 12 * k
            ),
        )
    join = hit.astype(F32).astype(BF16)

    place = {1: y, 0: z}

    def at(f, p):
        return dev(x, p, z, c) if f == 1 else dev(x, y, p, c)

    def up(f, s, a):
        p = place[f]
        o = lax.rem(p - s + 8, 8)
        return remote(
            region(f, c, a, o), region(f, c, a, o), sR.at[f], rR.at[f, 0, s, a],
            at(f, lax.rem(p + 1, 8)),
        )

    def down(f, s, a):
        p = place[f]
        o = lax.rem(p + s, 8)
        return remote(
            region(f, c, a, o), region(f, c, a, o), sR.at[f], rR.at[f, 1, s, a],
            at(f, lax.rem(p + 7, 8)),
        )

    def share(f, a, o):
        o = lax.rem(o + 8, 8)
        remote(
            region(f, c, a, o), region(f, c, a, o), sP.at[f], rP.at[f], dev(x, y, z, 1 - c)
        ).start()

    for f in (1, 0):
        local_wait(RA.at[f], rA.at[f])
        for b in range(2):
            piece = dot(join, RA[f, 4 * b : 4 * b + 4].reshape(128, 384)).astype(BF16)
            for a in range(3):
                W[
                    f, c, a, pl.ds(pl.multiple_of(80 * place[f], 16), 80),
                    128 * b : 128 * b + 128,
                ] = piece[:, 128 * a : 128 * a + 128]
        for a in range(3):
            up(f, 0, a).start()
            down(f, 0, a).start()
            share(f, a, place[f])
        if f == 1:
            for k in range(1, NX):
                t = lax.rem(x + k, NX)
                remote(G.at[x], G.at[x], sG, rG, dev(t, y, z, c)).start()
            for k in range(1, NX):
                t = lax.rem(x + k, NX)
                remote(Hs.at[t], Hc.at[x], sH, rH, dev(t, y, z, c)).start()
            Hc[x] = Hs[x]

    for s in range(4):
        for f in (1, 0):
            for a in range(3):
                up(f, s, a).wait_recv()
                if s < 3:
                    up(f, s + 1, a).start()
                share(f, a, place[f] - 1 - s)
                if s < 3:
                    down(f, s, a).wait_recv()
                    if s < 2:
                        down(f, s + 1, a).start()
                    share(f, a, place[f] + 1 + s)

    row8 = iota((8, 256), 0)
    local_wait(Hc.at[0:3], rH)
    zero = jnp.zeros((64, 256 - BLK), F32)
    sums = jnp.zeros((8, 256), F32)
    for img in range(2):
        tot = [jnp.zeros((1, 256), F32)] * 2
        sq = [jnp.zeros((1, 256), F32)] * 2
        for t in range(NX):
            both = Hc[t, 64 * img : 64 * img + 64, :].astype(F32)
            for a in range(2):
                v = jnp.concatenate([both[:, BLK * a : BLK * a + BLK], zero], axis=1)
                Hx[a, t, 64 * img : 64 * img + 64, :] = v
                tot[a] = tot[a] + jnp.sum(v, axis=0, keepdims=True)
                sq[a] = sq[a] + jnp.sum(v * v, axis=0, keepdims=True)
        for a in range(2):
            sums = jnp.where(row8 == 4 * a + img, tot[a], sums)
            sums = jnp.where(row8 == 4 * a + 2 + img, sq[a], sums)

    def send_sums(p, value):
        SS[p] = value
        ST[p, y] = value
        for k in range(1, NY):
            remote(
                SS.at[p], ST.at[p, y], sS.at[p], rS.at[p], dev(x, lax.rem(y + k, NY), z, c)
            ).start()

    gi = group_of(iota((256, 256), 0))
    gj = group_of(iota((256, 256), 1))
    same = jnp.logical_and(gi == gj, gi < 4).astype(F32)

    def take_sums(p):
        local_wait(ST.at[p, 0:7], rS.at[p])
        tot = ST[p, 0]
        for k in range(1, NY):
            tot = tot + ST[p, k]
        return dot(tot, same, precision=lax.Precision.HIGHEST) / NUMBER

    send_sums(0, sums)

    def combine(accs):
        rows = accs[0].shape[0]
        q = jnp.bitwise_and(iota((rows, 128), 0), 63)
        ln = iota((rows, 128), 1)
        t0 = jnp.zeros((rows, 128), F32)
        t1 = jnp.zeros((rows, 128), F32)
        for j in range(4):
            b = j // 2
            blk = accs[j % 2][:, 128 * b : 128 * b + 128]
            low = jnp.where(q == 63, 0.0, pltpu.roll(blk, rows - 1, 0))
            mid = pltpu.roll(blk, 128 - 40, 1)
            high = jnp.where(q == 0, 0.0, pltpu.roll(pltpu.roll(blk, 128 - 80, 1), 1, 0))
            v = jnp.where(ln < 40, low + mid + high, 0.0)
            if j:
                v = pltpu.roll(v, 40 * j, 1)
            if j < 3:
                t0 = t0 + v
            else:
                t0 = t0 + jnp.where(ln >= 120, v, 0.0)
                t1 = jnp.where(ln < 32, v, 0.0)
        return jnp.concatenate([t0, t1], axis=1)

    def conv(n, f, mul):
        for e, (ai, t) in enumerate(((0, 0), (2, 3))):
            HBs[n, e] = combine([mul(f, cc, ai, t, t + 1) for cc in range(2)])

        @pl.when(y > 0)
        def _():
            remote(HBs.at[n, 0], HBr.at[n, 0], sB.at[n, 0], rB.at[n, 0], dev(x, lax.rem(y + 7, 8), z, c)).start()

        @pl.when(y < NY - 1)
        def _():
            remote(HBs.at[n, 1], HBr.at[n, 1], sB.at[n, 1], rB.at[n, 1], dev(x, lax.rem(y + 1, 8), z, c)).start()

        for cc in range(2):
            AC[cc] = mul(f, cc, 1, 0, 4)
            AC[cc, 0:384] += mul(f, cc, 0, 1, 4)
            AC[cc, 128:512] += mul(f, cc, 2, 0, 3)
        BK[...] = combine([AC[0], AC[1]])

        @pl.when(y < NY - 1)
        def _():
            local_wait(HBr.at[n, 0], rB.at[n, 0])
            BK[384:512] += HBr[n, 0]

        @pl.when(y > 0)
        def _():
            local_wait(HBr.at[n, 1], rB.at[n, 1])
            BK[0:128] += HBr[n, 1]

    def mul_cot(f, cc, ai, t0, t1):
        return dot(G[t0:t1].reshape((t1 - t0) * PX, CH), W[f, cc, ai])

    def mul_grad(f, cc, ai, t0, t1):
        return dot(L[t0 * PX : t1 * PX, :], W1[cc, ai])

    def norm_sums(n, a, gain, shift):
        avg, inv = stats[a]
        first = [jnp.zeros((1, 256), F32)] * 2
        second = [jnp.zeros((1, 256), F32)] * 2
        for t in range(NX):
            for img in range(2):
                px = slice(t * PX + 64 * img, t * PX + 64 * img + 64)
                v = Hx[a, t, 64 * img : 64 * img + 64, :]
                normed = (v - avg[img : img + 1]) * inv[img : img + 1]
                linear = normed * gain + shift
                s = jax.nn.sigmoid(linear)
                scaled = BK[px, :] * s * (1.0 + linear * (1.0 - s)) * gain
                BK[px, :] = scaled
                first[img] = first[img] + jnp.sum(scaled, axis=0, keepdims=True)
                second[img] = second[img] + jnp.sum(scaled * normed, axis=0, keepdims=True)
        value = jnp.zeros((8, 256), F32)
        for img in range(2):
            value = jnp.where(row8 == img, first[img], value)
            value = jnp.where(row8 == 2 + img, second[img], value)
        send_sums(n, value)
        if n == 1:
            spare_time()
        got = take_sums(n)
        return got[0:2], got[2:4]

    def norm_apply(a, t, img, first, second):
        avg, inv = stats[a]
        px = slice(t * PX + 64 * img, t * PX + 64 * img + 64)
        v = Hx[a, t, 64 * img : 64 * img + 64, :]
        i_ = inv[img : img + 1]
        normed = (v - avg[img : img + 1]) * i_
        return i_ * (BK[px, :] - first[img : img + 1] - normed * second[img : img + 1])

    def spare_time():
        pick = (iota((CH, 256), 0) == iota((CH, 256), 1) + BLK * x) & (iota((CH, 256), 1) < BLK)
        pick = pick.astype(F32).astype(BF16)
        for t in range(NX):
            CC[t] = dot(G[t], pick)
        local_wait(W.at[0, 1 - c], rP.at[0])
        for k in range(NX):
            W1[:, :, 128 * k : 128 * k + 128, :] = W[0, :, :, BLK * k : BLK * k + 128, :]
            W1[:, :, 512 + 32 * k : 544 + 32 * k, :] = W[0, :, :, BLK * k + 128 : BLK * k + BLK, :]

    local_wait(G.at[0:3], rG)
    local_wait(W.at[1, 1 - c], rP.at[1])
    conv(0, 1, mul_cot)
    mean = take_sums(0)
    stats = []
    for a in range(2):
        avg = mean[4 * a : 4 * a + 2]
        inv = lax.rsqrt(mean[4 * a + 2 : 4 * a + 4] - avg * avg + 1e-05)
        stats.append((avg, inv))
    first, second = norm_sums(1, 0, params[0], params[1])
    for img in range(2):
        rest = jnp.zeros((64, 128), F32)
        for t in range(NX):
            v = norm_apply(0, t, img, first, second)
            Gh[x, t * PX + 64 * img : t * PX + 64 * img + 64, :] = v[:, 0:128].astype(BF16)
            rest = rest + (pltpu.roll(v[:, 128:256], 32 * t, 1) if t else v[:, 128:256])
        Gh[x, 512 + 64 * img : 576 + 64 * img, :] = rest.astype(BF16)
    for k in range(1, NX):
        remote(Gh.at[x], Gh.at[x], sGh, rGh, dev(lax.rem(x + k, NX), y, z, c)).start()
    local_wait(Gh.at[0:3], rGh)
    lane = iota((PX, 128), 1)
    rests = [Gh[k, 512:640, :].astype(F32) for k in range(NX)]
    for k in range(NX):
        L[:, 128 * k : 128 * k + 128] = Gh[k, 0:512, :]
    for t in range(NX):
        v = jnp.zeros((PX, 128), F32)
        for k in range(NX):
            w = pltpu.roll(rests[k], (32 * (k - t)) % 128, 1) if k != t else rests[k]
            v = jnp.where((lane >= 32 * k) & (lane < 32 * k + 32), w, v)
        L[t * PX : t * PX + PX, 512:640] = v.astype(BF16)

    conv(1, 0, mul_grad)
    first, second = norm_sums(2, 1, params[2], params[3])
    for t in range(NX):
        for img in range(2):
            q = slice(64 * img, 64 * img + 64)
            v = CC[t, q, :] + norm_apply(1, t, img, first, second)
            Os[t, q, :] = v.astype(BF16)
    for k in range(1, NX):
        t = lax.rem(x + k, NX)
        remote(Os.at[t], Oc.at[x], sO, rO, dev(t, y, z, c)).start()
    Oc[x] = Os[x]

    for f in (1, 0):
        mine = mine_y if f == 1 else mine_z
        local_wait(RA.at[f, 0:7], sA.at[f])

        @pl.when(jnp.logical_not(mine))
        def _():
            local_wait(RA.at[f, 0], sA0.at[f])

        local_wait(W.at[f, 0, :, 0:560, :], sR.at[f])
        local_wait(W.at[f, 0], sP.at[f])
    local_wait(G.at[0:3], sG)
    local_wait(Gh.at[0:3], sGh)
    local_wait(Hc.at[0:3], sH)
    for p in range(3):
        local_wait(ST.at[p, 0:7], sS.at[p])
    for n in range(2):
        @pl.when(y > 0)
        def _():
            local_wait(HBs.at[n, 0], sB.at[n, 0])

        @pl.when(y < NY - 1)
        def _():
            local_wait(HBs.at[n, 1], sB.at[n, 1])

    local_wait(Oc.at[0:3], rO)
    local_wait(Oc.at[0:3], sO)
    out[...] = jnp.concatenate([Oc[k, :, 0:BLK].astype(F32) for k in range(NX)], axis=1).astype(
        BF16
    )


def body(latent, hidden, cotangent, filter_one, filter_two, gain_one, shift_one, gain_two, shift_two):
    filters = [jnp.transpose(a, (0, 2, 1)) for a in (filter_one, filter_two)]
    rows = [a.reshape(PX, CH) for a in (cotangent, hidden, latent)]
    params = (gain_two, shift_two, gain_one, shift_one)
    vmem = pl.BlockSpec(memory_space=pltpu.VMEM)
    anywhere = pl.BlockSpec(memory_space=pl.ANY)
    dma = pltpu.SemaphoreType.DMA
    out = pl.pallas_call(
        kernel,
        out_shape=jax.ShapeDtypeStruct((PX, CH), BF16),
        in_specs=[anywhere] * 9,
        out_specs=vmem,
        scratch_shapes=[
            pltpu.VMEM((2, 9, 20, 40), BF16),
            [pltpu.VMEM((CH,), F32)] * 4,
            pltpu.VMEM((2, PX, CH), BF16),
            pltpu.VMEM((2, 32, 384), BF16),
            pltpu.VMEM((2, 2, 3, CH, 256), BF16),
            pltpu.VMEM((2, 3, CH, 256), BF16),
            pltpu.VMEM((2, 8, 32, 384), BF16),
            pltpu.VMEM((NX, PX, CH), BF16),
            pltpu.VMEM((NX, 640, 128), BF16),
            pltpu.VMEM((NX * PX, CH), BF16),
            pltpu.VMEM((NX, PX, 384), BF16),
            pltpu.VMEM((NX, PX, 384), BF16),
            pltpu.VMEM((2, NX, PX, 256), F32),
            pltpu.VMEM((3, 8, 256), F32),
            pltpu.VMEM((3, NY, 8, 256), F32),
            pltpu.VMEM((2, 2, PX, 256), F32),
            pltpu.VMEM((2, 2, PX, 256), F32),
            pltpu.VMEM((2, NX * PX, 256), F32),
            pltpu.VMEM((NX * PX, 256), F32),
            pltpu.VMEM((NX, PX, 256), BF16),
            pltpu.VMEM((NX, PX, 256), BF16),
            pltpu.VMEM((NX, PX, 256), F32),
            dma((2,)), dma((4,)), dma((2,)), dma,
            dma((2,)), dma((2,)), dma((2,)),
            dma((2,)), dma((2, 2, 4, 3)),
            dma((2,)), dma((2,)),
            dma, dma, dma, dma, dma, dma,
            dma((3,)), dma((3,)),
            dma((2, 2)), dma((2, 2)),
            dma, dma,
        ],
        compiler_params=pltpu.CompilerParams(
            collective_id=0, has_side_effects=True, vmem_limit_bytes=62 * 1024 * 1024
        ),
        name="block_backward",
    )(*filters, *rows, *params)
    return out.reshape(latent.shape)


def solution(mesh):
    in_specs = (
        P("dp", "rows", None, None),
        P("dp", "rows", None, None),
        P("dp", "rows", None, None),
        P(None, "dp", "rows"),
        P(None, "dp", "rows"),
        P(),
        P(),
        P(),
        P(),
    )
    out_specs = P("dp", "rows", None, None)
    return jax.shard_map(body, mesh=mesh, in_specs=in_specs, out_specs=out_specs, check_vma=False)
```

```python
import jax
import jax.numpy as jnp
from jax import lax
from jax.experimental import pallas as pl
from jax.experimental.pallas import tpu as pltpu
from jax.sharding import PartitionSpec as P

MESH = pl.DeviceIdType.MESH
F32 = jnp.float32
BF16 = jnp.bfloat16
NX, NY, NZ = 4, 8, 8
CH = 640
BLK = 160
PX = 128
NUMBER = 32 * 64 * 40


def dev(x, y, z, c):
    return (2 * z + c, 4 * y + x)


def iota(shape, dim):
    return lax.broadcasted_iota(jnp.int32, shape, dim)


def dot(a, b, **kw):
    return jnp.dot(a, b, preferred_element_type=F32, **kw)


def group_of(lane):
    g = jnp.zeros_like(lane)
    for edge in (40, 80, 120, 160):
        g = g + (lane >= edge).astype(jnp.int32)
    return g


def kernel(
    f1, f2, cot, hid, lat, g2, s2, g1, s1, out,
    FV, PV, HV, WB, W, W1, RA, G, Gh, L, Hs, Hc, Hx, SS, ST, HBs, HBr, AC, BK, Os, Oc, CC,
    lF, lP, lH, lC, sA, sA0, rA, sR, rR, sP, rP, sG, rG, sGh, rGh, sH, rH, sS, rS, sB, rB, sO, rO,
):
    dp = lax.axis_index("dp")
    rr = lax.axis_index("rows")
    c = lax.rem(dp, 2)
    z = lax.div(dp, 2)
    x = lax.rem(rr, NX)
    y = lax.div(rr, NX)
    X = lax.div(z, 2)
    mine_y = x == X
    mine_z = jnp.logical_and(x == X, y == z)

    def remote(src, dst, ss, rs, target):
        return pltpu.make_async_remote_copy(
            src_ref=src, dst_ref=dst, send_sem=ss, recv_sem=rs, device_id=target,
            device_id_type=MESH,
        )

    def local_wait(ref, sem):
        pltpu.make_async_copy(ref, ref, sem).wait()

    bar = pltpu.get_barrier_semaphore()

    def here(target):
        pl.semaphore_signal(bar, inc=1, device_id=target, device_id_type=MESH)

    for b in range(2):
        zs = 2 * x + lax.rem(z + b, 2)
        for k in range(NX):
            xs = lax.rem(x + k, NX)
            if b == 0 and k == 0:
                @pl.when(jnp.logical_not(mine_y))
                def _():
                    here(dev(xs, y, zs, c))

                @pl.when(jnp.logical_not(mine_z))
                def _():
                    here(dev(xs, z, zs, c))
            else:
                here(dev(xs, y, zs, c))
                here(dev(xs, z, zs, c))
    for k in range(1, NX):
        here(dev(lax.rem(x + k, NX), y, z, c))
    for k in range(1, NY):
        here(dev(x, lax.rem(y + k, NY), z, c))
    for k in (1, NZ - 1):
        here(dev(x, y, lax.rem(z + k, NZ), c))
    here(dev(x, y, z, 1 - c))

    loads = [pltpu.make_async_copy(r, FV.at[f], lF.at[f]) for f, r in enumerate((f1, f2))]
    loads += [pltpu.make_async_copy(r, HV.at[a], lH.at[a]) for a, r in enumerate((hid, lat))]
    loads += [
        pltpu.make_async_copy(r, PV[a], lP.at[a]) for a, r in enumerate((g2, s2, g1, s1))
    ]
    own_cot = pltpu.make_async_copy(cot, G.at[x], lC)
    for load in loads[1::-1] + loads[2:]:
        load.start()
    own_cot.start()
    WB[...] = jnp.zeros_like(WB)
    for f in (1, 0):
        loads[f].wait()
        for a in range(3):
            taps = [FV[f, 3 * a + b].astype(F32) for b in range(3)]
            WB[f, 0:20, 128 * a : 128 * a + 128] = jnp.concatenate(
                taps + [jnp.zeros((20, 8), F32)], axis=1
            ).astype(BF16)
    for a in range(2):
        loads[2 + a].wait()
    v = [HV[a].astype(F32) for a in range(2)]
    for k in range(NX):
        Hs[k] = jnp.concatenate(
            [v[a][:, BLK * k : BLK * k + BLK] for a in range(2)] + [jnp.zeros((PX, 64), F32)],
            axis=1,
        ).astype(BF16)
    params = []
    for a in range(4):
        loads[4 + a].wait()
        whole = PV[a][...].reshape(1, CH)
        p = jnp.zeros((1, BLK), F32)
        for k in range(NX):
            p = jnp.where(x == k, whole[:, BLK * k : BLK * k + BLK], p)
        params.append(jnp.concatenate([p, jnp.zeros((1, 256 - BLK), F32)], axis=1))
    own_cot.wait()

    pl.semaphore_wait(
        bar, 29 - mine_y.astype(jnp.int32) - mine_z.astype(jnp.int32)
    )

    slot = lax.rem(z, 2) * 4 + x
    along_y = {f: lax.rem(f + c, 2) == 1 for f in (1, 0)}
    mine = {f: jnp.where(along_y[f], mine_y.astype(jnp.int32), mine_z.astype(jnp.int32)) == 1 for f in (1, 0)}
    place = {f: jnp.where(along_y[f], y, z) for f in (1, 0)}

    def first_stage(f):
        for k in range(8):
            y_ = jnp.where(along_y[f], y, lax.rem(y + k, NY))
            z_ = jnp.where(along_y[f], lax.rem(z + k, NZ), y)
            target = dev(X, y_, z_, c)
            if k == 0:
                @pl.when(mine[f])
                def _():
                    pltpu.make_async_copy(WB.at[f], RA.at[f, slot], rA.at[f]).start()

                @pl.when(jnp.logical_not(mine[f]))
                def _():
                    remote(WB.at[f], RA.at[f, slot], sA0.at[f], rA.at[f], target).start()
            else:
                remote(WB.at[f], RA.at[f, slot], sA.at[f], rA.at[f], target).start()

    first_stage(1)
    for k in range(1, NX):
        t = lax.rem(x + k, NX)
        remote(G.at[x], G.at[x], sG, rG, dev(t, y, z, c)).start()
    for k in range(1, NX):
        t = lax.rem(x + k, NX)
        remote(Hs.at[t], Hc.at[x], sH, rH, dev(t, y, z, c)).start()
    Hc[x] = Hs[x]

    def region(f, cc, a, o):
        return W.at[f, cc, a, pl.ds(pl.multiple_of(80 * o, 16), 80), :]

    om = iota((80, 96), 0)
    mm_ = iota((80, 96), 1)
    hit = jnp.zeros((80, 96), jnp.bool_)
    for k in range(4):
        hit = jnp.logical_or(
            hit,
            jnp.logical_and(
                jnp.logical_and(mm_ >= 24 * k, mm_ < 24 * k + 20), om == mm_ - 4 * k
            ),
        )
    join = hit.astype(F32).astype(BF16)

    def at(f, p):
        return dev(x, jnp.where(along_y[f], p, y), jnp.where(along_y[f], z, p), c)

    def up(f, s, a):
        p = place[f]
        o = lax.rem(p - s + 8, 8)
        return remote(
            region(f, c, a, o), region(f, c, a, o), sR.at[f], rR.at[f, 0, s, a],
            at(f, lax.rem(p + 1, 8)),
        )

    def down(f, s, a):
        p = place[f]
        o = lax.rem(p + s, 8)
        return remote(
            region(f, c, a, o), region(f, c, a, o), sR.at[f], rR.at[f, 1, s, a],
            at(f, lax.rem(p + 7, 8)),
        )

    def share(f, a, o):
        o = lax.rem(o + 8, 8)
        remote(
            region(f, c, a, o), region(f, c, a, o), sP.at[f], rP.at[f], dev(x, y, z, 1 - c)
        ).start()

    def start_ring(f):
        local_wait(RA.at[f], rA.at[f])
        for b in range(2):
            piece = dot(join, RA[f, 4 * b : 4 * b + 4].reshape(96, 384)).astype(BF16)
            for a in range(3):
                W[
                    f, c, a, pl.ds(pl.multiple_of(80 * place[f], 16), 80),
                    128 * b : 128 * b + 128,
                ] = piece[:, 128 * a : 128 * a + 128]
        for a in range(3):
            up(f, 0, a).start()
            down(f, 0, a).start()
            share(f, a, place[f])

    def ring_step(f, s):
        for a in range(3):
            up(f, s, a).wait_recv()
            if s < 3:
                up(f, s + 1, a).start()
            share(f, a, place[f] - 1 - s)
            if s < 3:
                down(f, s, a).wait_recv()
                if s < 2:
                    down(f, s + 1, a).start()
                share(f, a, place[f] + 1 + s)

    start_ring(1)
    first_stage(0)
    for s in range(4):
        ring_step(1, s)

    row8 = iota((8, 256), 0)
    local_wait(Hc.at[0:3], rH)
    zero = jnp.zeros((64, 256 - BLK), F32)
    sums = jnp.zeros((8, 256), F32)
    for img in range(2):
        tot = [jnp.zeros((1, 256), F32)] * 2
        sq = [jnp.zeros((1, 256), F32)] * 2
        for t in range(NX):
            both = Hc[t, 64 * img : 64 * img + 64, :].astype(F32)
            for a in range(2):
                v = jnp.concatenate([both[:, BLK * a : BLK * a + BLK], zero], axis=1)
                Hx[a, t, 64 * img : 64 * img + 64, :] = v
                tot[a] = tot[a] + jnp.sum(v, axis=0, keepdims=True)
                sq[a] = sq[a] + jnp.sum(v * v, axis=0, keepdims=True)
        for a in range(2):
            sums = jnp.where(row8 == 4 * a + img, tot[a], sums)
            sums = jnp.where(row8 == 4 * a + 2 + img, sq[a], sums)

    def send_sums(p, value):
        SS[p] = value
        ST[p, y] = value
        for k in range(1, NY):
            remote(
                SS.at[p], ST.at[p, y], sS.at[p], rS.at[p], dev(x, lax.rem(y + k, NY), z, c)
            ).start()

    gi = group_of(iota((256, 256), 0))
    gj = group_of(iota((256, 256), 1))
    same = jnp.logical_and(gi == gj, gi < 4).astype(F32)

    def take_sums(p):
        local_wait(ST.at[p, 0:7], rS.at[p])
        tot = ST[p, 0]
        for k in range(1, NY):
            tot = tot + ST[p, k]
        return dot(tot, same, precision=lax.Precision.HIGHEST) / NUMBER

    send_sums(0, sums)
    start_ring(0)

    ln128 = iota((32, 128), 1)

    def pack(v):
        fold = v[0:32, 128:256]
        for g in range(1, 4):
            fold = fold + pltpu.roll(v[32 * g : 32 * g + 32, 128:256], 32 * g, 1)
        return jnp.concatenate([v[:, 0:128], fold], axis=0)

    def unpack(m):
        fold = m[128:160]
        rest = [jnp.where(ln128 < 32, fold, 0.0)]
        for g in range(1, 4):
            rest.append(jnp.where(ln128 < 32, pltpu.roll(fold, 128 - 32 * g, 1), 0.0))
        return jnp.concatenate([m[0:128], jnp.concatenate(rest, axis=0)], axis=1)

    def combine(accs):
        rows = accs[0].shape[0]
        q = jnp.bitwise_and(iota((rows, 128), 0), 63)
        ln = iota((rows, 128), 1)
        t0 = jnp.zeros((rows, 128), F32)
        t1 = jnp.zeros((rows, 128), F32)
        for j in range(4):
            b = j // 2
            blk = accs[j % 2][:, 128 * b : 128 * b + 128]
            low = jnp.where(q == 63, 0.0, pltpu.roll(blk, rows - 1, 0))
            mid = pltpu.roll(blk, 128 - 40, 1)
            high = jnp.where(q == 0, 0.0, pltpu.roll(pltpu.roll(blk, 128 - 80, 1), 1, 0))
            v = jnp.where(ln < 40, low + mid + high, 0.0)
            if j:
                v = pltpu.roll(v, 40 * j, 1)
            if j < 3:
                t0 = t0 + v
            else:
                t0 = t0 + jnp.where(ln >= 120, v, 0.0)
                t1 = jnp.where(ln < 32, v, 0.0)
        return jnp.concatenate([t0, t1], axis=1)

    def conv(n, f, mul):
        for e, (ai, t) in enumerate(((0, 0), (2, 3))):
            HBs[n, e] = pack(combine([mul(f, cc, ai, t, t + 1) for cc in range(2)]))

        @pl.when(y > 0)
        def _():
            remote(HBs.at[n, 0], HBr.at[n, 0], sB.at[n, 0], rB.at[n, 0], dev(x, lax.rem(y + 7, 8), z, c)).start()

        @pl.when(y < NY - 1)
        def _():
            remote(HBs.at[n, 1], HBr.at[n, 1], sB.at[n, 1], rB.at[n, 1], dev(x, lax.rem(y + 1, 8), z, c)).start()

        for cc in range(2):
            AC[cc] = mul(f, cc, 1, 0, 4)
            AC[cc, 0:384] += mul(f, cc, 0, 1, 4)
            AC[cc, 128:512] += mul(f, cc, 2, 0, 3)
        BK[...] = combine([AC[0], AC[1]])

    def take_halo(n, e):
        @pl.when(y < NY - 1 if e == 0 else y > 0)
        def _():
            local_wait(HBr.at[n, e], rB.at[n, e])
            px = slice(384, 512) if e == 0 else slice(0, 128)
            BK[px] += unpack(HBr[n, e])

    def mul_cot(f, cc, ai, t0, t1):
        return dot(G[t0:t1].reshape((t1 - t0) * PX, CH), W[f, cc, ai])

    def mul_grad(f, cc, ai, t0, t1):
        return dot(L[t0 * PX : t1 * PX, :], W1[cc, ai])

    def norm_sums(n, a, gain, shift):
        avg, inv = stats[a]
        first = [jnp.zeros((1, 256), F32)] * 2
        second = [jnp.zeros((1, 256), F32)] * 2
        for t in (1, 2, 0, 3):
            if t == 0:
                take_halo(n - 1, 1)
            if t == 3:
                take_halo(n - 1, 0)
            for img in range(2):
                px = slice(t * PX + 64 * img, t * PX + 64 * img + 64)
                v = Hx[a, t, 64 * img : 64 * img + 64, :]
                normed = (v - avg[img : img + 1]) * inv[img : img + 1]
                linear = normed * gain + shift
                s = jax.nn.sigmoid(linear)
                scaled = BK[px, :] * s * (1.0 + linear * (1.0 - s)) * gain
                BK[px, :] = scaled
                first[img] = first[img] + jnp.sum(scaled, axis=0, keepdims=True)
                second[img] = second[img] + jnp.sum(scaled * normed, axis=0, keepdims=True)
        value = jnp.zeros((8, 256), F32)
        for img in range(2):
            value = jnp.where(row8 == img, first[img], value)
            value = jnp.where(row8 == 2 + img, second[img], value)
        send_sums(n, value)
        if n == 1:
            ring_step(0, 1)
            spare_time()
            ring_step(0, 2)
        got = take_sums(n)
        return got[0:2], got[2:4]

    def norm_apply(a, t, img, first, second):
        avg, inv = stats[a]
        px = slice(t * PX + 64 * img, t * PX + 64 * img + 64)
        v = Hx[a, t, 64 * img : 64 * img + 64, :]
        i_ = inv[img : img + 1]
        normed = (v - avg[img : img + 1]) * i_
        return i_ * (BK[px, :] - first[img : img + 1] - normed * second[img : img + 1])

    def spare_time():
        pick = (iota((CH, 256), 0) == iota((CH, 256), 1) + BLK * x) & (iota((CH, 256), 1) < BLK)
        pick = pick.astype(F32).astype(BF16)
        for t in range(NX):
            CC[t] = dot(G[t], pick)

    local_wait(G.at[0:3], rG)
    local_wait(W.at[1, 1 - c], rP.at[1])
    conv(0, 1, mul_cot)
    ring_step(0, 0)
    mean = take_sums(0)
    stats = []
    for a in range(2):
        avg = mean[4 * a : 4 * a + 2]
        inv = lax.rsqrt(mean[4 * a + 2 : 4 * a + 4] - avg * avg + 1e-05)
        stats.append((avg, inv))
    first, second = norm_sums(1, 0, params[0], params[1])
    for img in range(2):
        rest = jnp.zeros((64, 128), F32)
        for t in range(NX):
            v = norm_apply(0, t, img, first, second)
            Gh[x, t * PX + 64 * img : t * PX + 64 * img + 64, :] = v[:, 0:128].astype(BF16)
            rest = rest + (pltpu.roll(v[:, 128:256], 32 * t, 1) if t else v[:, 128:256])
        Gh[x, 512 + 64 * img : 576 + 64 * img, :] = rest.astype(BF16)
    for k in range(1, NX):
        remote(Gh.at[x], Gh.at[x], sGh, rGh, dev(lax.rem(x + k, NX), y, z, c)).start()
    ring_step(0, 3)
    local_wait(W.at[0, 1 - c], rP.at[0])
    for k in range(NX):
        W1[:, :, 128 * k : 128 * k + 128, :] = W[0, :, :, BLK * k : BLK * k + 128, :]
        W1[:, :, 512 + 32 * k : 544 + 32 * k, :] = W[0, :, :, BLK * k + 128 : BLK * k + BLK, :]
    local_wait(Gh.at[0:3], rGh)
    lane = iota((PX, 128), 1)
    rests = [Gh[k, 512:640, :].astype(F32) for k in range(NX)]
    for k in range(NX):
        L[:, 128 * k : 128 * k + 128] = Gh[k, 0:512, :]
    for t in range(NX):
        v = jnp.zeros((PX, 128), F32)
        for k in range(NX):
            w = pltpu.roll(rests[k], (32 * (k - t)) % 128, 1) if k != t else rests[k]
            v = jnp.where((lane >= 32 * k) & (lane < 32 * k + 32), w, v)
        L[t * PX : t * PX + PX, 512:640] = v.astype(BF16)

    conv(1, 0, mul_grad)
    first, second = norm_sums(2, 1, params[2], params[3])
    for t in range(NX):
        v = jnp.concatenate([norm_apply(1, t, img, first, second) for img in range(2)], axis=0)
        Os[t] = pack(CC[t] + v).astype(BF16)
    for k in range(1, NX):
        t = lax.rem(x + k, NX)
        remote(Os.at[t], Oc.at[x], sO, rO, dev(t, y, z, c)).start()
    Oc[x] = Os[x]

    for f in (1, 0):
        local_wait(RA.at[f, 0:7], sA.at[f])

        @pl.when(jnp.logical_not(mine[f]))
        def _():
            local_wait(RA.at[f, 0], sA0.at[f])

        local_wait(W.at[f, 0, :, 0:560, :], sR.at[f])
        local_wait(W.at[f, 0], sP.at[f])
    local_wait(G.at[0:3], sG)
    local_wait(Gh.at[0:3], sGh)
    local_wait(Hc.at[0:3], sH)
    for p in range(3):
        local_wait(ST.at[p, 0:7], sS.at[p])
    for n in range(2):
        @pl.when(y > 0)
        def _():
            local_wait(HBs.at[n, 0], sB.at[n, 0])

        @pl.when(y < NY - 1)
        def _():
            local_wait(HBs.at[n, 1], sB.at[n, 1])

    local_wait(Oc.at[0:3], rO)
    local_wait(Oc.at[0:3], sO)
    out[...] = jnp.concatenate(
        [unpack(Oc[k].astype(F32))[:, 0:BLK] for k in range(NX)], axis=1
    ).astype(BF16)


def body(latent, hidden, cotangent, filter_one, filter_two, gain_one, shift_one, gain_two, shift_two):
    filters = [jnp.transpose(a, (0, 2, 1)) for a in (filter_one, filter_two)]
    rows = [a.reshape(PX, CH) for a in (cotangent, hidden, latent)]
    params = (gain_two, shift_two, gain_one, shift_one)
    vmem = pl.BlockSpec(memory_space=pltpu.VMEM)
    anywhere = pl.BlockSpec(memory_space=pl.ANY)
    dma = pltpu.SemaphoreType.DMA
    out = pl.pallas_call(
        kernel,
        out_shape=jax.ShapeDtypeStruct((PX, CH), BF16),
        in_specs=[anywhere] * 9,
        out_specs=vmem,
        scratch_shapes=[
            pltpu.VMEM((2, 9, 20, 40), BF16),
            [pltpu.VMEM((CH,), F32)] * 4,
            pltpu.VMEM((2, PX, CH), BF16),
            pltpu.VMEM((2, 24, 384), BF16),
            pltpu.VMEM((2, 2, 3, CH, 256), BF16),
            pltpu.VMEM((2, 3, CH, 256), BF16),
            pltpu.VMEM((2, 8, 24, 384), BF16),
            pltpu.VMEM((NX, PX, CH), BF16),
            pltpu.VMEM((NX, 640, 128), BF16),
            pltpu.VMEM((NX * PX, CH), BF16),
            pltpu.VMEM((NX, PX, 384), BF16),
            pltpu.VMEM((NX, PX, 384), BF16),
            pltpu.VMEM((2, NX, PX, 256), F32),
            pltpu.VMEM((3, 8, 256), F32),
            pltpu.VMEM((3, NY, 8, 256), F32),
            pltpu.VMEM((2, 2, BLK, 128), F32),
            pltpu.VMEM((2, 2, BLK, 128), F32),
            pltpu.VMEM((2, NX * PX, 256), F32),
            pltpu.VMEM((NX * PX, 256), F32),
            pltpu.VMEM((NX, BLK, 128), BF16),
            pltpu.VMEM((NX, BLK, 128), BF16),
            pltpu.VMEM((NX, PX, 256), F32),
            dma((2,)), dma((4,)), dma((2,)), dma,
            dma((2,)), dma((2,)), dma((2,)),
            dma((2,)), dma((2, 2, 4, 3)),
            dma((2,)), dma((2,)),
            dma, dma, dma, dma, dma, dma,
            dma((3,)), dma((3,)),
            dma((2, 2)), dma((2, 2)),
            dma, dma,
        ],
        compiler_params=pltpu.CompilerParams(
            collective_id=0, has_side_effects=True, vmem_limit_bytes=62 * 1024 * 1024
        ),
        name="block_backward",
    )(*filters, *rows, *params)
    return out.reshape(latent.shape)


def solution(mesh):
    in_specs = (
        P("dp", "rows", None, None),
        P("dp", "rows", None, None),
        P("dp", "rows", None, None),
        P(None, "dp", "rows"),
        P(None, "dp", "rows"),
        P(),
        P(),
        P(),
        P(),
    )
    out_specs = P("dp", "rows", None, None)
    return jax.shard_map(body, mesh=mesh, in_specs=in_specs, out_specs=out_specs, check_vma=False)
```

```python
import jax
import jax.numpy as jnp
from jax import lax
from jax.experimental import pallas as pl
from jax.experimental.pallas import tpu as pltpu
from jax.sharding import PartitionSpec as P

MESH = pl.DeviceIdType.MESH
F32 = jnp.float32
BF16 = jnp.bfloat16
NX, NY, NZ = 4, 8, 8
CH = 640
BLK = 160
PX = 128
NUMBER = 32 * 64 * 40


def dev(x, y, z, c):
    return (2 * z + c, 4 * y + x)


def iota(shape, dim):
    return lax.broadcasted_iota(jnp.int32, shape, dim)


def dot(a, b, **kw):
    return jnp.dot(a, b, preferred_element_type=F32, **kw)


def group_of(lane):
    g = jnp.zeros_like(lane)
    for edge in (40, 80, 120, 160):
        g = g + (lane >= edge).astype(jnp.int32)
    return g


def kernel(
    f1, f2, cot, hid, lat, g2, s2, g1, s1, out,
    FV, PV, HV, WB, W, W1, RA, G, Gh, L, Hs, Hc, Hx, SS, ST, Hb, HxB, PB, KB, HBs, HBr, AC, BK, Os, Oc, CC,
    lF, lP, lH, lC, sA, sA0, rA, sR, rR, sP, rP, sG, rG, sGh, rGh, sH, rH, sS, rS, sB, rB, sO, rO, sN, rN,
):
    dp = lax.axis_index("dp")
    rr = lax.axis_index("rows")
    c = lax.rem(dp, 2)
    z = lax.div(dp, 2)
    x = lax.rem(rr, NX)
    y = lax.div(rr, NX)
    X = lax.div(z, 2)
    mine_y = x == X
    mine_z = jnp.logical_and(x == X, y == z)

    def remote(src, dst, ss, rs, target):
        return pltpu.make_async_remote_copy(
            src_ref=src, dst_ref=dst, send_sem=ss, recv_sem=rs, device_id=target,
            device_id_type=MESH,
        )

    def local_wait(ref, sem):
        pltpu.make_async_copy(ref, ref, sem).wait()

    Hb[...] = jnp.zeros_like(Hb)
    bar = pltpu.get_barrier_semaphore()

    def here(target):
        pl.semaphore_signal(bar, inc=1, device_id=target, device_id_type=MESH)

    for b in range(2):
        zs = 2 * x + lax.rem(z + b, 2)
        for k in range(NX):
            xs = lax.rem(x + k, NX)
            if b == 0 and k == 0:
                @pl.when(jnp.logical_not(mine_y))
                def _():
                    here(dev(xs, y, zs, c))

                @pl.when(jnp.logical_not(mine_z))
                def _():
                    here(dev(xs, z, zs, c))
            else:
                here(dev(xs, y, zs, c))
                here(dev(xs, z, zs, c))
    for k in range(1, NX):
        here(dev(lax.rem(x + k, NX), y, z, c))
    for k in range(1, NY):
        here(dev(x, lax.rem(y + k, NY), z, c))
    for k in (1, 2, NZ - 2, NZ - 1):
        here(dev(x, y, lax.rem(z + k, NZ), c))
    here(dev(x, y, z, 1 - c))

    loads = [pltpu.make_async_copy(r, FV.at[f], lF.at[f]) for f, r in enumerate((f1, f2))]
    loads += [pltpu.make_async_copy(r, HV.at[a], lH.at[a]) for a, r in enumerate((hid, lat))]
    loads += [
        pltpu.make_async_copy(r, PV[a], lP.at[a]) for a, r in enumerate((g2, s2, g1, s1))
    ]
    own_cot = pltpu.make_async_copy(cot, G.at[x], lC)
    for load in loads[1::-1] + loads[2:]:
        load.start()
    own_cot.start()
    WB[...] = jnp.zeros_like(WB)
    for f in (1, 0):
        loads[f].wait()
        for a in range(3):
            taps = [FV[f, 3 * a + b].astype(F32) for b in range(3)]
            WB[f, 0:20, 128 * a : 128 * a + 128] = jnp.concatenate(
                taps + [jnp.zeros((20, 8), F32)], axis=1
            ).astype(BF16)
    for a in range(2):
        loads[2 + a].wait()
    v = [HV[a].astype(F32) for a in range(2)]
    for k in range(NX):
        Hs[k] = jnp.concatenate(
            [v[a][:, BLK * k : BLK * k + BLK] for a in range(2)] + [jnp.zeros((PX, 64), F32)],
            axis=1,
        ).astype(BF16)
    params = []
    for a in range(4):
        loads[4 + a].wait()
        whole = PV[a][...].reshape(1, CH)
        p = jnp.zeros((1, BLK), F32)
        for k in range(NX):
            p = jnp.where(x == k, whole[:, BLK * k : BLK * k + BLK], p)
        params.append(jnp.concatenate([p, jnp.zeros((1, 256 - BLK), F32)], axis=1))
    own_cot.wait()

    pl.semaphore_wait(
        bar, 31 - mine_y.astype(jnp.int32) - mine_z.astype(jnp.int32)
    )

    slot = lax.rem(z, 2) * 4 + x
    along_y = {f: lax.rem(f + c, 2) == 1 for f in (1, 0)}
    mine = {f: jnp.where(along_y[f], mine_y.astype(jnp.int32), mine_z.astype(jnp.int32)) == 1 for f in (1, 0)}
    place = {f: jnp.where(along_y[f], y, z) for f in (1, 0)}

    def first_stage(f):
        for k in range(8):
            y_ = jnp.where(along_y[f], y, lax.rem(y + k, NY))
            z_ = jnp.where(along_y[f], lax.rem(z + k, NZ), y)
            target = dev(X, y_, z_, c)
            if k == 0:
                @pl.when(mine[f])
                def _():
                    pltpu.make_async_copy(WB.at[f], RA.at[f, slot], rA.at[f]).start()

                @pl.when(jnp.logical_not(mine[f]))
                def _():
                    remote(WB.at[f], RA.at[f, slot], sA0.at[f], rA.at[f], target).start()
            else:
                remote(WB.at[f], RA.at[f, slot], sA.at[f], rA.at[f], target).start()

    first_stage(1)
    for k in range(1, NX):
        t = lax.rem(x + k, NX)
        remote(Hs.at[t], Hc.at[x], sH, rH, dev(t, y, z, c)).start()
    for k in range(1, NX):
        t = lax.rem(x + k, NX)
        remote(G.at[x], G.at[x], sG, rG, dev(t, y, z, c)).start()
    Hc[x] = Hs[x]

    def region(f, cc, a, o):
        return W.at[f, cc, a, pl.ds(pl.multiple_of(80 * o, 16), 80), :]

    om = iota((80, 96), 0)
    mm_ = iota((80, 96), 1)
    hit = jnp.zeros((80, 96), jnp.bool_)
    for k in range(4):
        hit = jnp.logical_or(
            hit,
            jnp.logical_and(
                jnp.logical_and(mm_ >= 24 * k, mm_ < 24 * k + 20), om == mm_ - 4 * k
            ),
        )
    join = hit.astype(F32).astype(BF16)

    def at(f, p):
        return dev(x, jnp.where(along_y[f], p, y), jnp.where(along_y[f], z, p), c)

    def ring(f, way, step, a, hops):
        p = place[f]
        sign = 1 if way == 0 else -1
        o = lax.rem(p - sign * (step + 1 - hops) + 8, 8)
        return remote(
            region(f, c, a, o), region(f, c, a, o), sR.at[f], rR.at[f, way, step, a],
            at(f, lax.rem(p + sign * hops + 8, 8)),
        )

    def share(f, a, o):
        o = lax.rem(o + 8, 8)
        remote(
            region(f, c, a, o), region(f, c, a, o), sP.at[f], rP.at[f], dev(x, y, z, 1 - c)
        ).start()

    def start_ring(f):
        local_wait(RA.at[f], rA.at[f])
        for b in range(2):
            piece = dot(join, RA[f, 4 * b : 4 * b + 4].reshape(96, 384)).astype(BF16)
            for a in range(3):
                W[
                    f, c, a, pl.ds(pl.multiple_of(80 * place[f], 16), 80),
                    128 * b : 128 * b + 128,
                ] = piece[:, 128 * a : 128 * a + 128]
        for hops in (2, 1):
            for a in range(3):
                for way in range(2):
                    ring(f, way, hops - 1, a, hops).start()
        for a in range(3):
            share(f, a, place[f])

    def ring_step(f, s):
        step = (1, 0, 2, 3)[s]
        for a in range(3):
            for way in range(2):
                if step == 3 and way != a % 2:
                    continue
                ring(f, way, step, a, 0).wait_recv()
                if step == 1:
                    ring(f, way, 2, a, 1).start()
                    if way == a % 2:
                        ring(f, way, 3, a, 2).start()
                share(f, a, place[f] - (step + 1) * (1 if way == 0 else -1))

    start_ring(1)
    first_stage(0)
    for s in range(2):
        ring_step(1, s)

    row8 = iota((8, 256), 0)
    local_wait(Hc.at[0:3], rH)
    @pl.when(y < NY - 1)
    def _():
        remote(Hc.at[3], Hb.at[0], sN.at[0], rN.at[0], dev(x, lax.rem(y + 1, 8), z, c)).start()

    @pl.when(y > 0)
    def _():
        remote(Hc.at[0], Hb.at[1], sN.at[1], rN.at[1], dev(x, lax.rem(y + 7, 8), z, c)).start()

    zero = jnp.zeros((64, 256 - BLK), F32)
    sums = jnp.zeros((8, 256), F32)
    for img in range(2):
        tot = [jnp.zeros((1, 256), F32)] * 2
        sq = [jnp.zeros((1, 256), F32)] * 2
        for t in range(NX):
            both = Hc[t, 64 * img : 64 * img + 64, :].astype(F32)
            for a in range(2):
                v = jnp.concatenate([both[:, BLK * a : BLK * a + BLK], zero], axis=1)
                Hx[a, t, 64 * img : 64 * img + 64, :] = v
                tot[a] = tot[a] + jnp.sum(v, axis=0, keepdims=True)
                sq[a] = sq[a] + jnp.sum(v * v, axis=0, keepdims=True)
        for a in range(2):
            sums = jnp.where(row8 == 4 * a + img, tot[a], sums)
            sums = jnp.where(row8 == 4 * a + 2 + img, sq[a], sums)

    def send_sums(p, value):
        SS[p] = value
        ST[p, y] = value
        for k in range(1, NY):
            remote(
                SS.at[p], ST.at[p, y], sS.at[p], rS.at[p], dev(x, lax.rem(y + k, NY), z, c)
            ).start()

    gi = group_of(iota((256, 256), 0))
    gj = group_of(iota((256, 256), 1))
    same = jnp.logical_and(gi == gj, gi < 4).astype(F32)

    def take_sums(p):
        local_wait(ST.at[p, 0:7], rS.at[p])
        tot = ST[p, 0]
        for k in range(1, NY):
            tot = tot + ST[p, k]
        return dot(tot, same, precision=lax.Precision.HIGHEST) / NUMBER

    send_sums(0, sums)
    for s in range(2, 4):
        ring_step(1, s)
    start_ring(0)

    ln128 = iota((32, 128), 1)

    def pack(v):
        fold = v[0:32, 128:256]
        for g in range(1, 4):
            fold = fold + pltpu.roll(v[32 * g : 32 * g + 32, 128:256], 32 * g, 1)
        return jnp.concatenate([v[:, 0:128], fold], axis=0)

    def unpack(m):
        fold = m[128:160]
        rest = [jnp.where(ln128 < 32, fold, 0.0)]
        for g in range(1, 4):
            rest.append(jnp.where(ln128 < 32, pltpu.roll(fold, 128 - 32 * g, 1), 0.0))
        return jnp.concatenate([m[0:128], jnp.concatenate(rest, axis=0)], axis=1)

    def combine(accs):
        rows = accs[0].shape[0]
        q = jnp.bitwise_and(iota((rows, 128), 0), 63)
        ln = iota((rows, 128), 1)
        t0 = jnp.zeros((rows, 128), F32)
        t1 = jnp.zeros((rows, 128), F32)
        for j in range(4):
            b = j // 2
            blk = accs[j % 2][:, 128 * b : 128 * b + 128]
            low = jnp.where(q == 63, 0.0, pltpu.roll(blk, rows - 1, 0))
            mid = pltpu.roll(blk, 128 - 40, 1)
            high = jnp.where(q == 0, 0.0, pltpu.roll(pltpu.roll(blk, 128 - 80, 1), 1, 0))
            v = jnp.where(ln < 40, low + mid + high, 0.0)
            if j:
                v = pltpu.roll(v, 40 * j, 1)
            if j < 3:
                t0 = t0 + v
            else:
                t0 = t0 + jnp.where(ln >= 120, v, 0.0)
                t1 = jnp.where(ln < 32, v, 0.0)
        return jnp.concatenate([t0, t1], axis=1)

    def conv(n, f, mul):
        for e, (ai, t) in enumerate(((0, 0), (2, 3))):
            PB[e] = combine([mul(f, cc, ai, t, t + 1) for cc in range(2)])
            HBs[n, e] = pack(PB[e])

        @pl.when(y > 0)
        def _():
            remote(HBs.at[n, 0], HBr.at[n, 0], sB.at[n, 0], rB.at[n, 0], dev(x, lax.rem(y + 7, 8), z, c)).start()

        @pl.when(y < NY - 1)
        def _():
            remote(HBs.at[n, 1], HBr.at[n, 1], sB.at[n, 1], rB.at[n, 1], dev(x, lax.rem(y + 1, 8), z, c)).start()

        for cc in range(2):
            AC[cc] = mul(f, cc, 1, 0, 4)
            AC[cc, 0:384] += mul(f, cc, 0, 1, 4)
            AC[cc, 128:512] += mul(f, cc, 2, 0, 3)
        BK[...] = combine([AC[0], AC[1]])

    def take_halo(n, e):
        @pl.when(y < NY - 1 if e == 0 else y > 0)
        def _():
            local_wait(HBr.at[n, e], rB.at[n, e])
            px = slice(384, 512) if e == 0 else slice(0, 128)
            BK[px] += unpack(HBr[n, e]) * KB[1 - e]

    def mul_cot(f, cc, ai, t0, t1):
        return dot(G[t0:t1].reshape((t1 - t0) * PX, CH), W[f, cc, ai])

    def mul_grad(f, cc, ai, t0, t1):
        return dot(L[t0 * PX : t1 * PX, :], W1[cc, ai])

    def norm_sums(n, a, gain, shift):
        avg, inv = stats[a]
        first = [jnp.zeros((1, 256), F32)] * 2
        second = [jnp.zeros((1, 256), F32)] * 2
        for t in (0, 1, 2, 3, 4, 5):
            for img in range(2):
                q = slice(64 * img, 64 * img + 64)
                px = slice(t * PX + 64 * img, t * PX + 64 * img + 64)
                v = Hx[a, t, q, :] if t < 4 else HxB[a, t - 4, q, :]
                normed = (v - avg[img : img + 1]) * inv[img : img + 1]
                linear = normed * gain + shift
                s = jax.nn.sigmoid(linear)
                slope = s * (1.0 + linear * (1.0 - s)) * gain
                if t < 4:
                    scaled = BK[px, :] * slope
                    BK[px, :] = scaled
                    if t in (0, 3):
                        KB[t // 3, q, :] = slope
                else:
                    scaled = jnp.where(y > 0 if t == 4 else y < NY - 1, PB[t - 4, q, :] * slope, 0.0)
                first[img] = first[img] + jnp.sum(scaled, axis=0, keepdims=True)
                second[img] = second[img] + jnp.sum(scaled * normed, axis=0, keepdims=True)
        value = jnp.zeros((8, 256), F32)
        for img in range(2):
            value = jnp.where(row8 == img, first[img], value)
            value = jnp.where(row8 == 2 + img, second[img], value)
        send_sums(n, value)
        if n == 1:
            spare_time()
            ring_step(0, 0)
        take_halo(n - 1, 1)
        take_halo(n - 1, 0)
        got = take_sums(n)
        return got[0:2], got[2:4]

    def norm_apply(a, t, img, first, second):
        avg, inv = stats[a]
        px = slice(t * PX + 64 * img, t * PX + 64 * img + 64)
        v = Hx[a, t, 64 * img : 64 * img + 64, :]
        i_ = inv[img : img + 1]
        normed = (v - avg[img : img + 1]) * i_
        return i_ * (BK[px, :] - first[img : img + 1] - normed * second[img : img + 1])

    def spare_time():
        pick = (iota((CH, 256), 0) == iota((CH, 256), 1) + BLK * x) & (iota((CH, 256), 1) < BLK)
        pick = pick.astype(F32).astype(BF16)
        for t in range(NX):
            CC[t] = dot(G[t], pick)

    local_wait(G.at[0:3], rG)
    local_wait(W.at[1, 1 - c], rP.at[1])
    conv(0, 1, mul_cot)
    mean = take_sums(0)
    stats = []
    for a in range(2):
        avg = mean[4 * a : 4 * a + 2]
        inv = lax.rsqrt(mean[4 * a + 2 : 4 * a + 4] - avg * avg + 1e-05)
        stats.append((avg, inv))
    @pl.when(y > 0)
    def _():
        local_wait(Hb.at[0], rN.at[0])

    @pl.when(y < NY - 1)
    def _():
        local_wait(Hb.at[1], rN.at[1])

    for e in range(2):
        both = Hb[e].astype(F32)
        for a in range(2):
            HxB[a, e] = jnp.concatenate(
                [both[:, BLK * a : BLK * a + BLK], jnp.zeros((PX, 256 - BLK), F32)], axis=1
            )
    first, second = norm_sums(1, 0, params[0], params[1])
    for img in range(2):
        rest = jnp.zeros((64, 128), F32)
        for t in range(NX):
            v = norm_apply(0, t, img, first, second)
            Gh[x, t * PX + 64 * img : t * PX + 64 * img + 64, :] = v[:, 0:128].astype(BF16)
            rest = rest + (pltpu.roll(v[:, 128:256], 32 * t, 1) if t else v[:, 128:256])
        Gh[x, 512 + 64 * img : 576 + 64 * img, :] = rest.astype(BF16)
    for k in range(1, NX):
        remote(Gh.at[x], Gh.at[x], sGh, rGh, dev(lax.rem(x + k, NX), y, z, c)).start()
    for s in range(1, 4):
        ring_step(0, s)
    local_wait(W.at[0, 1 - c], rP.at[0])
    for k in range(NX):
        W1[:, :, 128 * k : 128 * k + 128, :] = W[0, :, :, BLK * k : BLK * k + 128, :]
        W1[:, :, 512 + 32 * k : 544 + 32 * k, :] = W[0, :, :, BLK * k + 128 : BLK * k + BLK, :]
    local_wait(Gh.at[0:3], rGh)
    lane = iota((PX, 128), 1)
    rests = [Gh[k, 512:640, :].astype(F32) for k in range(NX)]
    for k in range(NX):
        L[:, 128 * k : 128 * k + 128] = Gh[k, 0:512, :]
    for t in range(NX):
        v = jnp.zeros((PX, 128), F32)
        for k in range(NX):
            w = pltpu.roll(rests[k], (32 * (k - t)) % 128, 1) if k != t else rests[k]
            v = jnp.where((lane >= 32 * k) & (lane < 32 * k + 32), w, v)
        L[t * PX : t * PX + PX, 512:640] = v.astype(BF16)

    conv(1, 0, mul_grad)
    first, second = norm_sums(2, 1, params[2], params[3])
    for t in range(NX):
        v = jnp.concatenate([norm_apply(1, t, img, first, second) for img in range(2)], axis=0)
        Os[t] = pack(CC[t] + v).astype(BF16)
    for k in range(1, NX):
        t = lax.rem(x + k, NX)
        remote(Os.at[t], Oc.at[x], sO, rO, dev(t, y, z, c)).start()
    Oc[x] = Os[x]

    for f in (1, 0):
        local_wait(RA.at[f, 0:7], sA.at[f])

        @pl.when(jnp.logical_not(mine[f]))
        def _():
            local_wait(RA.at[f, 0], sA0.at[f])

        local_wait(W.at[f, 0, :, 0:560, :], sR.at[f])
        local_wait(W.at[f, 0], sP.at[f])
    local_wait(G.at[0:3], sG)
    local_wait(Gh.at[0:3], sGh)
    local_wait(Hc.at[0:3], sH)

    @pl.when(y < NY - 1)
    def _():
        local_wait(Hc.at[3], sN.at[0])

    @pl.when(y > 0)
    def _():
        local_wait(Hc.at[0], sN.at[1])

    for p in range(3):
        local_wait(ST.at[p, 0:7], sS.at[p])
    for n in range(2):
        @pl.when(y > 0)
        def _():
            local_wait(HBs.at[n, 0], sB.at[n, 0])

        @pl.when(y < NY - 1)
        def _():
            local_wait(HBs.at[n, 1], sB.at[n, 1])

    local_wait(Oc.at[0:3], rO)
    local_wait(Oc.at[0:3], sO)
    out[...] = jnp.concatenate(
        [unpack(Oc[k].astype(F32))[:, 0:BLK] for k in range(NX)], axis=1
    ).astype(BF16)


def body(latent, hidden, cotangent, filter_one, filter_two, gain_one, shift_one, gain_two, shift_two):
    filters = [jnp.transpose(a, (0, 2, 1)) for a in (filter_one, filter_two)]
    rows = [a.reshape(PX, CH) for a in (cotangent, hidden, latent)]
    params = (gain_two, shift_two, gain_one, shift_one)
    vmem = pl.BlockSpec(memory_space=pltpu.VMEM)
    anywhere = pl.BlockSpec(memory_space=pl.ANY)
    dma = pltpu.SemaphoreType.DMA
    out = pl.pallas_call(
        kernel,
        out_shape=jax.ShapeDtypeStruct((PX, CH), BF16),
        in_specs=[anywhere] * 9,
        out_specs=vmem,
        scratch_shapes=[
            pltpu.VMEM((2, 9, 20, 40), BF16),
            [pltpu.VMEM((CH,), F32)] * 4,
            pltpu.VMEM((2, PX, CH), BF16),
            pltpu.VMEM((2, 24, 384), BF16),
            pltpu.VMEM((2, 2, 3, CH, 256), BF16),
            pltpu.VMEM((2, 3, CH, 256), BF16),
            pltpu.VMEM((2, 8, 24, 384), BF16),
            pltpu.VMEM((NX, PX, CH), BF16),
            pltpu.VMEM((NX, 640, 128), BF16),
            pltpu.VMEM((NX * PX, CH), BF16),
            pltpu.VMEM((NX, PX, 384), BF16),
            pltpu.VMEM((NX, PX, 384), BF16),
            pltpu.VMEM((2, NX, PX, 256), F32),
            pltpu.VMEM((3, 8, 256), F32),
            pltpu.VMEM((3, NY, 8, 256), F32),
            pltpu.VMEM((2, PX, 384), BF16),
            pltpu.VMEM((2, 2, PX, 256), F32),
            pltpu.VMEM((2, PX, 256), F32),
            pltpu.VMEM((2, PX, 256), F32),
            pltpu.VMEM((2, 2, BLK, 128), F32),
            pltpu.VMEM((2, 2, BLK, 128), F32),
            pltpu.VMEM((2, NX * PX, 256), F32),
            pltpu.VMEM((NX * PX, 256), F32),
            pltpu.VMEM((NX, BLK, 128), BF16),
            pltpu.VMEM((NX, BLK, 128), BF16),
            pltpu.VMEM((NX, PX, 256), F32),
            dma((2,)), dma((4,)), dma((2,)), dma,
            dma((2,)), dma((2,)), dma((2,)),
            dma((2,)), dma((2, 2, 4, 3)),
            dma((2,)), dma((2,)),
            dma, dma, dma, dma, dma, dma,
            dma((3,)), dma((3,)),
            dma((2, 2)), dma((2, 2)),
            dma, dma,
            dma((2,)), dma((2,)),
        ],
        compiler_params=pltpu.CompilerParams(
            collective_id=0, has_side_effects=True, vmem_limit_bytes=62 * 1024 * 1024
        ),
        name="block_backward",
    )(*filters, *rows, *params)
    return out.reshape(latent.shape)


def solution(mesh):
    in_specs = (
        P("dp", "rows", None, None),
        P("dp", "rows", None, None),
        P("dp", "rows", None, None),
        P(None, "dp", "rows"),
        P(None, "dp", "rows"),
        P(),
        P(),
        P(),
        P(),
    )
    out_specs = P("dp", "rows", None, None)
    return jax.shard_map(body, mesh=mesh, in_specs=in_specs, out_specs=out_specs, check_vma=False)
```

```python
import jax
import jax.numpy as jnp
from jax import lax
from jax.experimental import pallas as pl
from jax.experimental.pallas import tpu as pltpu
from jax.sharding import PartitionSpec as P

MESH = pl.DeviceIdType.MESH
F32 = jnp.float32
BF16 = jnp.bfloat16
NX, NY, NZ = 4, 8, 8
CH = 640
BLK = 160
PX = 128
NUMBER = 32 * 64 * 40


def dev(x, y, z, c):
    return (2 * z + c, 4 * y + x)


def iota(shape, dim):
    return lax.broadcasted_iota(jnp.int32, shape, dim)


def dot(a, b, **kw):
    return jnp.dot(a, b, preferred_element_type=F32, **kw)


def group_of(lane):
    g = jnp.zeros_like(lane)
    for edge in (40, 80, 120, 160):
        g = g + (lane >= edge).astype(jnp.int32)
    return g


def kernel(
    f1, f2, cot, hid, lat, g2, s2, g1, s1, out,
    FV, PV, HV, WB, W, W1, RA, G, Gh, L, Hs, Hc, Hx, SS, ST, Hb, HxB, NB, SB, PB, KB, HBs, HBr, AC, BK, Os, Oc, CC,
    lF, lP, lH, lC, sA, sA0, rA, sR, rR, sP, rP, sG, rG, sGh, rGh, sH, rH, sS, rS, sB, rB, sO, rO, sN, rN,
):
    dp = lax.axis_index("dp")
    rr = lax.axis_index("rows")
    c = lax.rem(dp, 2)
    z = lax.div(dp, 2)
    x = lax.rem(rr, NX)
    y = lax.div(rr, NX)
    X = lax.div(z, 2)
    mine_y = x == X
    mine_z = jnp.logical_and(x == X, y == z)

    def remote(src, dst, ss, rs, target):
        return pltpu.make_async_remote_copy(
            src_ref=src, dst_ref=dst, send_sem=ss, recv_sem=rs, device_id=target,
            device_id_type=MESH,
        )

    def local_wait(ref, sem):
        pltpu.make_async_copy(ref, ref, sem).wait()

    Hb[...] = jnp.zeros_like(Hb)
    bar = pltpu.get_barrier_semaphore()

    def here(target):
        pl.semaphore_signal(bar, inc=1, device_id=target, device_id_type=MESH)

    for b in range(2):
        zs = 2 * x + lax.rem(z + b, 2)
        for k in range(NX):
            xs = lax.rem(x + k, NX)
            if b == 0 and k == 0:
                @pl.when(jnp.logical_not(mine_y))
                def _():
                    here(dev(xs, y, zs, c))

                @pl.when(jnp.logical_not(mine_z))
                def _():
                    here(dev(xs, z, zs, c))
            else:
                here(dev(xs, y, zs, c))
                here(dev(xs, z, zs, c))
    for k in range(1, NX):
        here(dev(lax.rem(x + k, NX), y, z, c))
    for k in range(1, NY):
        here(dev(x, lax.rem(y + k, NY), z, c))
    for k in (1, 2, NZ - 2, NZ - 1):
        here(dev(x, y, lax.rem(z + k, NZ), c))
    here(dev(x, y, z, 1 - c))

    loads = [pltpu.make_async_copy(r, FV.at[f], lF.at[f]) for f, r in enumerate((f1, f2))]
    loads += [pltpu.make_async_copy(r, HV.at[a], lH.at[a]) for a, r in enumerate((hid, lat))]
    loads += [
        pltpu.make_async_copy(r, PV[a], lP.at[a]) for a, r in enumerate((g2, s2, g1, s1))
    ]
    own_cot = pltpu.make_async_copy(cot, G.at[x], lC)
    for load in loads[1::-1] + loads[2:]:
        load.start()
    own_cot.start()
    WB[...] = jnp.zeros_like(WB)

    def own_block(f):
        loads[f].wait()
        for a in range(3):
            taps = [FV[f, 3 * a + b].astype(F32) for b in range(3)]
            WB[f, 0:20, 128 * a : 128 * a + 128] = jnp.concatenate(
                taps + [jnp.zeros((20, 8), F32)], axis=1
            ).astype(BF16)

    own_block(1)

    pl.semaphore_wait(
        bar, 31 - mine_y.astype(jnp.int32) - mine_z.astype(jnp.int32)
    )

    slot = lax.rem(z, 2) * 4 + x
    along_y = {f: lax.rem(f + c, 2) == 1 for f in (1, 0)}
    mine = {f: jnp.where(along_y[f], mine_y.astype(jnp.int32), mine_z.astype(jnp.int32)) == 1 for f in (1, 0)}
    place = {f: jnp.where(along_y[f], y, z) for f in (1, 0)}

    def first_stage(f):
        for k in range(8):
            y_ = jnp.where(along_y[f], y, lax.rem(y + k, NY))
            z_ = jnp.where(along_y[f], lax.rem(z + k, NZ), y)
            target = dev(X, y_, z_, c)
            if k == 0:
                @pl.when(mine[f])
                def _():
                    pltpu.make_async_copy(WB.at[f], RA.at[f, slot], rA.at[f]).start()

                @pl.when(jnp.logical_not(mine[f]))
                def _():
                    remote(WB.at[f], RA.at[f, slot], sA0.at[f], rA.at[f], target).start()
            else:
                remote(WB.at[f], RA.at[f, slot], sA.at[f], rA.at[f], target).start()

    first_stage(1)
    for a in range(2):
        loads[2 + a].wait()
    v = [HV[a].astype(F32) for a in range(2)]
    for k in range(NX):
        Hs[k] = jnp.concatenate(
            [v[a][:, BLK * k : BLK * k + BLK] for a in range(2)] + [jnp.zeros((PX, 64), F32)],
            axis=1,
        ).astype(BF16)
    own_cot.wait()
    for k in range(1, NX):
        t = lax.rem(x + k, NX)
        remote(Hs.at[t], Hc.at[x], sH, rH, dev(t, y, z, c)).start()
    for k in range(1, NX):
        t = lax.rem(x + k, NX)
        remote(G.at[x], G.at[x], sG, rG, dev(t, y, z, c)).start()
    Hc[x] = Hs[x]
    own_block(0)
    params = []
    for a in range(4):
        loads[4 + a].wait()
        whole = PV[a][...].reshape(1, CH)
        p = jnp.zeros((1, BLK), F32)
        for k in range(NX):
            p = jnp.where(x == k, whole[:, BLK * k : BLK * k + BLK], p)
        params.append(jnp.concatenate([p, jnp.zeros((1, 256 - BLK), F32)], axis=1))

    def region(f, cc, a, o):
        return W.at[f, cc, a, pl.ds(pl.multiple_of(80 * o, 16), 80), :]

    om = iota((80, 96), 0)
    mm_ = iota((80, 96), 1)
    hit = jnp.zeros((80, 96), jnp.bool_)
    for k in range(4):
        hit = jnp.logical_or(
            hit,
            jnp.logical_and(
                jnp.logical_and(mm_ >= 24 * k, mm_ < 24 * k + 20), om == mm_ - 4 * k
            ),
        )
    join = hit.astype(F32).astype(BF16)

    def at(f, p):
        return dev(x, jnp.where(along_y[f], p, y), jnp.where(along_y[f], z, p), c)

    def ring(f, way, step, a, hops):
        p = place[f]
        sign = 1 if way == 0 else -1
        o = lax.rem(p - sign * (step + 1 - hops) + 8, 8)
        return remote(
            region(f, c, a, o), region(f, c, a, o), sR.at[f], rR.at[f, way, step, a],
            at(f, lax.rem(p + sign * hops + 8, 8)),
        )

    def share(f, a, o):
        o = lax.rem(o + 8, 8)
        remote(
            region(f, c, a, o), region(f, c, a, o), sP.at[f], rP.at[f], dev(x, y, z, 1 - c)
        ).start()

    def start_ring(f):
        local_wait(RA.at[f], rA.at[f])
        for b in range(2):
            piece = dot(join, RA[f, 4 * b : 4 * b + 4].reshape(96, 384)).astype(BF16)
            for a in range(3):
                W[
                    f, c, a, pl.ds(pl.multiple_of(80 * place[f], 16), 80),
                    128 * b : 128 * b + 128,
                ] = piece[:, 128 * a : 128 * a + 128]
        for hops in (2, 1):
            for a in range(3):
                for way in range(2):
                    ring(f, way, hops - 1, a, hops).start()
        for a in range(3):
            share(f, a, place[f])

    def ring_step(f, s):
        step = (1, 0, 2, 3)[s]
        for a in range(3):
            for way in range(2):
                if step == 3 and way != a % 2:
                    continue
                ring(f, way, step, a, 0).wait_recv()
                if step == 1:
                    ring(f, way, 2, a, 1).start()
                    if way == a % 2:
                        ring(f, way, 3, a, 2).start()
                share(f, a, place[f] - (step + 1) * (1 if way == 0 else -1))

    start_ring(1)
    first_stage(0)
    for s in range(2):
        ring_step(1, s)

    row8 = iota((8, 256), 0)
    local_wait(Hc.at[0:3], rH)
    @pl.when(y < NY - 1)
    def _():
        remote(Hc.at[3], Hb.at[0], sN.at[0], rN.at[0], dev(x, lax.rem(y + 1, 8), z, c)).start()

    @pl.when(y > 0)
    def _():
        remote(Hc.at[0], Hb.at[1], sN.at[1], rN.at[1], dev(x, lax.rem(y + 7, 8), z, c)).start()

    zero = jnp.zeros((64, 256 - BLK), F32)
    sums = jnp.zeros((8, 256), F32)
    for img in range(2):
        tot = [jnp.zeros((1, 256), F32)] * 2
        sq = [jnp.zeros((1, 256), F32)] * 2
        for t in range(NX):
            both = Hc[t, 64 * img : 64 * img + 64, :].astype(F32)
            for a in range(2):
                v = jnp.concatenate([both[:, BLK * a : BLK * a + BLK], zero], axis=1)
                Hx[a, t, 64 * img : 64 * img + 64, :] = v
                tot[a] = tot[a] + jnp.sum(v, axis=0, keepdims=True)
                sq[a] = sq[a] + jnp.sum(v * v, axis=0, keepdims=True)
        for a in range(2):
            sums = jnp.where(row8 == 4 * a + img, tot[a], sums)
            sums = jnp.where(row8 == 4 * a + 2 + img, sq[a], sums)

    gi = group_of(iota((256, 256), 0))
    gj = group_of(iota((256, 256), 1))
    same = jnp.logical_and(gi == gj, gi < 4).astype(F32).astype(BF16)

    def group_totals(v):
        high = v.astype(BF16)
        left = v - high.astype(F32)
        mid = left.astype(BF16)
        low = (left - mid.astype(F32)).astype(BF16)
        terms = jnp.concatenate([high.astype(F32), mid.astype(F32), low.astype(F32)], axis=0).astype(BF16)
        got = dot(terms, same[:, 0:128])
        return got[0:8] + got[8:16] + got[16:24]

    def send_sums(p, value):
        value = group_totals(value)
        SS[p] = value
        ST[p, y] = value
        for k in range(1, NY):
            remote(
                SS.at[p], ST.at[p, y], sS.at[p], rS.at[p], dev(x, lax.rem(y + k, NY), z, c)
            ).start()

    def take_sums(p):
        local_wait(ST.at[p, 0:7], rS.at[p])
        tot = ST[p, 0]
        for k in range(1, NY):
            tot = tot + ST[p, k]
        tot = tot * (1.0 / NUMBER)
        last = jnp.where(iota((8, 128), 1) < 32, tot[:, 127:128], 0.0)
        return jnp.concatenate([tot, last], axis=1)

    send_sums(0, sums)
    for s in range(2, 4):
        ring_step(1, s)
    start_ring(0)

    ln128 = iota((32, 128), 1)

    def pack(v):
        fold = v[0:32, 128:256]
        for g in range(1, 4):
            fold = fold + pltpu.roll(v[32 * g : 32 * g + 32, 128:256], 32 * g, 1)
        return jnp.concatenate([v[:, 0:128], fold], axis=0)

    def unpack(m):
        fold = m[128:160]
        rest = [jnp.where(ln128 < 32, fold, 0.0)]
        for g in range(1, 4):
            rest.append(jnp.where(ln128 < 32, pltpu.roll(fold, 128 - 32 * g, 1), 0.0))
        return jnp.concatenate([m[0:128], jnp.concatenate(rest, axis=0)], axis=1)

    def combine(accs):
        rows = accs[0].shape[0]
        q = jnp.bitwise_and(iota((rows, 128), 0), 63)
        ln = iota((rows, 128), 1)
        t0 = jnp.zeros((rows, 128), F32)
        t1 = jnp.zeros((rows, 128), F32)
        for p in range(3):
            r = []
            for j in range(4):
                b = j // 2
                blk = accs[j % 2][:, 128 * b : 128 * b + 128]
                shift = (40 * j - 40 * p) % 128
                r.append(pltpu.roll(blk, shift, 1) if shift else blk)
            u0 = jnp.where(ln < 40, r[0], jnp.where(ln < 80, r[1], jnp.where(ln < 120, r[2], r[3])))
            u1 = jnp.where(ln < 32, r[3], 0.0)
            if p == 0:
                u0, u1 = (jnp.where(q == 63, 0.0, pltpu.roll(u, rows - 1, 0)) for u in (u0, u1))
            if p == 2:
                u0, u1 = (jnp.where(q == 0, 0.0, pltpu.roll(u, 1, 0)) for u in (u0, u1))
            t0 = t0 + u0
            t1 = t1 + u1
        return jnp.concatenate([t0, t1], axis=1)

    def conv(n, f, mul):
        for e, (ai, t) in enumerate(((0, 0), (2, 3))):
            PB[e] = combine([mul(f, cc, ai, t, t + 1) for cc in range(2)])
            HBs[n, e] = pack(PB[e])

        @pl.when(y > 0)
        def _():
            remote(HBs.at[n, 0], HBr.at[n, 0], sB.at[n, 0], rB.at[n, 0], dev(x, lax.rem(y + 7, 8), z, c)).start()

        @pl.when(y < NY - 1)
        def _():
            remote(HBs.at[n, 1], HBr.at[n, 1], sB.at[n, 1], rB.at[n, 1], dev(x, lax.rem(y + 1, 8), z, c)).start()

        for cc in range(2):
            AC[cc] = mul(f, cc, 1, 0, 4)
            AC[cc, 0:384] += mul(f, cc, 0, 1, 4)
            AC[cc, 128:512] += mul(f, cc, 2, 0, 3)
        BK[...] = combine([AC[0], AC[1]])

    def take_halo(n, e):
        @pl.when(y < NY - 1 if e == 0 else y > 0)
        def _():
            local_wait(HBr.at[n, e], rB.at[n, e])
            px = slice(384, 512) if e == 0 else slice(0, 128)
            BK[px] += unpack(HBr[n, e]) * KB[1 - e]

    def mul_cot(f, cc, ai, t0, t1):
        return dot(G[t0:t1].reshape((t1 - t0) * PX, CH), W[f, cc, ai])

    def mul_grad(f, cc, ai, t0, t1):
        return dot(L[t0 * PX : t1 * PX, :], W1[cc, ai])

    def slopes(a, t, img, gain, shift):
        avg, inv = stats[a]
        q = slice(64 * img, 64 * img + 64)
        v = Hx[a, t, q, :] if t < 4 else HxB[a, t - 4, q, :]
        normed = (v - avg[img : img + 1]) * inv[img : img + 1]
        linear = normed * gain + shift
        s = jax.nn.sigmoid(linear)
        return normed, s * (1.0 + linear * (1.0 - s)) * gain

    def norm_sums(n, a, gain, shift):
        first = [jnp.zeros((1, 256), F32)] * 2
        second = [jnp.zeros((1, 256), F32)] * 2
        for t in range(6):
            for img in range(2):
                q = slice(64 * img, 64 * img + 64)
                px = slice(t * PX + 64 * img, t * PX + 64 * img + 64)
                if n == 1:
                    normed, slope = slopes(a, t, img, gain, shift)
                else:
                    normed, slope = NB[t, q, :], SB[t, q, :]
                if t < 4:
                    scaled = BK[px, :] * slope
                    BK[px, :] = scaled
                    if t in (0, 3):
                        KB[t // 3, q, :] = slope
                else:
                    scaled = jnp.where(y > 0 if t == 4 else y < NY - 1, PB[t - 4, q, :] * slope, 0.0)
                first[img] = first[img] + jnp.sum(scaled, axis=0, keepdims=True)
                second[img] = second[img] + jnp.sum(scaled * normed, axis=0, keepdims=True)
        value = jnp.zeros((8, 256), F32)
        for img in range(2):
            value = jnp.where(row8 == img, first[img], value)
            value = jnp.where(row8 == 2 + img, second[img], value)
        send_sums(n, value)
        if n == 1:
            spare_time()
            ring_step(0, 0)
        take_halo(n - 1, 1)
        take_halo(n - 1, 0)
        got = take_sums(n)
        return got[0:2], got[2:4]

    def norm_apply(a, t, img, first, second):
        avg, inv = stats[a]
        px = slice(t * PX + 64 * img, t * PX + 64 * img + 64)
        v = Hx[a, t, 64 * img : 64 * img + 64, :]
        i_ = inv[img : img + 1]
        normed = (v - avg[img : img + 1]) * i_
        return i_ * (BK[px, :] - first[img : img + 1] - normed * second[img : img + 1])

    def spare_time():
        pick = (iota((CH, 256), 0) == iota((CH, 256), 1) + BLK * x) & (iota((CH, 256), 1) < BLK)
        pick = pick.astype(F32).astype(BF16)
        for t in range(NX):
            CC[t] = dot(G[t], pick)

    local_wait(G.at[0:3], rG)
    local_wait(W.at[1, 1 - c], rP.at[1])
    conv(0, 1, mul_cot)
    mean = take_sums(0)
    stats = []
    for a in range(2):
        avg = mean[4 * a : 4 * a + 2]
        inv = lax.rsqrt(mean[4 * a + 2 : 4 * a + 4] - avg * avg + 1e-05)
        stats.append((avg, inv))
    @pl.when(y > 0)
    def _():
        local_wait(Hb.at[0], rN.at[0])

    @pl.when(y < NY - 1)
    def _():
        local_wait(Hb.at[1], rN.at[1])

    for e in range(2):
        both = Hb[e].astype(F32)
        for a in range(2):
            HxB[a, e] = jnp.concatenate(
                [both[:, BLK * a : BLK * a + BLK], jnp.zeros((PX, 256 - BLK), F32)], axis=1
            )
    first, second = norm_sums(1, 0, params[0], params[1])
    for img in range(2):
        rest = jnp.zeros((64, 128), F32)
        for t in range(NX):
            v = norm_apply(0, t, img, first, second)
            Gh[x, t * PX + 64 * img : t * PX + 64 * img + 64, :] = v[:, 0:128].astype(BF16)
            rest = rest + (pltpu.roll(v[:, 128:256], 32 * t, 1) if t else v[:, 128:256])
        Gh[x, 512 + 64 * img : 576 + 64 * img, :] = rest.astype(BF16)
    for k in range(1, NX):
        remote(Gh.at[x], Gh.at[x], sGh, rGh, dev(lax.rem(x + k, NX), y, z, c)).start()
    for s in range(1, 4):
        ring_step(0, s)
    local_wait(W.at[0, 1 - c], rP.at[0])
    for k in range(NX):
        W1[:, :, 128 * k : 128 * k + 128, :] = W[0, :, :, BLK * k : BLK * k + 128, :]
        W1[:, :, 512 + 32 * k : 544 + 32 * k, :] = W[0, :, :, BLK * k + 128 : BLK * k + BLK, :]
    for t in range(6):
        for img in range(2):
            q = slice(64 * img, 64 * img + 64)
            NB[t, q, :], SB[t, q, :] = slopes(1, t, img, params[2], params[3])
    local_wait(Gh.at[0:3], rGh)
    lane = iota((PX, 128), 1)
    rests = [Gh[k, 512:640, :].astype(F32) for k in range(NX)]
    for k in range(NX):
        L[:, 128 * k : 128 * k + 128] = Gh[k, 0:512, :]
    for t in range(NX):
        v = jnp.zeros((PX, 128), F32)
        for k in range(NX):
            w = pltpu.roll(rests[k], (32 * (k - t)) % 128, 1) if k != t else rests[k]
            v = jnp.where((lane >= 32 * k) & (lane < 32 * k + 32), w, v)
        L[t * PX : t * PX + PX, 512:640] = v.astype(BF16)

    conv(1, 0, mul_grad)
    first, second = norm_sums(2, 1, params[2], params[3])
    for t in range(NX):
        v = jnp.concatenate([norm_apply(1, t, img, first, second) for img in range(2)], axis=0)
        Os[t] = pack(CC[t] + v).astype(BF16)
    for k in range(1, NX):
        t = lax.rem(x + k, NX)
        remote(Os.at[t], Oc.at[x], sO, rO, dev(t, y, z, c)).start()
    Oc[x] = Os[x]

    for f in (1, 0):
        local_wait(RA.at[f, 0:7], sA.at[f])

        @pl.when(jnp.logical_not(mine[f]))
        def _():
            local_wait(RA.at[f, 0], sA0.at[f])

        local_wait(W.at[f, 0, :, 0:560, :], sR.at[f])
        local_wait(W.at[f, 0], sP.at[f])
    local_wait(G.at[0:3], sG)
    local_wait(Gh.at[0:3], sGh)
    local_wait(Hc.at[0:3], sH)

    @pl.when(y < NY - 1)
    def _():
        local_wait(Hc.at[3], sN.at[0])

    @pl.when(y > 0)
    def _():
        local_wait(Hc.at[0], sN.at[1])

    for p in range(3):
        local_wait(ST.at[p, 0:7], sS.at[p])
    for n in range(2):
        @pl.when(y > 0)
        def _():
            local_wait(HBs.at[n, 0], sB.at[n, 0])

        @pl.when(y < NY - 1)
        def _():
            local_wait(HBs.at[n, 1], sB.at[n, 1])

    local_wait(Oc.at[0:3], rO)
    local_wait(Oc.at[0:3], sO)
    out[...] = jnp.concatenate(
        [unpack(Oc[k].astype(F32))[:, 0:BLK] for k in range(NX)], axis=1
    ).astype(BF16)


def body(latent, hidden, cotangent, filter_one, filter_two, gain_one, shift_one, gain_two, shift_two):
    filters = [jnp.transpose(a, (0, 2, 1)) for a in (filter_one, filter_two)]
    rows = [a.reshape(PX, CH) for a in (cotangent, hidden, latent)]
    params = (gain_two, shift_two, gain_one, shift_one)
    vmem = pl.BlockSpec(memory_space=pltpu.VMEM)
    anywhere = pl.BlockSpec(memory_space=pl.ANY)
    dma = pltpu.SemaphoreType.DMA
    out = pl.pallas_call(
        kernel,
        out_shape=jax.ShapeDtypeStruct((PX, CH), BF16),
        in_specs=[anywhere] * 9,
        out_specs=vmem,
        scratch_shapes=[
            pltpu.VMEM((2, 9, 20, 40), BF16),
            [pltpu.VMEM((CH,), F32)] * 4,
            pltpu.VMEM((2, PX, CH), BF16),
            pltpu.VMEM((2, 24, 384), BF16),
            pltpu.VMEM((2, 2, 3, CH, 256), BF16),
            pltpu.VMEM((2, 3, CH, 256), BF16),
            pltpu.VMEM((2, 8, 24, 384), BF16),
            pltpu.VMEM((NX, PX, CH), BF16),
            pltpu.VMEM((NX, 640, 128), BF16),
            pltpu.VMEM((NX * PX, CH), BF16),
            pltpu.VMEM((NX, PX, 384), BF16),
            pltpu.VMEM((NX, PX, 384), BF16),
            pltpu.VMEM((2, NX, PX, 256), F32),
            pltpu.VMEM((3, 8, 128), F32),
            pltpu.VMEM((3, NY, 8, 128), F32),
            pltpu.VMEM((2, PX, 384), BF16),
            pltpu.VMEM((2, 2, PX, 256), F32),
            pltpu.VMEM((6, PX, 256), F32),
            pltpu.VMEM((6, PX, 256), F32),
            pltpu.VMEM((2, PX, 256), F32),
            pltpu.VMEM((2, PX, 256), F32),
            pltpu.VMEM((2, 2, BLK, 128), F32),
            pltpu.VMEM((2, 2, BLK, 128), F32),
            pltpu.VMEM((2, NX * PX, 256), F32),
            pltpu.VMEM((NX * PX, 256), F32),
            pltpu.VMEM((NX, BLK, 128), BF16),
            pltpu.VMEM((NX, BLK, 128), BF16),
            pltpu.VMEM((NX, PX, 256), F32),
            dma((2,)), dma((4,)), dma((2,)), dma,
            dma((2,)), dma((2,)), dma((2,)),
            dma((2,)), dma((2, 2, 4, 3)),
            dma((2,)), dma((2,)),
            dma, dma, dma, dma, dma, dma,
            dma((3,)), dma((3,)),
            dma((2, 2)), dma((2, 2)),
            dma, dma,
            dma((2,)), dma((2,)),
        ],
        compiler_params=pltpu.CompilerParams(
            collective_id=0, has_side_effects=True, vmem_limit_bytes=62 * 1024 * 1024
        ),
        name="block_backward",
    )(*filters, *rows, *params)
    return out.reshape(latent.shape)


def solution(mesh):
    in_specs = (
        P("dp", "rows", None, None),
        P("dp", "rows", None, None),
        P("dp", "rows", None, None),
        P(None, "dp", "rows"),
        P(None, "dp", "rows"),
        P(),
        P(),
        P(),
        P(),
    )
    out_specs = P("dp", "rows", None, None)
    return jax.shard_map(body, mesh=mesh, in_specs=in_specs, out_specs=out_specs, check_vma=False)
```

```python
import jax
import jax.numpy as jnp
from jax import lax
from jax.experimental import pallas as pl
from jax.experimental.pallas import tpu as pltpu
from jax.sharding import PartitionSpec as P

MESH = pl.DeviceIdType.MESH
F32 = jnp.float32
BF16 = jnp.bfloat16
NX, NY, NZ = 4, 8, 8
CH = 640
BLK = 160
PX = 128
NUMBER = 32 * 64 * 40


def dev(x, y, z, c):
    return (2 * z + c, 4 * y + x)


def iota(shape, dim):
    return lax.broadcasted_iota(jnp.int32, shape, dim)


def dot(a, b, **kw):
    return jnp.dot(a, b, preferred_element_type=F32, **kw)


def group_of(lane):
    g = jnp.zeros_like(lane)
    for edge in (40, 80, 120, 160):
        g = g + (lane >= edge).astype(jnp.int32)
    return g


def kernel(
    f1, f2, cot, hid, lat, g2, s2, g1, s1, out,
    FV, PV, HV, WB, W, W1, RA, G, Gh, L, Hs, Hc, Hx, SS, ST, Hb, HxB, NB, SB, PB, KB, HBs, HBr, AC, BK, Os, Oc, CC,
    lF, lP, lH, lC, sA, sA0, rA, sR, rR, sP, rP, sG, rG, sGh, rGh, sH, rH, sS, rS, sB, rB, sO, rO, sN, rN,
):
    dp = lax.axis_index("dp")
    rr = lax.axis_index("rows")
    c = lax.rem(dp, 2)
    z = lax.div(dp, 2)
    x = lax.rem(rr, NX)
    y = lax.div(rr, NX)
    X = lax.div(z, 2)
    mine_y = x == X
    mine_z = jnp.logical_and(x == X, y == z)

    def remote(src, dst, ss, rs, target):
        return pltpu.make_async_remote_copy(
            src_ref=src, dst_ref=dst, send_sem=ss, recv_sem=rs, device_id=target,
            device_id_type=MESH,
        )

    def local_wait(ref, sem):
        pltpu.make_async_copy(ref, ref, sem).wait()

    Hb[...] = jnp.zeros_like(Hb)
    bar = pltpu.get_barrier_semaphore()

    def here(target):
        pl.semaphore_signal(bar, inc=1, device_id=target, device_id_type=MESH)

    for b in range(2):
        zs = 2 * x + lax.rem(z + b, 2)
        for k in range(NX):
            xs = lax.rem(x + k, NX)
            if b == 0 and k == 0:
                @pl.when(jnp.logical_not(mine_y))
                def _():
                    here(dev(xs, y, zs, c))

                @pl.when(jnp.logical_not(mine_z))
                def _():
                    here(dev(xs, z, zs, c))
            else:
                here(dev(xs, y, zs, c))
                here(dev(xs, z, zs, c))
    for k in range(1, NX):
        here(dev(lax.rem(x + k, NX), y, z, c))
    for k in range(1, NY):
        here(dev(x, lax.rem(y + k, NY), z, c))
    for k in (1, 2, NZ - 2, NZ - 1):
        here(dev(x, y, lax.rem(z + k, NZ), c))
    here(dev(x, y, z, 1 - c))

    loads = [pltpu.make_async_copy(r, FV.at[f], lF.at[f]) for f, r in enumerate((f1, f2))]
    loads += [pltpu.make_async_copy(r, HV.at[a], lH.at[a]) for a, r in enumerate((hid, lat))]
    loads += [
        pltpu.make_async_copy(r, PV[a], lP.at[a]) for a, r in enumerate((g2, s2, g1, s1))
    ]
    own_cot = pltpu.make_async_copy(cot, G.at[x], lC)
    for load in loads[1::-1] + loads[2:]:
        load.start()
    own_cot.start()
    WB[...] = jnp.zeros_like(WB)

    def own_block(f):
        loads[f].wait()
        for a in range(3):
            taps = [FV[f, 3 * a + b].astype(F32) for b in range(3)]
            WB[f, 0:20, 128 * a : 128 * a + 128] = jnp.concatenate(
                taps + [jnp.zeros((20, 8), F32)], axis=1
            ).astype(BF16)

    own_block(1)

    pl.semaphore_wait(
        bar, 31 - mine_y.astype(jnp.int32) - mine_z.astype(jnp.int32)
    )

    slot = lax.rem(z, 2) * 4 + x
    along_y = {f: lax.rem(f + c, 2) == 1 for f in (1, 0)}
    mine = {f: jnp.where(along_y[f], mine_y.astype(jnp.int32), mine_z.astype(jnp.int32)) == 1 for f in (1, 0)}
    place = {f: jnp.where(along_y[f], y, z) for f in (1, 0)}

    def first_stage(f):
        for k in range(8):
            y_ = jnp.where(along_y[f], y, lax.rem(y + k, NY))
            z_ = jnp.where(along_y[f], lax.rem(z + k, NZ), y)
            target = dev(X, y_, z_, c)
            if k == 0:
                @pl.when(mine[f])
                def _():
                    pltpu.make_async_copy(WB.at[f], RA.at[f, slot], rA.at[f]).start()

                @pl.when(jnp.logical_not(mine[f]))
                def _():
                    remote(WB.at[f], RA.at[f, slot], sA0.at[f], rA.at[f], target).start()
            else:
                remote(WB.at[f], RA.at[f, slot], sA.at[f], rA.at[f], target).start()

    first_stage(1)
    for a in range(2):
        loads[2 + a].wait()
    v = [HV[a].astype(F32) for a in range(2)]
    for k in range(NX):
        Hs[k] = jnp.concatenate(
            [v[a][:, BLK * k : BLK * k + BLK] for a in range(2)] + [jnp.zeros((PX, 64), F32)],
            axis=1,
        ).astype(BF16)
    own_cot.wait()
    for k in range(1, NX):
        t = lax.rem(x + k, NX)
        remote(Hs.at[t], Hc.at[x], sH, rH, dev(t, y, z, c)).start()
    for k in range(1, NX):
        t = lax.rem(x + k, NX)
        remote(G.at[x], G.at[x], sG, rG, dev(t, y, z, c)).start()
    Hc[x] = Hs[x]
    own_block(0)
    params = []
    for a in range(4):
        loads[4 + a].wait()
        whole = PV[a][...].reshape(1, CH)
        p = jnp.zeros((1, BLK), F32)
        for k in range(NX):
            p = jnp.where(x == k, whole[:, BLK * k : BLK * k + BLK], p)
        params.append(jnp.concatenate([p, jnp.zeros((1, 256 - BLK), F32)], axis=1))

    def region(f, cc, a, o):
        return W.at[f, cc, a, pl.ds(pl.multiple_of(80 * o, 16), 80), :]

    om = iota((80, 96), 0)
    mm_ = iota((80, 96), 1)
    hit = jnp.zeros((80, 96), jnp.bool_)
    for k in range(4):
        hit = jnp.logical_or(
            hit,
            jnp.logical_and(
                jnp.logical_and(mm_ >= 24 * k, mm_ < 24 * k + 20), om == mm_ - 4 * k
            ),
        )
    join = hit.astype(F32).astype(BF16)

    def at(f, p):
        return dev(x, jnp.where(along_y[f], p, y), jnp.where(along_y[f], z, p), c)

    def ring(f, way, step, a, hops):
        p = place[f]
        sign = 1 if way == 0 else -1
        o = lax.rem(p - sign * (step + 1 - hops) + 8, 8)
        return remote(
            region(f, c, a, o), region(f, c, a, o), sR.at[f], rR.at[f, way, step, a],
            at(f, lax.rem(p + sign * hops + 8, 8)),
        )

    def share(f, a, o):
        o = lax.rem(o + 8, 8)
        remote(
            region(f, c, a, o), region(f, c, a, o), sP.at[f], rP.at[f], dev(x, y, z, 1 - c)
        ).start()

    def start_ring(f):
        local_wait(RA.at[f], rA.at[f])
        for b in range(2):
            piece = dot(join, RA[f, 4 * b : 4 * b + 4].reshape(96, 384)).astype(BF16)
            for a in range(3):
                W[
                    f, c, a, pl.ds(pl.multiple_of(80 * place[f], 16), 80),
                    128 * b : 128 * b + 128,
                ] = piece[:, 128 * a : 128 * a + 128]
        for hops in (2, 1):
            for a in range(3):
                for way in range(2):
                    ring(f, way, hops - 1, a, hops).start()
        for a in range(3):
            share(f, a, place[f])

    def ring_step(f, s):
        step = (1, 0, 2, 3)[s]
        for a in range(3):
            for way in range(2):
                if step == 3 and way != a % 2:
                    continue
                ring(f, way, step, a, 0).wait_recv()
                if step == 1:
                    ring(f, way, 2, a, 1).start()
                    if way == a % 2:
                        ring(f, way, 3, a, 2).start()
                share(f, a, place[f] - (step + 1) * (1 if way == 0 else -1))

    start_ring(1)
    first_stage(0)
    for s in range(2):
        ring_step(1, s)

    row8 = iota((8, 256), 0)
    local_wait(Hc.at[0:3], rH)
    @pl.when(y < NY - 1)
    def _():
        remote(Hc.at[3], Hb.at[0], sN.at[0], rN.at[0], dev(x, lax.rem(y + 1, 8), z, c)).start()

    @pl.when(y > 0)
    def _():
        remote(Hc.at[0], Hb.at[1], sN.at[1], rN.at[1], dev(x, lax.rem(y + 7, 8), z, c)).start()

    zero = jnp.zeros((64, 256 - BLK), F32)
    sums = jnp.zeros((8, 256), F32)
    for img in range(2):
        tot = [jnp.zeros((1, 256), F32)] * 2
        sq = [jnp.zeros((1, 256), F32)] * 2
        for t in range(NX):
            both = Hc[t, 64 * img : 64 * img + 64, :].astype(F32)
            for a in range(2):
                v = jnp.concatenate([both[:, BLK * a : BLK * a + BLK], zero], axis=1)
                Hx[a, t, 64 * img : 64 * img + 64, :] = v
                tot[a] = tot[a] + jnp.sum(v, axis=0, keepdims=True)
                sq[a] = sq[a] + jnp.sum(v * v, axis=0, keepdims=True)
        for a in range(2):
            sums = jnp.where(row8 == 4 * a + img, tot[a], sums)
            sums = jnp.where(row8 == 4 * a + 2 + img, sq[a], sums)

    gi = group_of(iota((256, 256), 0))
    gj = group_of(iota((256, 256), 1))
    same = jnp.logical_and(gi == gj, gi < 4).astype(F32).astype(BF16)

    def group_totals(v):
        high = v.astype(BF16)
        left = v - high.astype(F32)
        mid = left.astype(BF16)
        low = (left - mid.astype(F32)).astype(BF16)
        terms = jnp.concatenate([high.astype(F32), mid.astype(F32), low.astype(F32)], axis=0).astype(BF16)
        got = dot(terms, same[:, 0:128])
        return got[0:8] + got[8:16] + got[16:24]

    def send_sums(p, value):
        value = group_totals(value)
        SS[p] = value
        ST[p, y] = value
        for k in range(1, NY):
            remote(
                SS.at[p], ST.at[p, y], sS.at[p], rS.at[p], dev(x, lax.rem(y + k, NY), z, c)
            ).start()

    def take_sums(p):
        local_wait(ST.at[p, 0:7], rS.at[p])
        tot = ST[p, 0]
        for k in range(1, NY):
            tot = tot + ST[p, k]
        tot = tot * (1.0 / NUMBER)
        last = jnp.where(iota((8, 128), 1) < 32, tot[:, 127:128], 0.0)
        return jnp.concatenate([tot, last], axis=1)

    send_sums(0, sums)
    for s in range(2, 4):
        ring_step(1, s)
    start_ring(0)

    ln128 = iota((16, 128), 1)

    def pack(v):
        fold = v[0:16, 128:256]
        for g in range(1, 4):
            fold = fold + pltpu.roll(v[16 * g : 16 * g + 16, 128:256], 32 * g, 1)
        return jnp.concatenate([v[:, 0:128], fold], axis=0)

    def unpack(m):
        fold = m[64:80]
        rest = [jnp.where(ln128 < 32, fold, 0.0)]
        for g in range(1, 4):
            rest.append(jnp.where(ln128 < 32, pltpu.roll(fold, 128 - 32 * g, 1), 0.0))
        return jnp.concatenate([m[0:64], jnp.concatenate(rest, axis=0)], axis=1)

    def combine(accs):
        rows = accs[0].shape[0]
        q = jnp.bitwise_and(iota((rows, 128), 0), 63)
        ln = iota((rows, 128), 1)
        t0 = jnp.zeros((rows, 128), F32)
        t1 = jnp.zeros((rows, 128), F32)
        for p in range(3):
            r = []
            for j in range(4):
                b = j // 2
                blk = accs[j % 2][:, 128 * b : 128 * b + 128]
                shift = (40 * j - 40 * p) % 128
                r.append(pltpu.roll(blk, shift, 1) if shift else blk)
            u0 = jnp.where(ln < 40, r[0], jnp.where(ln < 80, r[1], jnp.where(ln < 120, r[2], r[3])))
            u1 = jnp.where(ln < 32, r[3], 0.0)
            if p == 0:
                u0, u1 = (jnp.where(q == 63, 0.0, pltpu.roll(u, rows - 1, 0)) for u in (u0, u1))
            if p == 2:
                u0, u1 = (jnp.where(q == 0, 0.0, pltpu.roll(u, 1, 0)) for u in (u0, u1))
            t0 = t0 + u0
            t1 = t1 + u1
        return jnp.concatenate([t0, t1], axis=1)

    def conv(n, img, mul):
        for cc in range(2):
            AC[cc] = mul(img, cc, 1, 0, 4)
            AC[cc, 0:192] += mul(img, cc, 0, 1, 4)
            AC[cc, 64:256] += mul(img, cc, 2, 0, 3)
        BK[img] = combine([AC[0], AC[1]])
        for e, (ai, t) in enumerate(((0, 0), (2, 3))):
            PB[img, e] = combine([mul(img, cc, ai, t, t + 1) for cc in range(2)])
            HBs[n, img, e] = pack(PB[img, e])

        @pl.when(y > 0)
        def _():
            remote(
                HBs.at[n, img, 0], HBr.at[n, img, 0], sB.at[n, img, 0], rB.at[n, img, 0],
                dev(x, lax.rem(y + 7, 8), z, c),
            ).start()

        @pl.when(y < NY - 1)
        def _():
            remote(
                HBs.at[n, img, 1], HBr.at[n, img, 1], sB.at[n, img, 1], rB.at[n, img, 1],
                dev(x, lax.rem(y + 1, 8), z, c),
            ).start()

    def take_halo(n, img, e):
        @pl.when(y < NY - 1 if e == 0 else y > 0)
        def _():
            local_wait(HBr.at[n, img, e], rB.at[n, img, e])
            px = slice(192, 256) if e == 0 else slice(0, 64)
            BK[img, px] += unpack(HBr[n, img, e]) * KB[img, 1 - e]

    def mul_cot(img, cc, ai, t0, t1):
        rows = G[t0:t1, 64 * img : 64 * img + 64, :].reshape((t1 - t0) * 64, CH)
        return dot(rows, W[1, cc, ai])

    def mul_grad(img, cc, ai, t0, t1):
        return dot(L[img, 64 * t0 : 64 * t1, :], W1[cc, ai])

    def slopes(a, img):
        avg, inv = (v[img : img + 1] for v in stats[a])
        gain, shift = params[2 * a], params[2 * a + 1]
        q = slice(64 * img, 64 * img + 64)
        for t in range(6):
            v = Hx[a, t, q, :] if t < 4 else HxB[a, t - 4, q, :]
            normed = (v - avg) * inv
            linear = normed * gain + shift
            s = jax.nn.sigmoid(linear)
            NB[img, t] = normed
            SB[img, t] = s * (1.0 + linear * (1.0 - s)) * gain

    def norm_sums(n, img):
        first = jnp.zeros((1, 256), F32)
        second = jnp.zeros((1, 256), F32)
        for t in range(6):
            slope = SB[img, t]
            if t < 4:
                px = slice(64 * t, 64 * t + 64)
                scaled = BK[img, px, :] * slope
                BK[img, px, :] = scaled
                if t in (0, 3):
                    KB[img, t // 3] = slope
            else:
                valid = y > 0 if t == 4 else y < NY - 1
                scaled = jnp.where(valid, PB[img, t - 4] * slope, 0.0)
            first = first + jnp.sum(scaled, axis=0, keepdims=True)
            second = second + jnp.sum(scaled * NB[img, t], axis=0, keepdims=True)
        value = jnp.where(row8 == 0, first, jnp.where(row8 == 1, second, 0.0))
        send_sums(2 * n + 1 + img, value)

    def norm_finish(n, img):
        take_halo(n, img, 1)
        take_halo(n, img, 0)
        got = take_sums(2 * n + 1 + img)
        inv = stats[n][1][img : img + 1]
        first, second = got[0:1], got[1:2]
        return [
            inv * (BK[img, 64 * t : 64 * t + 64, :] - first - NB[img, t] * second) for t in range(NX)
        ]

    local_wait(G.at[0:3], rG)
    local_wait(W.at[1, 1 - c], rP.at[1])
    conv(0, 0, mul_cot)
    mean = take_sums(0)
    stats = []
    for a in range(2):
        avg = mean[4 * a : 4 * a + 2]
        inv = lax.rsqrt(mean[4 * a + 2 : 4 * a + 4] - avg * avg + 1e-05)
        stats.append((avg, inv))
    @pl.when(y > 0)
    def _():
        local_wait(Hb.at[0], rN.at[0])

    @pl.when(y < NY - 1)
    def _():
        local_wait(Hb.at[1], rN.at[1])

    for e in range(2):
        both = Hb[e].astype(F32)
        for a in range(2):
            HxB[a, e] = jnp.concatenate(
                [both[:, BLK * a : BLK * a + BLK], jnp.zeros((PX, 256 - BLK), F32)], axis=1
            )
    slopes(0, 0)
    norm_sums(0, 0)
    conv(0, 1, mul_cot)
    slopes(0, 1)
    norm_sums(0, 1)
    ring_step(0, 0)
    pick = (iota((CH, 256), 0) == iota((CH, 256), 1) + BLK * x) & (iota((CH, 256), 1) < BLK)
    pick = pick.astype(F32).astype(BF16)
    for t in range(NX):
        CC[t] = dot(G[t], pick)
    for img in range(2):
        rest = jnp.zeros((64, 128), F32)
        for t, v in enumerate(norm_finish(0, img)):
            Gh[img, x, 64 * t : 64 * t + 64, :] = v[:, 0:128].astype(BF16)
            rest = rest + (pltpu.roll(v[:, 128:256], 32 * t, 1) if t else v[:, 128:256])
        Gh[img, x, 256:320, :] = rest.astype(BF16)
        for k in range(1, NX):
            remote(
                Gh.at[img, x], Gh.at[img, x], sGh.at[img], rGh.at[img],
                dev(lax.rem(x + k, NX), y, z, c),
            ).start()
    for s in range(1, 4):
        ring_step(0, s)
    local_wait(W.at[0, 1 - c], rP.at[0])
    for k in range(NX):
        W1[:, :, 128 * k : 128 * k + 128, :] = W[0, :, :, BLK * k : BLK * k + 128, :]
        W1[:, :, 512 + 32 * k : 544 + 32 * k, :] = W[0, :, :, BLK * k + 128 : BLK * k + BLK, :]
    for img in range(2):
        slopes(1, img)
    lane = iota((64, 128), 1)
    for img in range(2):
        local_wait(Gh.at[img, 0:3], rGh.at[img])
        rests = [Gh[img, k, 256:320, :].astype(F32) for k in range(NX)]
        for k in range(NX):
            L[img, :, 128 * k : 128 * k + 128] = Gh[img, k, 0:256, :]
        for t in range(NX):
            v = jnp.zeros((64, 128), F32)
            for k in range(NX):
                w = pltpu.roll(rests[k], (32 * (k - t)) % 128, 1) if k != t else rests[k]
                v = jnp.where((lane >= 32 * k) & (lane < 32 * k + 32), w, v)
            L[img, 64 * t : 64 * t + 64, 512:640] = v.astype(BF16)
        conv(1, img, mul_grad)
        norm_sums(1, img)
    for img in range(2):
        for t, v in enumerate(norm_finish(1, img)):
            Os[img, t] = pack(CC[t, 64 * img : 64 * img + 64, :] + v).astype(BF16)
        for k in range(1, NX):
            t = lax.rem(x + k, NX)
            remote(
                Os.at[img, t], Oc.at[img, x], sO.at[img], rO.at[img], dev(t, y, z, c)
            ).start()
        Oc[img, x] = Os[img, x]

    for f in (1, 0):
        local_wait(RA.at[f, 0:7], sA.at[f])

        @pl.when(jnp.logical_not(mine[f]))
        def _():
            local_wait(RA.at[f, 0], sA0.at[f])

        local_wait(W.at[f, 0, :, 0:560, :], sR.at[f])
        local_wait(W.at[f, 0], sP.at[f])
    local_wait(G.at[0:3], sG)
    for img in range(2):
        local_wait(Gh.at[img, 0:3], sGh.at[img])
    local_wait(Hc.at[0:3], sH)

    @pl.when(y < NY - 1)
    def _():
        local_wait(Hc.at[3], sN.at[0])

    @pl.when(y > 0)
    def _():
        local_wait(Hc.at[0], sN.at[1])

    for p in range(5):
        local_wait(ST.at[p, 0:7], sS.at[p])
    for n, img in ((0, 0), (0, 1), (1, 0), (1, 1)):
        @pl.when(y > 0)
        def _():
            local_wait(HBs.at[n, img, 0], sB.at[n, img, 0])

        @pl.when(y < NY - 1)
        def _():
            local_wait(HBs.at[n, img, 1], sB.at[n, img, 1])

    for img in range(2):
        local_wait(Oc.at[img, 0:3], rO.at[img])
        out[64 * img : 64 * img + 64, :] = jnp.concatenate(
            [unpack(Oc[img, k].astype(F32))[:, 0:BLK] for k in range(NX)], axis=1
        ).astype(BF16)
    for img in range(2):
        local_wait(Oc.at[img, 0:3], sO.at[img])


def body(latent, hidden, cotangent, filter_one, filter_two, gain_one, shift_one, gain_two, shift_two):
    filters = [jnp.transpose(a, (0, 2, 1)) for a in (filter_one, filter_two)]
    rows = [a.reshape(PX, CH) for a in (cotangent, hidden, latent)]
    params = (gain_two, shift_two, gain_one, shift_one)
    vmem = pl.BlockSpec(memory_space=pltpu.VMEM)
    anywhere = pl.BlockSpec(memory_space=pl.ANY)
    dma = pltpu.SemaphoreType.DMA
    out = pl.pallas_call(
        kernel,
        out_shape=jax.ShapeDtypeStruct((PX, CH), BF16),
        in_specs=[anywhere] * 9,
        out_specs=vmem,
        scratch_shapes=[
            pltpu.VMEM((2, 9, 20, 40), BF16),
            [pltpu.VMEM((CH,), F32)] * 4,
            pltpu.VMEM((2, PX, CH), BF16),
            pltpu.VMEM((2, 24, 384), BF16),
            pltpu.VMEM((2, 2, 3, CH, 256), BF16),
            pltpu.VMEM((2, 3, CH, 256), BF16),
            pltpu.VMEM((2, 8, 24, 384), BF16),
            pltpu.VMEM((NX, PX, CH), BF16),
            pltpu.VMEM((2, NX, 320, 128), BF16),
            pltpu.VMEM((2, NX * 64, CH), BF16),
            pltpu.VMEM((NX, PX, 384), BF16),
            pltpu.VMEM((NX, PX, 384), BF16),
            pltpu.VMEM((2, NX, PX, 256), F32),
            pltpu.VMEM((5, 8, 128), F32),
            pltpu.VMEM((5, NY, 8, 128), F32),
            pltpu.VMEM((2, PX, 384), BF16),
            pltpu.VMEM((2, 2, PX, 256), F32),
            pltpu.VMEM((2, 6, 64, 256), F32),
            pltpu.VMEM((2, 6, 64, 256), F32),
            pltpu.VMEM((2, 2, 64, 256), F32),
            pltpu.VMEM((2, 2, 64, 256), F32),
            pltpu.VMEM((2, 2, 2, 80, 128), F32),
            pltpu.VMEM((2, 2, 2, 80, 128), F32),
            pltpu.VMEM((2, NX * 64, 256), F32),
            pltpu.VMEM((2, NX * 64, 256), F32),
            pltpu.VMEM((2, NX, 80, 128), BF16),
            pltpu.VMEM((2, NX, 80, 128), BF16),
            pltpu.VMEM((NX, PX, 256), F32),
            dma((2,)), dma((4,)), dma((2,)), dma,
            dma((2,)), dma((2,)), dma((2,)),
            dma((2,)), dma((2, 2, 4, 3)),
            dma((2,)), dma((2,)),
            dma, dma, dma((2,)), dma((2,)), dma, dma,
            dma((5,)), dma((5,)),
            dma((2, 2, 2)), dma((2, 2, 2)),
            dma((2,)), dma((2,)),
            dma((2,)), dma((2,)),
        ],
        compiler_params=pltpu.CompilerParams(
            collective_id=0, has_side_effects=True, vmem_limit_bytes=62 * 1024 * 1024
        ),
        name="block_backward",
    )(*filters, *rows, *params)
    return out.reshape(latent.shape)


def solution(mesh):
    in_specs = (
        P("dp", "rows", None, None),
        P("dp", "rows", None, None),
        P("dp", "rows", None, None),
        P(None, "dp", "rows"),
        P(None, "dp", "rows"),
        P(),
        P(),
        P(),
        P(),
    )
    out_specs = P("dp", "rows", None, None)
    return jax.shard_map(body, mesh=mesh, in_specs=in_specs, out_specs=out_specs, check_vma=False)
```

```python
import jax
import jax.numpy as jnp
from jax import lax
from jax.experimental import pallas as pl
from jax.experimental.pallas import tpu as pltpu
from jax.sharding import PartitionSpec as P

MESH = pl.DeviceIdType.MESH
F32 = jnp.float32
BF16 = jnp.bfloat16
NX, NY, NZ = 4, 8, 8
CH = 640
BLK = 160
PX = 128
NUMBER = 32 * 64 * 40
FAR_FIRST = (4, 3, 5, 2, 6, 1, 7)


def dev(x, y, z, c):
    return (2 * z + c, 4 * y + x)


def iota(shape, dim):
    return lax.broadcasted_iota(jnp.int32, shape, dim)


def dot(a, b, **kw):
    return jnp.dot(a, b, preferred_element_type=F32, **kw)


def group_of(lane):
    g = jnp.zeros_like(lane)
    for edge in (40, 80, 120, 160):
        g = g + (lane >= edge).astype(jnp.int32)
    return g


def kernel(
    f1, f2, cot, hid, lat, g2, s2, g1, s1, out,
    FV, PV, HV, WB, W, W1, RA, G, Gh, L, Hs, Hc, Hx, SS, ST, Hb, HxB, NB, SB, PB, KB, HBs, HBr, AC, BK, Os, Oc, CC,
    lF, lP, lH, lC, sA, sA0, rA, sR, rR, sP, rP, sG, rG, sGh, rGh, sH, rH, sS, rS, sB, rB, sO, rO, sN, rN,
):
    dp = lax.axis_index("dp")
    rr = lax.axis_index("rows")
    c = lax.rem(dp, 2)
    z = lax.div(dp, 2)
    x = lax.rem(rr, NX)
    y = lax.div(rr, NX)
    X = lax.div(z, 2)
    mine_y = x == X
    mine_z = jnp.logical_and(x == X, y == z)

    def remote(src, dst, ss, rs, target):
        return pltpu.make_async_remote_copy(
            src_ref=src, dst_ref=dst, send_sem=ss, recv_sem=rs, device_id=target,
            device_id_type=MESH,
        )

    def local_wait(ref, sem):
        pltpu.make_async_copy(ref, ref, sem).wait()

    Hb[...] = jnp.zeros_like(Hb)
    bar = pltpu.get_barrier_semaphore()

    def here(target):
        pl.semaphore_signal(bar, inc=1, device_id=target, device_id_type=MESH)

    for b in range(2):
        zs = 2 * x + lax.rem(z + b, 2)
        for k in range(NX):
            xs = lax.rem(x + k, NX)
            if b == 0 and k == 0:
                @pl.when(jnp.logical_not(mine_y))
                def _():
                    here(dev(xs, y, zs, c))

                @pl.when(jnp.logical_not(mine_z))
                def _():
                    here(dev(xs, z, zs, c))
            else:
                here(dev(xs, y, zs, c))
                here(dev(xs, z, zs, c))
    for k in range(1, NX):
        here(dev(lax.rem(x + k, NX), y, z, c))
    for k in range(1, NY):
        here(dev(x, lax.rem(y + k, NY), z, c))
    for k in (1, 2, NZ - 2, NZ - 1):
        here(dev(x, y, lax.rem(z + k, NZ), c))
    here(dev(x, y, z, 1 - c))

    loads = [pltpu.make_async_copy(r, FV.at[f], lF.at[f]) for f, r in enumerate((f1, f2))]
    loads += [pltpu.make_async_copy(r, HV.at[a], lH.at[a]) for a, r in enumerate((hid, lat))]
    loads += [
        pltpu.make_async_copy(r, PV[a], lP.at[a]) for a, r in enumerate((g2, s2, g1, s1))
    ]
    own_cot = pltpu.make_async_copy(cot, G.at[x], lC)
    for load in loads[1::-1] + loads[2:]:
        load.start()
    own_cot.start()
    WB[...] = jnp.zeros_like(WB)

    def own_block(f):
        loads[f].wait()
        for a in range(3):
            taps = [FV[f, 3 * a + b].astype(F32) for b in range(3)]
            WB[f, 0:20, 128 * a : 128 * a + 128] = jnp.concatenate(
                taps + [jnp.zeros((20, 8), F32)], axis=1
            ).astype(BF16)

    own_block(1)

    pl.semaphore_wait(
        bar, 31 - mine_y.astype(jnp.int32) - mine_z.astype(jnp.int32)
    )

    slot = lax.rem(z, 2) * 4 + x
    along_y = {f: lax.rem(f + c, 2) == 1 for f in (1, 0)}
    mine = {f: jnp.where(along_y[f], mine_y.astype(jnp.int32), mine_z.astype(jnp.int32)) == 1 for f in (1, 0)}
    place = {f: jnp.where(along_y[f], y, z) for f in (1, 0)}

    def first_stage(f):
        for k in FAR_FIRST + (0,):
            y_ = jnp.where(along_y[f], y, lax.rem(y + k, NY))
            z_ = jnp.where(along_y[f], lax.rem(z + k, NZ), y)
            target = dev(X, y_, z_, c)
            if k == 0:
                @pl.when(mine[f])
                def _():
                    pltpu.make_async_copy(WB.at[f], RA.at[f, slot], rA.at[f]).start()

                @pl.when(jnp.logical_not(mine[f]))
                def _():
                    remote(WB.at[f], RA.at[f, slot], sA0.at[f], rA.at[f], target).start()
            else:
                remote(WB.at[f], RA.at[f, slot], sA.at[f], rA.at[f], target).start()

    first_stage(1)
    for a in range(2):
        loads[2 + a].wait()
    v = [HV[a].astype(F32) for a in range(2)]
    for k in range(NX):
        Hs[k] = jnp.concatenate(
            [v[a][:, BLK * k : BLK * k + BLK] for a in range(2)] + [jnp.zeros((PX, 64), F32)],
            axis=1,
        ).astype(BF16)
    own_cot.wait()
    for k in range(1, NX):
        t = lax.rem(x + k, NX)
        remote(Hs.at[t], Hc.at[x], sH, rH, dev(t, y, z, c)).start()
    for k in range(1, NX):
        t = lax.rem(x + k, NX)
        remote(G.at[x], G.at[x], sG, rG, dev(t, y, z, c)).start()
    Hc[x] = Hs[x]
    own_block(0)
    params = []
    for a in range(4):
        loads[4 + a].wait()
        whole = PV[a][...].reshape(1, CH)
        p = jnp.zeros((1, BLK), F32)
        for k in range(NX):
            p = jnp.where(x == k, whole[:, BLK * k : BLK * k + BLK], p)
        params.append(jnp.concatenate([p, jnp.zeros((1, 256 - BLK), F32)], axis=1))

    def region(f, cc, a, o):
        return W.at[f, cc, a, pl.ds(pl.multiple_of(80 * o, 16), 80), :]

    om = iota((80, 96), 0)
    mm_ = iota((80, 96), 1)
    hit = jnp.zeros((80, 96), jnp.bool_)
    for k in range(4):
        hit = jnp.logical_or(
            hit,
            jnp.logical_and(
                jnp.logical_and(mm_ >= 24 * k, mm_ < 24 * k + 20), om == mm_ - 4 * k
            ),
        )
    join = hit.astype(F32).astype(BF16)

    def at(f, p):
        return dev(x, jnp.where(along_y[f], p, y), jnp.where(along_y[f], z, p), c)

    def ring(f, way, step, a, hops):
        p = place[f]
        sign = 1 if way == 0 else -1
        o = lax.rem(p - sign * (step + 1 - hops) + 8, 8)
        return remote(
            region(f, c, a, o), region(f, c, a, o), sR.at[f], rR.at[f, way, step, a],
            at(f, lax.rem(p + sign * hops + 8, 8)),
        )

    def share(f, a, o):
        o = lax.rem(o + 8, 8)
        remote(
            region(f, c, a, o), region(f, c, a, o), sP.at[f], rP.at[f], dev(x, y, z, 1 - c)
        ).start()

    def start_ring(f):
        local_wait(RA.at[f], rA.at[f])
        for b in range(2):
            piece = dot(join, RA[f, 4 * b : 4 * b + 4].reshape(96, 384)).astype(BF16)
            for a in range(3):
                W[
                    f, c, a, pl.ds(pl.multiple_of(80 * place[f], 16), 80),
                    128 * b : 128 * b + 128,
                ] = piece[:, 128 * a : 128 * a + 128]
        for hops in (2, 1):
            for a in range(3):
                for way in range(2):
                    ring(f, way, hops - 1, a, hops).start()
        for a in range(3):
            share(f, a, place[f])

    def ring_step(f, s):
        step = (1, 0, 2, 3)[s]
        for a in range(3):
            for way in range(2):
                if step == 3 and way != a % 2:
                    continue
                ring(f, way, step, a, 0).wait_recv()
                if step == 1:
                    ring(f, way, 2, a, 1).start()
                    if way == a % 2:
                        ring(f, way, 3, a, 2).start()
                share(f, a, place[f] - (step + 1) * (1 if way == 0 else -1))

    start_ring(1)
    first_stage(0)
    for s in range(2):
        ring_step(1, s)

    row8 = iota((8, 256), 0)
    local_wait(Hc.at[0:3], rH)
    zero = jnp.zeros((64, 256 - BLK), F32)
    sums = jnp.zeros((8, 256), F32)
    for img in range(2):
        tot = [jnp.zeros((1, 256), F32)] * 2
        sq = [jnp.zeros((1, 256), F32)] * 2
        for t in range(NX):
            both = Hc[t, 64 * img : 64 * img + 64, :].astype(F32)
            for a in range(2):
                v = jnp.concatenate([both[:, BLK * a : BLK * a + BLK], zero], axis=1)
                Hx[a, t, 64 * img : 64 * img + 64, :] = v
                tot[a] = tot[a] + jnp.sum(v, axis=0, keepdims=True)
                sq[a] = sq[a] + jnp.sum(v * v, axis=0, keepdims=True)
        for a in range(2):
            sums = jnp.where(row8 == 4 * a + img, tot[a], sums)
            sums = jnp.where(row8 == 4 * a + 2 + img, sq[a], sums)

    gi = group_of(iota((256, 256), 0))
    gj = group_of(iota((256, 256), 1))
    same = jnp.logical_and(gi == gj, gi < 4).astype(F32).astype(BF16)

    def group_totals(v):
        high = v.astype(BF16)
        left = v - high.astype(F32)
        mid = left.astype(BF16)
        low = (left - mid.astype(F32)).astype(BF16)
        terms = jnp.concatenate([high.astype(F32), mid.astype(F32), low.astype(F32)], axis=0).astype(BF16)
        got = dot(terms, same[:, 0:128])
        return got[0:8] + got[8:16] + got[16:24]

    def send_sums(p, value):
        value = group_totals(value)
        SS[p] = value
        ST[p, y] = value
        for k in FAR_FIRST:
            remote(
                SS.at[p], ST.at[p, y], sS.at[p], rS.at[p], dev(x, lax.rem(y + k, NY), z, c)
            ).start()

    def take_sums(p):
        local_wait(ST.at[p, 0:7], rS.at[p])
        tot = ST[p, 0]
        for k in range(1, NY):
            tot = tot + ST[p, k]
        tot = tot * (1.0 / NUMBER)
        last = jnp.where(iota((8, 128), 1) < 32, tot[:, 127:128], 0.0)
        return jnp.concatenate([tot, last], axis=1)

    send_sums(0, sums)
    @pl.when(y < NY - 1)
    def _():
        remote(Hc.at[3], Hb.at[0], sN.at[0], rN.at[0], dev(x, lax.rem(y + 1, 8), z, c)).start()

    @pl.when(y > 0)
    def _():
        remote(Hc.at[0], Hb.at[1], sN.at[1], rN.at[1], dev(x, lax.rem(y + 7, 8), z, c)).start()

    ring_step(1, 2)
    start_ring(0)
    ring_step(1, 3)

    ln128 = iota((16, 128), 1)

    def pack(v):
        fold = v[0:16, 128:256]
        for g in range(1, 4):
            fold = fold + pltpu.roll(v[16 * g : 16 * g + 16, 128:256], 32 * g, 1)
        return jnp.concatenate([v[:, 0:128], fold], axis=0)

    def unpack(m):
        fold = m[64:80]
        rest = [jnp.where(ln128 < 32, fold, 0.0)]
        for g in range(1, 4):
            rest.append(jnp.where(ln128 < 32, pltpu.roll(fold, 128 - 32 * g, 1), 0.0))
        return jnp.concatenate([m[0:64], jnp.concatenate(rest, axis=0)], axis=1)

    def combine(accs):
        rows = accs[0].shape[0]
        q = jnp.bitwise_and(iota((rows, 128), 0), 63)
        ln = iota((rows, 128), 1)
        t0 = jnp.zeros((rows, 128), F32)
        t1 = jnp.zeros((rows, 128), F32)
        for p in range(3):
            r = []
            for j in range(4):
                b = j // 2
                blk = accs[j % 2][:, 128 * b : 128 * b + 128]
                shift = (40 * j - 40 * p) % 128
                r.append(pltpu.roll(blk, shift, 1) if shift else blk)
            u0 = jnp.where(ln < 40, r[0], jnp.where(ln < 80, r[1], jnp.where(ln < 120, r[2], r[3])))
            u1 = jnp.where(ln < 32, r[3], 0.0)
            if p == 0:
                u0, u1 = (jnp.where(q == 63, 0.0, pltpu.roll(u, rows - 1, 0)) for u in (u0, u1))
            if p == 2:
                u0, u1 = (jnp.where(q == 0, 0.0, pltpu.roll(u, 1, 0)) for u in (u0, u1))
            t0 = t0 + u0
            t1 = t1 + u1
        return jnp.concatenate([t0, t1], axis=1)

    def conv(n, img, mul):
        for cc in range(2):
            AC[cc] = mul(img, cc, 1, 0, 4)
            AC[cc, 0:192] += mul(img, cc, 0, 1, 4)
            AC[cc, 64:256] += mul(img, cc, 2, 0, 3)
        BK[img] = combine([AC[0], AC[1]])
        for e, (ai, t) in enumerate(((0, 0), (2, 3))):
            PB[img, e] = combine([mul(img, cc, ai, t, t + 1) for cc in range(2)])
            HBs[n, img, e] = pack(PB[img, e])

        @pl.when(y > 0)
        def _():
            remote(
                HBs.at[n, img, 0], HBr.at[n, img, 0], sB.at[n, img, 0], rB.at[n, img, 0],
                dev(x, lax.rem(y + 7, 8), z, c),
            ).start()

        @pl.when(y < NY - 1)
        def _():
            remote(
                HBs.at[n, img, 1], HBr.at[n, img, 1], sB.at[n, img, 1], rB.at[n, img, 1],
                dev(x, lax.rem(y + 1, 8), z, c),
            ).start()

    def take_halo(n, img, e):
        @pl.when(y < NY - 1 if e == 0 else y > 0)
        def _():
            local_wait(HBr.at[n, img, e], rB.at[n, img, e])
            px = slice(192, 256) if e == 0 else slice(0, 64)
            BK[img, px] += unpack(HBr[n, img, e]) * KB[img, 1 - e]

    def mul_cot(img, cc, ai, t0, t1):
        rows = G[t0:t1, 64 * img : 64 * img + 64, :].reshape((t1 - t0) * 64, CH)
        return dot(rows, W[1, cc, ai])

    def mul_grad(img, cc, ai, t0, t1):
        return dot(L[img, 64 * t0 : 64 * t1, :], W1[cc, ai])

    def slopes(a, img):
        avg, inv = (v[img : img + 1] for v in stats[a])
        gain, shift = params[2 * a], params[2 * a + 1]
        q = slice(64 * img, 64 * img + 64)
        for t in range(6):
            v = Hx[a, t, q, :] if t < 4 else HxB[a, t - 4, q, :]
            normed = (v - avg) * inv
            linear = normed * gain + shift
            s = jax.nn.sigmoid(linear)
            NB[img, t] = normed
            SB[img, t] = s * (1.0 + linear * (1.0 - s)) * gain

    def norm_sums(n, img):
        first = jnp.zeros((1, 256), F32)
        second = jnp.zeros((1, 256), F32)
        for t in range(6):
            slope = SB[img, t]
            if t < 4:
                px = slice(64 * t, 64 * t + 64)
                scaled = BK[img, px, :] * slope
                BK[img, px, :] = scaled
                if t in (0, 3):
                    KB[img, t // 3] = slope
            else:
                valid = y > 0 if t == 4 else y < NY - 1
                scaled = jnp.where(valid, PB[img, t - 4] * slope, 0.0)
            first = first + jnp.sum(scaled, axis=0, keepdims=True)
            second = second + jnp.sum(scaled * NB[img, t], axis=0, keepdims=True)
        value = jnp.where(row8 == 0, first, jnp.where(row8 == 1, second, 0.0))
        send_sums(2 * n + 1 + img, value)

    def norm_finish(n, img):
        take_halo(n, img, 1)
        take_halo(n, img, 0)
        got = take_sums(2 * n + 1 + img)
        inv = stats[n][1][img : img + 1]
        first, second = got[0:1], got[1:2]
        return [
            inv * (BK[img, 64 * t : 64 * t + 64, :] - first - NB[img, t] * second) for t in range(NX)
        ]

    local_wait(G.at[0:3], rG)
    local_wait(W.at[1, 1 - c], rP.at[1])
    conv(0, 0, mul_cot)
    mean = take_sums(0)
    stats = []
    for a in range(2):
        avg = mean[4 * a : 4 * a + 2]
        inv = lax.rsqrt(mean[4 * a + 2 : 4 * a + 4] - avg * avg + 1e-05)
        stats.append((avg, inv))
    @pl.when(y > 0)
    def _():
        local_wait(Hb.at[0], rN.at[0])

    @pl.when(y < NY - 1)
    def _():
        local_wait(Hb.at[1], rN.at[1])

    for e in range(2):
        both = Hb[e].astype(F32)
        for a in range(2):
            HxB[a, e] = jnp.concatenate(
                [both[:, BLK * a : BLK * a + BLK], jnp.zeros((PX, 256 - BLK), F32)], axis=1
            )
    slopes(0, 0)
    norm_sums(0, 0)
    conv(0, 1, mul_cot)
    slopes(0, 1)
    norm_sums(0, 1)
    ring_step(0, 0)
    pick = (iota((CH, 256), 0) == iota((CH, 256), 1) + BLK * x) & (iota((CH, 256), 1) < BLK)
    pick = pick.astype(F32).astype(BF16)
    for t in range(NX):
        CC[t] = dot(G[t], pick)
    for img in range(2):
        rest = jnp.zeros((64, 128), F32)
        for t, v in enumerate(norm_finish(0, img)):
            Gh[img, x, 64 * t : 64 * t + 64, :] = v[:, 0:128].astype(BF16)
            rest = rest + (pltpu.roll(v[:, 128:256], 32 * t, 1) if t else v[:, 128:256])
        Gh[img, x, 256:320, :] = rest.astype(BF16)
        for k in (2, 1, 3):
            remote(
                Gh.at[img, x], Gh.at[img, x], sGh.at[img], rGh.at[img],
                dev(lax.rem(x + k, NX), y, z, c),
            ).start()
    for s in range(1, 4):
        ring_step(0, s)
    local_wait(W.at[0, 1 - c], rP.at[0])
    for k in range(NX):
        W1[:, :, 128 * k : 128 * k + 128, :] = W[0, :, :, BLK * k : BLK * k + 128, :]
        W1[:, :, 512 + 32 * k : 544 + 32 * k, :] = W[0, :, :, BLK * k + 128 : BLK * k + BLK, :]
    for img in range(2):
        slopes(1, img)
    lane = iota((64, 128), 1)
    for img in range(2):
        local_wait(Gh.at[img, 0:3], rGh.at[img])
        rests = [Gh[img, k, 256:320, :].astype(F32) for k in range(NX)]
        for k in range(NX):
            L[img, :, 128 * k : 128 * k + 128] = Gh[img, k, 0:256, :]
        for t in range(NX):
            v = jnp.zeros((64, 128), F32)
            for k in range(NX):
                w = pltpu.roll(rests[k], (32 * (k - t)) % 128, 1) if k != t else rests[k]
                v = jnp.where((lane >= 32 * k) & (lane < 32 * k + 32), w, v)
            L[img, 64 * t : 64 * t + 64, 512:640] = v.astype(BF16)
        conv(1, img, mul_grad)
        norm_sums(1, img)
    for img in range(2):
        for t, v in enumerate(norm_finish(1, img)):
            Os[img, t] = pack(CC[t, 64 * img : 64 * img + 64, :] + v).astype(BF16)
        for k in (2, 1, 3):
            t = lax.rem(x + k, NX)
            remote(
                Os.at[img, t], Oc.at[img, x], sO.at[img], rO.at[img], dev(t, y, z, c)
            ).start()
        Oc[img, x] = Os[img, x]

    for f in (1, 0):
        local_wait(RA.at[f, 0:7], sA.at[f])

        @pl.when(jnp.logical_not(mine[f]))
        def _():
            local_wait(RA.at[f, 0], sA0.at[f])

        local_wait(W.at[f, 0, :, 0:560, :], sR.at[f])
        local_wait(W.at[f, 0], sP.at[f])
    local_wait(G.at[0:3], sG)
    for img in range(2):
        local_wait(Gh.at[img, 0:3], sGh.at[img])
    local_wait(Hc.at[0:3], sH)

    @pl.when(y < NY - 1)
    def _():
        local_wait(Hc.at[3], sN.at[0])

    @pl.when(y > 0)
    def _():
        local_wait(Hc.at[0], sN.at[1])

    for p in range(5):
        local_wait(ST.at[p, 0:7], sS.at[p])
    for n, img in ((0, 0), (0, 1), (1, 0), (1, 1)):
        @pl.when(y > 0)
        def _():
            local_wait(HBs.at[n, img, 0], sB.at[n, img, 0])

        @pl.when(y < NY - 1)
        def _():
            local_wait(HBs.at[n, img, 1], sB.at[n, img, 1])

    for img in range(2):
        local_wait(Oc.at[img, 0:3], rO.at[img])
        out[64 * img : 64 * img + 64, :] = jnp.concatenate(
            [unpack(Oc[img, k].astype(F32))[:, 0:BLK] for k in range(NX)], axis=1
        ).astype(BF16)
    for img in range(2):
        local_wait(Oc.at[img, 0:3], sO.at[img])


def body(latent, hidden, cotangent, filter_one, filter_two, gain_one, shift_one, gain_two, shift_two):
    filters = [jnp.transpose(a, (0, 2, 1)) for a in (filter_one, filter_two)]
    rows = [a.reshape(PX, CH) for a in (cotangent, hidden, latent)]
    params = (gain_two, shift_two, gain_one, shift_one)
    vmem = pl.BlockSpec(memory_space=pltpu.VMEM)
    anywhere = pl.BlockSpec(memory_space=pl.ANY)
    dma = pltpu.SemaphoreType.DMA
    out = pl.pallas_call(
        kernel,
        out_shape=jax.ShapeDtypeStruct((PX, CH), BF16),
        in_specs=[anywhere] * 9,
        out_specs=vmem,
        scratch_shapes=[
            pltpu.VMEM((2, 9, 20, 40), BF16),
            [pltpu.VMEM((CH,), F32)] * 4,
            pltpu.VMEM((2, PX, CH), BF16),
            pltpu.VMEM((2, 24, 384), BF16),
            pltpu.VMEM((2, 2, 3, CH, 256), BF16),
            pltpu.VMEM((2, 3, CH, 256), BF16),
            pltpu.VMEM((2, 8, 24, 384), BF16),
            pltpu.VMEM((NX, PX, CH), BF16),
            pltpu.VMEM((2, NX, 320, 128), BF16),
            pltpu.VMEM((2, NX * 64, CH), BF16),
            pltpu.VMEM((NX, PX, 384), BF16),
            pltpu.VMEM((NX, PX, 384), BF16),
            pltpu.VMEM((2, NX, PX, 256), F32),
            pltpu.VMEM((5, 8, 128), F32),
            pltpu.VMEM((5, NY, 8, 128), F32),
            pltpu.VMEM((2, PX, 384), BF16),
            pltpu.VMEM((2, 2, PX, 256), F32),
            pltpu.VMEM((2, 6, 64, 256), F32),
            pltpu.VMEM((2, 6, 64, 256), F32),
            pltpu.VMEM((2, 2, 64, 256), F32),
            pltpu.VMEM((2, 2, 64, 256), F32),
            pltpu.VMEM((2, 2, 2, 80, 128), F32),
            pltpu.VMEM((2, 2, 2, 80, 128), F32),
            pltpu.VMEM((2, NX * 64, 256), F32),
            pltpu.VMEM((2, NX * 64, 256), F32),
            pltpu.VMEM((2, NX, 80, 128), BF16),
            pltpu.VMEM((2, NX, 80, 128), BF16),
            pltpu.VMEM((NX, PX, 256), F32),
            dma((2,)), dma((4,)), dma((2,)), dma,
            dma((2,)), dma((2,)), dma((2,)),
            dma((2,)), dma((2, 2, 4, 3)),
            dma((2,)), dma((2,)),
            dma, dma, dma((2,)), dma((2,)), dma, dma,
            dma((5,)), dma((5,)),
            dma((2, 2, 2)), dma((2, 2, 2)),
            dma((2,)), dma((2,)),
            dma((2,)), dma((2,)),
        ],
        compiler_params=pltpu.CompilerParams(
            collective_id=0, has_side_effects=True, vmem_limit_bytes=62 * 1024 * 1024
        ),
        name="block_backward",
    )(*filters, *rows, *params)
    return out.reshape(latent.shape)


def solution(mesh):
    in_specs = (
        P("dp", "rows", None, None),
        P("dp", "rows", None, None),
        P("dp", "rows", None, None),
        P(None, "dp", "rows"),
        P(None, "dp", "rows"),
        P(),
        P(),
        P(),
        P(),
    )
    out_specs = P("dp", "rows", None, None)
    return jax.shard_map(body, mesh=mesh, in_specs=in_specs, out_specs=out_specs, check_vma=False)
```

```python
import jax
import jax.numpy as jnp
from jax import lax
from jax.experimental import pallas as pl
from jax.experimental.pallas import tpu as pltpu
from jax.sharding import PartitionSpec as P

MESH = pl.DeviceIdType.MESH
F32 = jnp.float32
BF16 = jnp.bfloat16
NX, NY, NZ = 4, 8, 8
CH = 640
BLK = 160
PX = 128
NUMBER = 32 * 64 * 40
FAR_FIRST = (4, 3, 5, 2, 6, 1, 7)


def dev(x, y, z, c):
    return (2 * z + c, 4 * y + x)


def iota(shape, dim):
    return lax.broadcasted_iota(jnp.int32, shape, dim)


def dot(a, b, **kw):
    return jnp.dot(a, b, preferred_element_type=F32, **kw)


def group_of(lane):
    g = jnp.zeros_like(lane)
    for edge in (40, 80, 120, 160):
        g = g + (lane >= edge).astype(jnp.int32)
    return g


def kernel(
    f1, f2, cot, hid, lat, g2, s2, g1, s1, out,
    FV, PV, HV, WB, W, W1, RA, G, Gh, L, Hs, Hc, Hx, SS, ST, Hb, HxB, NB, SB, PB, KB, HBs, HBr, AC, BK, Os, Oc, CC,
    lF, lP, lH, lC, sA, sA0, rA, sR, rR, sP, rP, sG, rG, sGh, rGh, sH, rH, sS, rS, sB, rB, sO, rO, sN, rN,
):
    dp = lax.axis_index("dp")
    rr = lax.axis_index("rows")
    c = lax.rem(dp, 2)
    z = lax.div(dp, 2)
    x = lax.rem(rr, NX)
    y = lax.div(rr, NX)
    X = lax.div(z, 2)
    mine_y = x == X
    mine_z = jnp.logical_and(x == X, y == z)

    def remote(src, dst, ss, rs, target):
        return pltpu.make_async_remote_copy(
            src_ref=src, dst_ref=dst, send_sem=ss, recv_sem=rs, device_id=target,
            device_id_type=MESH,
        )

    def local_wait(ref, sem):
        pltpu.make_async_copy(ref, ref, sem).wait()

    Hb[...] = jnp.zeros_like(Hb)
    bar = pltpu.get_barrier_semaphore()

    def here(target):
        pl.semaphore_signal(bar, inc=1, device_id=target, device_id_type=MESH)

    for b in range(2):
        zs = 2 * x + lax.rem(z + b, 2)
        for k in range(NX):
            xs = lax.rem(x + k, NX)
            if b == 0 and k == 0:
                @pl.when(jnp.logical_not(mine_y))
                def _():
                    here(dev(xs, y, zs, c))

                @pl.when(jnp.logical_not(mine_z))
                def _():
                    here(dev(xs, z, zs, c))
            else:
                here(dev(xs, y, zs, c))
                here(dev(xs, z, zs, c))
    for k in range(1, NX):
        here(dev(lax.rem(x + k, NX), y, z, c))
    for k in range(1, NY):
        here(dev(x, lax.rem(y + k, NY), z, c))
    for k in (1, 2, NZ - 2, NZ - 1):
        here(dev(x, y, lax.rem(z + k, NZ), c))
    here(dev(x, y, z, 1 - c))

    loads = [pltpu.make_async_copy(r, FV.at[f], lF.at[f]) for f, r in enumerate((f1, f2))]
    loads += [pltpu.make_async_copy(r, HV.at[a], lH.at[a]) for a, r in enumerate((hid, lat))]
    loads += [
        pltpu.make_async_copy(r, PV[a], lP.at[a]) for a, r in enumerate((g2, s2, g1, s1))
    ]
    own_cot = pltpu.make_async_copy(cot, G.at[x], lC)
    for load in loads[1::-1] + loads[2:]:
        load.start()
    own_cot.start()
    WB[...] = jnp.zeros_like(WB)

    def own_block(f):
        loads[f].wait()
        for a in range(3):
            taps = [FV[f, 3 * a + b].astype(F32) for b in range(3)]
            WB[f, 0:20, 128 * a : 128 * a + 128] = jnp.concatenate(
                taps + [jnp.zeros((20, 8), F32)], axis=1
            ).astype(BF16)

    own_block(1)

    pl.semaphore_wait(
        bar, 31 - mine_y.astype(jnp.int32) - mine_z.astype(jnp.int32)
    )

    slot = lax.rem(z, 2) * 4 + x
    along_y = {f: lax.rem(f + c, 2) == 1 for f in (1, 0)}
    mine = {f: jnp.where(along_y[f], mine_y.astype(jnp.int32), mine_z.astype(jnp.int32)) == 1 for f in (1, 0)}
    place = {f: jnp.where(along_y[f], y, z) for f in (1, 0)}

    def first_stage(f):
        for k in FAR_FIRST + (0,):
            y_ = jnp.where(along_y[f], y, lax.rem(y + k, NY))
            z_ = jnp.where(along_y[f], lax.rem(z + k, NZ), y)
            target = dev(X, y_, z_, c)
            if k == 0:
                @pl.when(mine[f])
                def _():
                    pltpu.make_async_copy(WB.at[f], RA.at[f, slot], rA.at[f]).start()

                @pl.when(jnp.logical_not(mine[f]))
                def _():
                    remote(WB.at[f], RA.at[f, slot], sA0.at[f], rA.at[f], target).start()
            else:
                remote(WB.at[f], RA.at[f, slot], sA.at[f], rA.at[f], target).start()

    first_stage(1)
    for a in range(2):
        loads[2 + a].wait()
    v = [HV[a].astype(F32) for a in range(2)]
    for k in range(NX):
        Hs[k] = jnp.concatenate(
            [v[a][:, BLK * k : BLK * k + BLK] for a in range(2)] + [jnp.zeros((PX, 64), F32)],
            axis=1,
        ).astype(BF16)
    own_cot.wait()
    for k in range(1, NX):
        t = lax.rem(x + k, NX)
        remote(Hs.at[t], Hc.at[x], sH, rH, dev(t, y, z, c)).start()
    for k in range(1, NX):
        t = lax.rem(x + k, NX)
        remote(G.at[x], G.at[x], sG, rG, dev(t, y, z, c)).start()
    Hc[x] = Hs[x]
    own_block(0)
    params = []
    for a in range(4):
        loads[4 + a].wait()
        whole = PV[a][...].reshape(1, CH)
        p = jnp.zeros((1, BLK), F32)
        for k in range(NX):
            p = jnp.where(x == k, whole[:, BLK * k : BLK * k + BLK], p)
        params.append(jnp.concatenate([p, jnp.zeros((1, 256 - BLK), F32)], axis=1))

    def region(f, cc, a, o):
        return W.at[f, cc, a, pl.ds(pl.multiple_of(80 * o, 16), 80), :]

    om = iota((80, 96), 0)
    mm_ = iota((80, 96), 1)
    hit = jnp.zeros((80, 96), jnp.bool_)
    for k in range(4):
        hit = jnp.logical_or(
            hit,
            jnp.logical_and(
                jnp.logical_and(mm_ >= 24 * k, mm_ < 24 * k + 20), om == mm_ - 4 * k
            ),
        )
    join = hit.astype(F32).astype(BF16)

    def at(f, p):
        return dev(x, jnp.where(along_y[f], p, y), jnp.where(along_y[f], z, p), c)

    def ring(f, way, step, a, hops):
        p = place[f]
        sign = 1 if way == 0 else -1
        o = lax.rem(p - sign * (step + 1 - hops) + 8, 8)
        return remote(
            region(f, c, a, o), region(f, c, a, o), sR.at[f], rR.at[f, way, step, a],
            at(f, lax.rem(p + sign * hops + 8, 8)),
        )

    def share(f, a, o):
        o = lax.rem(o + 8, 8)
        remote(
            region(f, c, a, o), region(f, c, a, o), sP.at[f], rP.at[f], dev(x, y, z, 1 - c)
        ).start()

    def start_ring(f):
        local_wait(RA.at[f], rA.at[f])
        for b in range(2):
            piece = dot(join, RA[f, 4 * b : 4 * b + 4].reshape(96, 384)).astype(BF16)
            for a in range(3):
                W[
                    f, c, a, pl.ds(pl.multiple_of(80 * place[f], 16), 80),
                    128 * b : 128 * b + 128,
                ] = piece[:, 128 * a : 128 * a + 128]
        for hops in (2, 1):
            for a in range(3):
                for way in range(2):
                    ring(f, way, hops - 1, a, hops).start()
        for a in range(3):
            share(f, a, place[f])

    def ring_step(f, s):
        step = (1, 0, 2, 3)[s]
        for a in range(3):
            for way in range(2):
                if step == 3 and way != a % 2:
                    continue
                ring(f, way, step, a, 0).wait_recv()
                if step == 1:
                    ring(f, way, 2, a, 1).start()
                    if way == a % 2:
                        ring(f, way, 3, a, 2).start()
                share(f, a, place[f] - (step + 1) * (1 if way == 0 else -1))

    start_ring(1)
    first_stage(0)
    for s in range(2):
        ring_step(1, s)

    row8 = iota((8, 256), 0)
    local_wait(Hc.at[0:3], rH)
    zero = jnp.zeros((64, 256 - BLK), F32)
    sums = jnp.zeros((8, 256), F32)
    for img in range(2):
        tot = [jnp.zeros((1, 256), F32)] * 2
        sq = [jnp.zeros((1, 256), F32)] * 2
        for t in range(NX):
            both = Hc[t, 64 * img : 64 * img + 64, :].astype(F32)
            for a in range(2):
                v = jnp.concatenate([both[:, BLK * a : BLK * a + BLK], zero], axis=1)
                Hx[a, t, 64 * img : 64 * img + 64, :] = v
                tot[a] = tot[a] + jnp.sum(v, axis=0, keepdims=True)
                sq[a] = sq[a] + jnp.sum(v * v, axis=0, keepdims=True)
        for a in range(2):
            sums = jnp.where(row8 == 4 * a + img, tot[a], sums)
            sums = jnp.where(row8 == 4 * a + 2 + img, sq[a], sums)

    gi = group_of(iota((256, 256), 0))
    gj = group_of(iota((256, 256), 1))
    same = jnp.logical_and(gi == gj, gi < 4).astype(F32).astype(BF16)

    def group_totals(v):
        high = v.astype(BF16)
        left = v - high.astype(F32)
        mid = left.astype(BF16)
        low = (left - mid.astype(F32)).astype(BF16)
        terms = jnp.concatenate([high.astype(F32), mid.astype(F32), low.astype(F32)], axis=0).astype(BF16)
        got = dot(terms, same[:, 0:128])
        return got[0:8] + got[8:16] + got[16:24]

    def send_sums(p, value):
        value = group_totals(value)
        SS[p] = value
        ST[p, y] = value
        for k in FAR_FIRST:
            remote(
                SS.at[p], ST.at[p, y], sS.at[p], rS.at[p], dev(x, lax.rem(y + k, NY), z, c)
            ).start()

    def take_sums(p):
        local_wait(ST.at[p, 0:7], rS.at[p])
        tot = ST[p, 0]
        for k in range(1, NY):
            tot = tot + ST[p, k]
        tot = tot * (1.0 / NUMBER)
        last = jnp.where(iota((8, 128), 1) < 32, tot[:, 127:128], 0.0)
        return jnp.concatenate([tot, last], axis=1)

    send_sums(0, sums)
    @pl.when(y < NY - 1)
    def _():
        remote(Hc.at[3], Hb.at[0], sN.at[0], rN.at[0], dev(x, lax.rem(y + 1, 8), z, c)).start()

    @pl.when(y > 0)
    def _():
        remote(Hc.at[0], Hb.at[1], sN.at[1], rN.at[1], dev(x, lax.rem(y + 7, 8), z, c)).start()

    ring_step(1, 2)
    @pl.when(c == 1)
    def _():
        start_ring(0)

    ring_step(1, 3)

    @pl.when(c == 0)
    def _():
        start_ring(0)


    ln128 = iota((16, 128), 1)

    def pack(v):
        fold = v[0:16, 128:256]
        for g in range(1, 4):
            fold = fold + pltpu.roll(v[16 * g : 16 * g + 16, 128:256], 32 * g, 1)
        return jnp.concatenate([v[:, 0:128], fold], axis=0)

    def unpack(m):
        fold = m[64:80]
        rest = [jnp.where(ln128 < 32, fold, 0.0)]
        for g in range(1, 4):
            rest.append(jnp.where(ln128 < 32, pltpu.roll(fold, 128 - 32 * g, 1), 0.0))
        return jnp.concatenate([m[0:64], jnp.concatenate(rest, axis=0)], axis=1)

    def combine(accs):
        rows = accs[0].shape[0]
        q = jnp.bitwise_and(iota((rows, 128), 0), 63)
        ln = iota((rows, 128), 1)
        t0 = jnp.zeros((rows, 128), F32)
        t1 = jnp.zeros((rows, 128), F32)
        for p in range(3):
            r = []
            for j in range(4):
                b = j // 2
                blk = accs[j % 2][:, 128 * b : 128 * b + 128]
                shift = (40 * j - 40 * p) % 128
                r.append(pltpu.roll(blk, shift, 1) if shift else blk)
            u0 = jnp.where(ln < 40, r[0], jnp.where(ln < 80, r[1], jnp.where(ln < 120, r[2], r[3])))
            u1 = jnp.where(ln < 32, r[3], 0.0)
            if p == 0:
                u0, u1 = (jnp.where(q == 63, 0.0, pltpu.roll(u, rows - 1, 0)) for u in (u0, u1))
            if p == 2:
                u0, u1 = (jnp.where(q == 0, 0.0, pltpu.roll(u, 1, 0)) for u in (u0, u1))
            t0 = t0 + u0
            t1 = t1 + u1
        return jnp.concatenate([t0, t1], axis=1)

    def conv(n, img, mul):
        for cc in range(2):
            AC[cc, 256:384] = jnp.zeros((128, 256), F32)
            AC[cc, 0:256] = mul(img, cc, 0)
            AC[cc, 64:320] += mul(img, cc, 1)
            AC[cc, 128:384] += mul(img, cc, 2)
        back = combine([AC[0], AC[1]])
        BK[img] = back[64:320]
        for e in range(2):
            PB[img, e] = back[320 * e : 320 * e + 64]
            HBs[n, img, e] = pack(back[320 * e : 320 * e + 64])

    def send_halo(n, img):
        @pl.when(y > 0)
        def _():
            remote(
                HBs.at[n, img, 0], HBr.at[n, img, 0], sB.at[n, img, 0], rB.at[n, img, 0],
                dev(x, lax.rem(y + 7, 8), z, c),
            ).start()

        @pl.when(y < NY - 1)
        def _():
            remote(
                HBs.at[n, img, 1], HBr.at[n, img, 1], sB.at[n, img, 1], rB.at[n, img, 1],
                dev(x, lax.rem(y + 1, 8), z, c),
            ).start()

    def take_halo(n, img, e):
        @pl.when(y < NY - 1 if e == 0 else y > 0)
        def _():
            local_wait(HBr.at[n, img, e], rB.at[n, img, e])
            px = slice(192, 256) if e == 0 else slice(0, 64)
            BK[img, px] += unpack(HBr[n, img, e]) * KB[img, 1 - e]

    def mul_cot(img, cc, ai):
        return dot(G[:, 64 * img : 64 * img + 64, :].reshape(NX * 64, CH), W[1, cc, ai])

    def mul_grad(img, cc, ai):
        return dot(L[img], W1[cc, ai])

    def slopes(a, img):
        avg, inv = (v[img : img + 1] for v in stats[a])
        gain, shift = params[2 * a], params[2 * a + 1]
        q = slice(64 * img, 64 * img + 64)
        for t in range(6):
            v = Hx[a, t, q, :] if t < 4 else HxB[a, t - 4, q, :]
            normed = (v - avg) * inv
            linear = normed * gain + shift
            s = jax.nn.sigmoid(linear)
            NB[img, t] = normed
            SB[img, t] = s * (1.0 + linear * (1.0 - s)) * gain

    def norm_sums(n, img):
        first = jnp.zeros((1, 256), F32)
        second = jnp.zeros((1, 256), F32)
        for t in range(6):
            slope = SB[img, t]
            if t < 4:
                px = slice(64 * t, 64 * t + 64)
                scaled = BK[img, px, :] * slope
                BK[img, px, :] = scaled
                if t in (0, 3):
                    KB[img, t // 3] = slope
            else:
                valid = y > 0 if t == 4 else y < NY - 1
                scaled = jnp.where(valid, PB[img, t - 4] * slope, 0.0)
            first = first + jnp.sum(scaled, axis=0, keepdims=True)
            second = second + jnp.sum(scaled * NB[img, t], axis=0, keepdims=True)
        value = jnp.where(row8 == 0, first, jnp.where(row8 == 1, second, 0.0))
        send_sums(2 * n + 1 + img, value)
        send_halo(n, img)

    def norm_finish(n, img):
        take_halo(n, img, 1)
        take_halo(n, img, 0)
        got = take_sums(2 * n + 1 + img)
        inv = stats[n][1][img : img + 1]
        first, second = got[0:1], got[1:2]
        return [
            inv * (BK[img, 64 * t : 64 * t + 64, :] - first - NB[img, t] * second) for t in range(NX)
        ]

    local_wait(G.at[0:3], rG)
    local_wait(W.at[1, 1 - c], rP.at[1])
    conv(0, 0, mul_cot)
    mean = take_sums(0)
    stats = []
    for a in range(2):
        avg = mean[4 * a : 4 * a + 2]
        inv = lax.rsqrt(mean[4 * a + 2 : 4 * a + 4] - avg * avg + 1e-05)
        stats.append((avg, inv))
    @pl.when(y > 0)
    def _():
        local_wait(Hb.at[0], rN.at[0])

    @pl.when(y < NY - 1)
    def _():
        local_wait(Hb.at[1], rN.at[1])

    for e in range(2):
        both = Hb[e].astype(F32)
        for a in range(2):
            HxB[a, e] = jnp.concatenate(
                [both[:, BLK * a : BLK * a + BLK], jnp.zeros((PX, 256 - BLK), F32)], axis=1
            )
    slopes(0, 0)
    norm_sums(0, 0)
    slopes(0, 1)
    conv(0, 1, mul_cot)
    norm_sums(0, 1)
    ring_step(0, 0)
    pick = (iota((CH, 256), 0) == iota((CH, 256), 1) + BLK * x) & (iota((CH, 256), 1) < BLK)
    pick = pick.astype(F32).astype(BF16)
    for t in range(NX):
        CC[t] = dot(G[t], pick)
    for img in range(2):
        rest = jnp.zeros((64, 128), F32)
        for t, v in enumerate(norm_finish(0, img)):
            Gh[img, x, 64 * t : 64 * t + 64, :] = v[:, 0:128].astype(BF16)
            rest = rest + (pltpu.roll(v[:, 128:256], 32 * t, 1) if t else v[:, 128:256])
        Gh[img, x, 256:320, :] = rest.astype(BF16)
        for k in (2, 1, 3):
            remote(
                Gh.at[img, x], Gh.at[img, x], sGh.at[img], rGh.at[img],
                dev(lax.rem(x + k, NX), y, z, c),
            ).start()
    for s in range(1, 4):
        ring_step(0, s)
    local_wait(W.at[0, 1 - c], rP.at[0])
    for k in range(NX):
        W1[:, :, 128 * k : 128 * k + 128, :] = W[0, :, :, BLK * k : BLK * k + 128, :]
        W1[:, :, 512 + 32 * k : 544 + 32 * k, :] = W[0, :, :, BLK * k + 128 : BLK * k + BLK, :]
    for img in range(2):
        slopes(1, img)
    lane = iota((64, 128), 1)
    for img in range(2):
        local_wait(Gh.at[img, 0:3], rGh.at[img])
        rests = [Gh[img, k, 256:320, :].astype(F32) for k in range(NX)]
        for k in range(NX):
            L[img, :, 128 * k : 128 * k + 128] = Gh[img, k, 0:256, :]
        for t in range(NX):
            v = jnp.zeros((64, 128), F32)
            for k in range(NX):
                w = pltpu.roll(rests[k], (32 * (k - t)) % 128, 1) if k != t else rests[k]
                v = jnp.where((lane >= 32 * k) & (lane < 32 * k + 32), w, v)
            L[img, 64 * t : 64 * t + 64, 512:640] = v.astype(BF16)
        conv(1, img, mul_grad)
        norm_sums(1, img)
    for img in range(2):
        for t, v in enumerate(norm_finish(1, img)):
            Os[img, t] = pack(CC[t, 64 * img : 64 * img + 64, :] + v).astype(BF16)
        for k in (2, 1, 3):
            t = lax.rem(x + k, NX)
            remote(
                Os.at[img, t], Oc.at[img, x], sO.at[img], rO.at[img], dev(t, y, z, c)
            ).start()
        Oc[img, x] = Os[img, x]

    for f in (1, 0):
        local_wait(RA.at[f, 0:7], sA.at[f])

        @pl.when(jnp.logical_not(mine[f]))
        def _():
            local_wait(RA.at[f, 0], sA0.at[f])

        local_wait(W.at[f, 0, :, 0:560, :], sR.at[f])
        local_wait(W.at[f, 0], sP.at[f])
    local_wait(G.at[0:3], sG)
    for img in range(2):
        local_wait(Gh.at[img, 0:3], sGh.at[img])
    local_wait(Hc.at[0:3], sH)

    @pl.when(y < NY - 1)
    def _():
        local_wait(Hc.at[3], sN.at[0])

    @pl.when(y > 0)
    def _():
        local_wait(Hc.at[0], sN.at[1])

    for p in range(5):
        local_wait(ST.at[p, 0:7], sS.at[p])
    for n, img in ((0, 0), (0, 1), (1, 0), (1, 1)):
        @pl.when(y > 0)
        def _():
            local_wait(HBs.at[n, img, 0], sB.at[n, img, 0])

        @pl.when(y < NY - 1)
        def _():
            local_wait(HBs.at[n, img, 1], sB.at[n, img, 1])

    for img in range(2):
        local_wait(Oc.at[img, 0:3], rO.at[img])
        out[64 * img : 64 * img + 64, :] = jnp.concatenate(
            [unpack(Oc[img, k].astype(F32))[:, 0:BLK] for k in range(NX)], axis=1
        ).astype(BF16)
    for img in range(2):
        local_wait(Oc.at[img, 0:3], sO.at[img])


def body(latent, hidden, cotangent, filter_one, filter_two, gain_one, shift_one, gain_two, shift_two):
    filters = [jnp.transpose(a, (0, 2, 1)) for a in (filter_one, filter_two)]
    rows = [a.reshape(PX, CH) for a in (cotangent, hidden, latent)]
    params = (gain_two, shift_two, gain_one, shift_one)
    vmem = pl.BlockSpec(memory_space=pltpu.VMEM)
    anywhere = pl.BlockSpec(memory_space=pl.ANY)
    dma = pltpu.SemaphoreType.DMA
    out = pl.pallas_call(
        kernel,
        out_shape=jax.ShapeDtypeStruct((PX, CH), BF16),
        in_specs=[anywhere] * 9,
        out_specs=vmem,
        scratch_shapes=[
            pltpu.VMEM((2, 9, 20, 40), BF16),
            [pltpu.VMEM((CH,), F32)] * 4,
            pltpu.VMEM((2, PX, CH), BF16),
            pltpu.VMEM((2, 24, 384), BF16),
            pltpu.VMEM((2, 2, 3, CH, 256), BF16),
            pltpu.VMEM((2, 3, CH, 256), BF16),
            pltpu.VMEM((2, 8, 24, 384), BF16),
            pltpu.VMEM((NX, PX, CH), BF16),
            pltpu.VMEM((2, NX, 320, 128), BF16),
            pltpu.VMEM((2, NX * 64, CH), BF16),
            pltpu.VMEM((NX, PX, 384), BF16),
            pltpu.VMEM((NX, PX, 384), BF16),
            pltpu.VMEM((2, NX, PX, 256), F32),
            pltpu.VMEM((5, 8, 128), F32),
            pltpu.VMEM((5, NY, 8, 128), F32),
            pltpu.VMEM((2, PX, 384), BF16),
            pltpu.VMEM((2, 2, PX, 256), F32),
            pltpu.VMEM((2, 6, 64, 256), F32),
            pltpu.VMEM((2, 6, 64, 256), F32),
            pltpu.VMEM((2, 2, 64, 256), F32),
            pltpu.VMEM((2, 2, 64, 256), F32),
            pltpu.VMEM((2, 2, 2, 80, 128), F32),
            pltpu.VMEM((2, 2, 2, 80, 128), F32),
            pltpu.VMEM((2, 384, 256), F32),
            pltpu.VMEM((2, NX * 64, 256), F32),
            pltpu.VMEM((2, NX, 80, 128), BF16),
            pltpu.VMEM((2, NX, 80, 128), BF16),
            pltpu.VMEM((NX, PX, 256), F32),
            dma((2,)), dma((4,)), dma((2,)), dma,
            dma((2,)), dma((2,)), dma((2,)),
            dma((2,)), dma((2, 2, 4, 3)),
            dma((2,)), dma((2,)),
            dma, dma, dma((2,)), dma((2,)), dma, dma,
            dma((5,)), dma((5,)),
            dma((2, 2, 2)), dma((2, 2, 2)),
            dma((2,)), dma((2,)),
            dma((2,)), dma((2,)),
        ],
        compiler_params=pltpu.CompilerParams(
            collective_id=0, has_side_effects=True, vmem_limit_bytes=62 * 1024 * 1024
        ),
        name="block_backward",
    )(*filters, *rows, *params)
    return out.reshape(latent.shape)


def solution(mesh):
    in_specs = (
        P("dp", "rows", None, None),
        P("dp", "rows", None, None),
        P("dp", "rows", None, None),
        P(None, "dp", "rows"),
        P(None, "dp", "rows"),
        P(),
        P(),
        P(),
        P(),
    )
    out_specs = P("dp", "rows", None, None)
    return jax.shard_map(body, mesh=mesh, in_specs=in_specs, out_specs=out_specs, check_vma=False)
```

```python
import jax
import jax.numpy as jnp
from jax import lax
from jax.experimental import pallas as pl
from jax.experimental.pallas import tpu as pltpu
from jax.sharding import PartitionSpec as P

MESH = pl.DeviceIdType.MESH
F32 = jnp.float32
BF16 = jnp.bfloat16
NX, NY, NZ = 4, 8, 8
CH = 640
BLK = 160
PX = 128
NUMBER = 32 * 64 * 40
FAR_FIRST = (4, 3, 5, 2, 6, 1, 7)


def dev(x, y, z, c):
    return (2 * z + c, 4 * y + x)


def iota(shape, dim):
    return lax.broadcasted_iota(jnp.int32, shape, dim)


def dot(a, b, **kw):
    return jnp.dot(a, b, preferred_element_type=F32, **kw)


def group_of(lane):
    g = jnp.zeros_like(lane)
    for edge in (40, 80, 120, 160):
        g = g + (lane >= edge).astype(jnp.int32)
    return g


def kernel(
    f1, f2, cot, hid, lat, g2, s2, g1, s1, out,
    FV, PV, HV, WB, W, W1, RA, G, Gh, L, Hs, Hc, Hx, SS, ST, Hb, HxB, NB, SB, PB, KB, HBs, HBr, AC, BK, Os, Oc, CC,
    lF, lP, lH, lC, sA, sA0, rA, sR, rR, sP, rP, sG, rG, sGh, rGh, sH, rH, sS, rS, sB, rB, sO, rO, sN, rN,
):
    dp = lax.axis_index("dp")
    rr = lax.axis_index("rows")
    c = lax.rem(dp, 2)
    z = lax.div(dp, 2)
    x = lax.rem(rr, NX)
    y = lax.div(rr, NX)
    X = lax.div(z, 2)
    mine_y = x == X
    mine_z = jnp.logical_and(x == X, y == z)

    def remote(src, dst, ss, rs, target):
        return pltpu.make_async_remote_copy(
            src_ref=src, dst_ref=dst, send_sem=ss, recv_sem=rs, device_id=target,
            device_id_type=MESH,
        )

    def local_wait(ref, sem):
        pltpu.make_async_copy(ref, ref, sem).wait()

    Hb[...] = jnp.zeros_like(Hb)
    bar = pltpu.get_barrier_semaphore()

    def here(target):
        pl.semaphore_signal(bar, inc=1, device_id=target, device_id_type=MESH)

    for b in range(2):
        zs = 2 * x + lax.rem(z + b, 2)
        for k in range(NX):
            xs = lax.rem(x + k, NX)
            if b == 0 and k == 0:
                @pl.when(jnp.logical_not(mine_y))
                def _():
                    here(dev(xs, y, zs, c))

                @pl.when(jnp.logical_not(mine_z))
                def _():
                    here(dev(xs, z, zs, c))
            else:
                here(dev(xs, y, zs, c))
                here(dev(xs, z, zs, c))
    for k in range(1, NX):
        here(dev(lax.rem(x + k, NX), y, z, c))
    for k in range(1, NY):
        here(dev(x, lax.rem(y + k, NY), z, c))
    for k in (1, 2, NZ - 2, NZ - 1):
        here(dev(x, y, lax.rem(z + k, NZ), c))
    here(dev(x, y, z, 1 - c))

    loads = [pltpu.make_async_copy(r, FV.at[f], lF.at[f]) for f, r in enumerate((f1, f2))]
    loads += [pltpu.make_async_copy(r, HV.at[a], lH.at[a]) for a, r in enumerate((hid, lat))]
    loads += [
        pltpu.make_async_copy(r, PV[a], lP.at[a]) for a, r in enumerate((g2, s2, g1, s1))
    ]
    own_cot = pltpu.make_async_copy(cot, G.at[x], lC)
    for load in loads[1::-1] + loads[2:]:
        load.start()
    own_cot.start()
    WB[...] = jnp.zeros_like(WB)

    def own_block(f):
        loads[f].wait()
        for a in range(3):
            taps = [FV[f, 3 * a + b].astype(F32) for b in range(3)]
            WB[f, 0:20, 128 * a : 128 * a + 128] = jnp.concatenate(
                taps + [jnp.zeros((20, 8), F32)], axis=1
            ).astype(BF16)

    own_block(1)

    pl.semaphore_wait(
        bar, 31 - mine_y.astype(jnp.int32) - mine_z.astype(jnp.int32)
    )

    slot = lax.rem(z, 2) * 4 + x
    along_y = {f: lax.rem(f + c, 2) == 1 for f in (1, 0)}
    mine = {f: jnp.where(along_y[f], mine_y.astype(jnp.int32), mine_z.astype(jnp.int32)) == 1 for f in (1, 0)}
    place = {f: jnp.where(along_y[f], y, z) for f in (1, 0)}

    def first_stage(f):
        for k in FAR_FIRST + (0,):
            y_ = jnp.where(along_y[f], y, lax.rem(y + k, NY))
            z_ = jnp.where(along_y[f], lax.rem(z + k, NZ), y)
            target = dev(X, y_, z_, c)
            if k == 0:
                @pl.when(mine[f])
                def _():
                    pltpu.make_async_copy(WB.at[f], RA.at[f, slot], rA.at[f]).start()

                @pl.when(jnp.logical_not(mine[f]))
                def _():
                    remote(WB.at[f], RA.at[f, slot], sA0.at[f], rA.at[f], target).start()
            else:
                remote(WB.at[f], RA.at[f, slot], sA.at[f], rA.at[f], target).start()

    first_stage(1)
    for a in range(2):
        loads[2 + a].wait()
    v = [HV[a].astype(F32) for a in range(2)]
    for k in range(NX):
        Hs[k] = jnp.concatenate(
            [v[a][:, BLK * k : BLK * k + BLK] for a in range(2)] + [jnp.zeros((PX, 64), F32)],
            axis=1,
        ).astype(BF16)
    own_cot.wait()
    for k in (2, 1, 3):
        t = lax.rem(x + k, NX)
        remote(Hs.at[t], Hc.at[x], sH, rH, dev(t, y, z, c)).start()
    Hc[x] = Hs[x]
    own_block(0)
    params = []
    for a in range(4):
        loads[4 + a].wait()
        whole = PV[a][...].reshape(1, CH)
        p = jnp.zeros((1, BLK), F32)
        for k in range(NX):
            p = jnp.where(x == k, whole[:, BLK * k : BLK * k + BLK], p)
        params.append(jnp.concatenate([p, jnp.zeros((1, 256 - BLK), F32)], axis=1))

    def region(f, cc, a, o):
        return W.at[f, cc, a, pl.ds(pl.multiple_of(80 * o, 16), 80), :]

    om = iota((80, 96), 0)
    mm_ = iota((80, 96), 1)
    hit = jnp.zeros((80, 96), jnp.bool_)
    for k in range(4):
        hit = jnp.logical_or(
            hit,
            jnp.logical_and(
                jnp.logical_and(mm_ >= 24 * k, mm_ < 24 * k + 20), om == mm_ - 4 * k
            ),
        )
    join = hit.astype(F32).astype(BF16)

    def at(f, p):
        return dev(x, jnp.where(along_y[f], p, y), jnp.where(along_y[f], z, p), c)

    def ring(f, way, step, a, hops):
        p = place[f]
        sign = 1 if way == 0 else -1
        o = lax.rem(p - sign * (step + 1 - hops) + 8, 8)
        return remote(
            region(f, c, a, o), region(f, c, a, o), sR.at[f], rR.at[f, way, step, a],
            at(f, lax.rem(p + sign * hops + 8, 8)),
        )

    def share(f, a, o):
        o = lax.rem(o + 8, 8)
        remote(
            region(f, c, a, o), region(f, c, a, o), sP.at[f], rP.at[f], dev(x, y, z, 1 - c)
        ).start()

    def start_ring(f):
        local_wait(RA.at[f], rA.at[f])
        for b in range(2):
            piece = dot(join, RA[f, 4 * b : 4 * b + 4].reshape(96, 384)).astype(BF16)
            for a in range(3):
                W[
                    f, c, a, pl.ds(pl.multiple_of(80 * place[f], 16), 80),
                    128 * b : 128 * b + 128,
                ] = piece[:, 128 * a : 128 * a + 128]
        for hops in (2, 1):
            for a in range(3):
                for way in range(2):
                    ring(f, way, hops - 1, a, hops).start()
        for a in range(3):
            share(f, a, place[f])

    def ring_step(f, s):
        step = (1, 0, 2, 3)[s]
        for a in range(3):
            for way in range(2):
                if step == 3 and way != a % 2:
                    continue
                ring(f, way, step, a, 0).wait_recv()
                if step == 1:
                    ring(f, way, 2, a, 1).start()
                    if way == a % 2:
                        ring(f, way, 3, a, 2).start()
                share(f, a, place[f] - (step + 1) * (1 if way == 0 else -1))

    start_ring(1)
    for k in (2, 1, 3):
        t = lax.rem(x + k, NX)
        remote(G.at[x], G.at[x], sG, rG, dev(t, y, z, c)).start()
    first_stage(0)
    for s in range(2):
        ring_step(1, s)

    row8 = iota((8, 256), 0)
    local_wait(Hc.at[0:3], rH)
    zero = jnp.zeros((64, 256 - BLK), F32)
    sums = jnp.zeros((8, 256), F32)
    for img in range(2):
        tot = [jnp.zeros((1, 256), F32)] * 2
        sq = [jnp.zeros((1, 256), F32)] * 2
        for t in range(NX):
            both = Hc[t, 64 * img : 64 * img + 64, :].astype(F32)
            for a in range(2):
                v = jnp.concatenate([both[:, BLK * a : BLK * a + BLK], zero], axis=1)
                Hx[a, t, 64 * img : 64 * img + 64, :] = v
                tot[a] = tot[a] + jnp.sum(v, axis=0, keepdims=True)
                sq[a] = sq[a] + jnp.sum(v * v, axis=0, keepdims=True)
        for a in range(2):
            sums = jnp.where(row8 == 4 * a + img, tot[a], sums)
            sums = jnp.where(row8 == 4 * a + 2 + img, sq[a], sums)

    gi = group_of(iota((256, 256), 0))
    gj = group_of(iota((256, 256), 1))
    same = jnp.logical_and(gi == gj, gi < 4).astype(F32).astype(BF16)

    def group_totals(v):
        high = v.astype(BF16)
        left = v - high.astype(F32)
        mid = left.astype(BF16)
        low = (left - mid.astype(F32)).astype(BF16)
        terms = jnp.concatenate([high.astype(F32), mid.astype(F32), low.astype(F32)], axis=0).astype(BF16)
        got = dot(terms, same[:, 0:128])
        return got[0:8] + got[8:16] + got[16:24]

    def send_sums(p, value):
        value = group_totals(value)
        SS[p] = value
        ST[p, y] = value
        for k in FAR_FIRST:
            remote(
                SS.at[p], ST.at[p, y], sS.at[p], rS.at[p], dev(x, lax.rem(y + k, NY), z, c)
            ).start()

    def take_sums(p):
        local_wait(ST.at[p, 0:7], rS.at[p])
        tot = ST[p, 0]
        for k in range(1, NY):
            tot = tot + ST[p, k]
        tot = tot * (1.0 / NUMBER)
        last = jnp.where(iota((8, 128), 1) < 32, tot[:, 127:128], 0.0)
        return jnp.concatenate([tot, last], axis=1)

    send_sums(0, sums)
    @pl.when(y < NY - 1)
    def _():
        remote(Hc.at[3], Hb.at[0], sN.at[0], rN.at[0], dev(x, lax.rem(y + 1, 8), z, c)).start()

    @pl.when(y > 0)
    def _():
        remote(Hc.at[0], Hb.at[1], sN.at[1], rN.at[1], dev(x, lax.rem(y + 7, 8), z, c)).start()

    ring_step(1, 2)
    @pl.when(c == 1)
    def _():
        start_ring(0)

    ring_step(1, 3)

    @pl.when(c == 0)
    def _():
        start_ring(0)


    ln128 = iota((16, 128), 1)

    def pack(v):
        fold = v[0:16, 128:256]
        for g in range(1, 4):
            fold = fold + pltpu.roll(v[16 * g : 16 * g + 16, 128:256], 32 * g, 1)
        return jnp.concatenate([v[:, 0:128], fold], axis=0)

    def unpack(m):
        fold = m[64:80]
        rest = [jnp.where(ln128 < 32, fold, 0.0)]
        for g in range(1, 4):
            rest.append(jnp.where(ln128 < 32, pltpu.roll(fold, 128 - 32 * g, 1), 0.0))
        return jnp.concatenate([m[0:64], jnp.concatenate(rest, axis=0)], axis=1)

    def combine(accs):
        rows = accs[0].shape[0]
        q = jnp.bitwise_and(iota((rows, 128), 0), 63)
        ln = iota((rows, 128), 1)
        t0 = jnp.zeros((rows, 128), F32)
        t1 = jnp.zeros((rows, 128), F32)
        for p in range(3):
            r = []
            for j in range(4):
                b = j // 2
                blk = accs[j % 2][:, 128 * b : 128 * b + 128]
                shift = (40 * j - 40 * p) % 128
                r.append(pltpu.roll(blk, shift, 1) if shift else blk)
            u0 = jnp.where(ln < 40, r[0], jnp.where(ln < 80, r[1], jnp.where(ln < 120, r[2], r[3])))
            u1 = jnp.where(ln < 32, r[3], 0.0)
            if p == 0:
                u0, u1 = (jnp.where(q == 63, 0.0, pltpu.roll(u, rows - 1, 0)) for u in (u0, u1))
            if p == 2:
                u0, u1 = (jnp.where(q == 0, 0.0, pltpu.roll(u, 1, 0)) for u in (u0, u1))
            t0 = t0 + u0
            t1 = t1 + u1
        return jnp.concatenate([t0, t1], axis=1)

    def conv(n, img, mul):
        for cc in range(2):
            AC[cc, 256:384] = jnp.zeros((128, 256), F32)
            AC[cc, 0:256] = mul(img, cc, 0)
            AC[cc, 64:320] += mul(img, cc, 1)
            AC[cc, 128:384] += mul(img, cc, 2)
        back = combine([AC[0], AC[1]])
        BK[img] = back[64:320]
        for e in range(2):
            PB[img, e] = back[320 * e : 320 * e + 64]
            HBs[n, img, e] = pack(back[320 * e : 320 * e + 64])

    def send_halo(n, img):
        @pl.when(y > 0)
        def _():
            remote(
                HBs.at[n, img, 0], HBr.at[n, img, 0], sB.at[n, img, 0], rB.at[n, img, 0],
                dev(x, lax.rem(y + 7, 8), z, c),
            ).start()

        @pl.when(y < NY - 1)
        def _():
            remote(
                HBs.at[n, img, 1], HBr.at[n, img, 1], sB.at[n, img, 1], rB.at[n, img, 1],
                dev(x, lax.rem(y + 1, 8), z, c),
            ).start()

    def take_halo(n, img, e):
        @pl.when(y < NY - 1 if e == 0 else y > 0)
        def _():
            local_wait(HBr.at[n, img, e], rB.at[n, img, e])
            px = slice(192, 256) if e == 0 else slice(0, 64)
            BK[img, px] += unpack(HBr[n, img, e]) * KB[img, 1 - e]

    def mul_cot(img, cc, ai):
        return dot(G[:, 64 * img : 64 * img + 64, :].reshape(NX * 64, CH), W[1, cc, ai])

    def mul_grad(img, cc, ai):
        return dot(L[img], W1[cc, ai])

    def slopes(a, img):
        avg, inv = (v[img : img + 1] for v in stats[a])
        gain, shift = params[2 * a], params[2 * a + 1]
        q = slice(64 * img, 64 * img + 64)
        for t in range(6):
            v = Hx[a, t, q, :] if t < 4 else HxB[a, t - 4, q, :]
            normed = (v - avg) * inv
            linear = normed * gain + shift
            s = jax.nn.sigmoid(linear)
            NB[img, t] = normed
            SB[img, t] = s * (1.0 + linear * (1.0 - s)) * gain

    def norm_sums(n, img):
        first = jnp.zeros((1, 256), F32)
        second = jnp.zeros((1, 256), F32)
        for t in range(6):
            slope = SB[img, t]
            if t < 4:
                px = slice(64 * t, 64 * t + 64)
                scaled = BK[img, px, :] * slope
                BK[img, px, :] = scaled
                if t in (0, 3):
                    KB[img, t // 3] = slope
            else:
                valid = y > 0 if t == 4 else y < NY - 1
                scaled = jnp.where(valid, PB[img, t - 4] * slope, 0.0)
            first = first + jnp.sum(scaled, axis=0, keepdims=True)
            second = second + jnp.sum(scaled * NB[img, t], axis=0, keepdims=True)
        value = jnp.where(row8 == 0, first, jnp.where(row8 == 1, second, 0.0))
        send_sums(2 * n + 1 + img, value)
        send_halo(n, img)

    def norm_finish(n, img):
        take_halo(n, img, 1)
        take_halo(n, img, 0)
        got = take_sums(2 * n + 1 + img)
        inv = stats[n][1][img : img + 1]
        first, second = got[0:1], got[1:2]
        return [
            inv * (BK[img, 64 * t : 64 * t + 64, :] - first - NB[img, t] * second) for t in range(NX)
        ]

    local_wait(G.at[0:3], rG)
    local_wait(W.at[1, 1 - c], rP.at[1])
    conv(0, 0, mul_cot)
    mean = take_sums(0)
    stats = []
    for a in range(2):
        avg = mean[4 * a : 4 * a + 2]
        inv = lax.rsqrt(mean[4 * a + 2 : 4 * a + 4] - avg * avg + 1e-05)
        stats.append((avg, inv))
    @pl.when(y > 0)
    def _():
        local_wait(Hb.at[0], rN.at[0])

    @pl.when(y < NY - 1)
    def _():
        local_wait(Hb.at[1], rN.at[1])

    for e in range(2):
        both = Hb[e].astype(F32)
        for a in range(2):
            HxB[a, e] = jnp.concatenate(
                [both[:, BLK * a : BLK * a + BLK], jnp.zeros((PX, 256 - BLK), F32)], axis=1
            )
    slopes(0, 0)
    norm_sums(0, 0)
    slopes(0, 1)
    conv(0, 1, mul_cot)
    norm_sums(0, 1)
    ring_step(0, 0)
    pick = (iota((CH, 256), 0) == iota((CH, 256), 1) + BLK * x) & (iota((CH, 256), 1) < BLK)
    pick = pick.astype(F32).astype(BF16)
    for t in range(NX):
        CC[t] = dot(G[t], pick)
    for img in range(2):
        rest = jnp.zeros((64, 128), F32)
        for t, v in enumerate(norm_finish(0, img)):
            Gh[img, x, 64 * t : 64 * t + 64, :] = v[:, 0:128].astype(BF16)
            rest = rest + (pltpu.roll(v[:, 128:256], 32 * t, 1) if t else v[:, 128:256])
        Gh[img, x, 256:320, :] = rest.astype(BF16)
        for k in (2, 1, 3):
            remote(
                Gh.at[img, x], Gh.at[img, x], sGh.at[img], rGh.at[img],
                dev(lax.rem(x + k, NX), y, z, c),
            ).start()
    for s in range(1, 4):
        ring_step(0, s)
    local_wait(W.at[0, 1 - c], rP.at[0])
    for k in range(NX):
        W1[:, :, 128 * k : 128 * k + 128, :] = W[0, :, :, BLK * k : BLK * k + 128, :]
        W1[:, :, 512 + 32 * k : 544 + 32 * k, :] = W[0, :, :, BLK * k + 128 : BLK * k + BLK, :]
    for img in range(2):
        slopes(1, img)
    lane = iota((64, 128), 1)
    for img in range(2):
        local_wait(Gh.at[img, 0:3], rGh.at[img])
        rests = [Gh[img, k, 256:320, :].astype(F32) for k in range(NX)]
        for k in range(NX):
            L[img, :, 128 * k : 128 * k + 128] = Gh[img, k, 0:256, :]
        for t in range(NX):
            v = jnp.zeros((64, 128), F32)
            for k in range(NX):
                w = pltpu.roll(rests[k], (32 * (k - t)) % 128, 1) if k != t else rests[k]
                v = jnp.where((lane >= 32 * k) & (lane < 32 * k + 32), w, v)
            L[img, 64 * t : 64 * t + 64, 512:640] = v.astype(BF16)
        conv(1, img, mul_grad)
        norm_sums(1, img)
    for img in range(2):
        for t, v in enumerate(norm_finish(1, img)):
            Os[img, t] = pack(CC[t, 64 * img : 64 * img + 64, :] + v).astype(BF16)
        for k in (2, 1, 3):
            t = lax.rem(x + k, NX)
            remote(
                Os.at[img, t], Oc.at[img, x], sO.at[img], rO.at[img], dev(t, y, z, c)
            ).start()
        Oc[img, x] = Os[img, x]

    for f in (1, 0):
        local_wait(RA.at[f, 0:7], sA.at[f])

        @pl.when(jnp.logical_not(mine[f]))
        def _():
            local_wait(RA.at[f, 0], sA0.at[f])

        local_wait(W.at[f, 0, :, 0:560, :], sR.at[f])
        local_wait(W.at[f, 0], sP.at[f])
    local_wait(G.at[0:3], sG)
    for img in range(2):
        local_wait(Gh.at[img, 0:3], sGh.at[img])
    local_wait(Hc.at[0:3], sH)

    @pl.when(y < NY - 1)
    def _():
        local_wait(Hc.at[3], sN.at[0])

    @pl.when(y > 0)
    def _():
        local_wait(Hc.at[0], sN.at[1])

    for p in range(5):
        local_wait(ST.at[p, 0:7], sS.at[p])
    for n, img in ((0, 0), (0, 1), (1, 0), (1, 1)):
        @pl.when(y > 0)
        def _():
            local_wait(HBs.at[n, img, 0], sB.at[n, img, 0])

        @pl.when(y < NY - 1)
        def _():
            local_wait(HBs.at[n, img, 1], sB.at[n, img, 1])

    for img in range(2):
        local_wait(Oc.at[img, 0:3], rO.at[img])
        out[64 * img : 64 * img + 64, :] = jnp.concatenate(
            [unpack(Oc[img, k].astype(F32))[:, 0:BLK] for k in range(NX)], axis=1
        ).astype(BF16)
    for img in range(2):
        local_wait(Oc.at[img, 0:3], sO.at[img])


def body(latent, hidden, cotangent, filter_one, filter_two, gain_one, shift_one, gain_two, shift_two):
    filters = [jnp.transpose(a, (0, 2, 1)) for a in (filter_one, filter_two)]
    rows = [a.reshape(PX, CH) for a in (cotangent, hidden, latent)]
    params = (gain_two, shift_two, gain_one, shift_one)
    vmem = pl.BlockSpec(memory_space=pltpu.VMEM)
    anywhere = pl.BlockSpec(memory_space=pl.ANY)
    dma = pltpu.SemaphoreType.DMA
    out = pl.pallas_call(
        kernel,
        out_shape=jax.ShapeDtypeStruct((PX, CH), BF16),
        in_specs=[anywhere] * 9,
        out_specs=vmem,
        scratch_shapes=[
            pltpu.VMEM((2, 9, 20, 40), BF16),
            [pltpu.VMEM((CH,), F32)] * 4,
            pltpu.VMEM((2, PX, CH), BF16),
            pltpu.VMEM((2, 24, 384), BF16),
            pltpu.VMEM((2, 2, 3, CH, 256), BF16),
            pltpu.VMEM((2, 3, CH, 256), BF16),
            pltpu.VMEM((2, 8, 24, 384), BF16),
            pltpu.VMEM((NX, PX, CH), BF16),
            pltpu.VMEM((2, NX, 320, 128), BF16),
            pltpu.VMEM((2, NX * 64, CH), BF16),
            pltpu.VMEM((NX, PX, 384), BF16),
            pltpu.VMEM((NX, PX, 384), BF16),
            pltpu.VMEM((2, NX, PX, 256), F32),
            pltpu.VMEM((5, 8, 128), F32),
            pltpu.VMEM((5, NY, 8, 128), F32),
            pltpu.VMEM((2, PX, 384), BF16),
            pltpu.VMEM((2, 2, PX, 256), F32),
            pltpu.VMEM((2, 6, 64, 256), F32),
            pltpu.VMEM((2, 6, 64, 256), F32),
            pltpu.VMEM((2, 2, 64, 256), F32),
            pltpu.VMEM((2, 2, 64, 256), F32),
            pltpu.VMEM((2, 2, 2, 80, 128), F32),
            pltpu.VMEM((2, 2, 2, 80, 128), F32),
            pltpu.VMEM((2, 384, 256), F32),
            pltpu.VMEM((2, NX * 64, 256), F32),
            pltpu.VMEM((2, NX, 80, 128), BF16),
            pltpu.VMEM((2, NX, 80, 128), BF16),
            pltpu.VMEM((NX, PX, 256), F32),
            dma((2,)), dma((4,)), dma((2,)), dma,
            dma((2,)), dma((2,)), dma((2,)),
            dma((2,)), dma((2, 2, 4, 3)),
            dma((2,)), dma((2,)),
            dma, dma, dma((2,)), dma((2,)), dma, dma,
            dma((5,)), dma((5,)),
            dma((2, 2, 2)), dma((2, 2, 2)),
            dma((2,)), dma((2,)),
            dma((2,)), dma((2,)),
        ],
        compiler_params=pltpu.CompilerParams(
            collective_id=0, has_side_effects=True, vmem_limit_bytes=62 * 1024 * 1024
        ),
        name="block_backward",
    )(*filters, *rows, *params)
    return out.reshape(latent.shape)


def solution(mesh):
    in_specs = (
        P("dp", "rows", None, None),
        P("dp", "rows", None, None),
        P("dp", "rows", None, None),
        P(None, "dp", "rows"),
        P(None, "dp", "rows"),
        P(),
        P(),
        P(),
        P(),
    )
    out_specs = P("dp", "rows", None, None)
    return jax.shard_map(body, mesh=mesh, in_specs=in_specs, out_specs=out_specs, check_vma=False)
```

```python
import jax
import jax.numpy as jnp
from jax import lax
from jax.experimental import pallas as pl
from jax.experimental.pallas import tpu as pltpu
from jax.sharding import PartitionSpec as P

MESH = pl.DeviceIdType.MESH
F32 = jnp.float32
BF16 = jnp.bfloat16
NX, NY, NZ = 4, 8, 8
CH = 640
BLK = 160
PX = 128
NUMBER = 32 * 64 * 40
FAR_FIRST = (4, 3, 5, 2, 6, 1, 7)


def dev(x, y, z, c):
    return (2 * z + c, 4 * y + x)


def iota(shape, dim):
    return lax.broadcasted_iota(jnp.int32, shape, dim)


def dot(a, b, **kw):
    return jnp.dot(a, b, preferred_element_type=F32, **kw)


def group_of(lane):
    g = jnp.zeros_like(lane)
    for edge in (40, 80, 120, 160):
        g = g + (lane >= edge).astype(jnp.int32)
    return g


def kernel(
    f1, f2, cot, hid, lat, g2, s2, g1, s1, out,
    FV, PV, HV, WB, W, W1, RA, G, Gh, L, Hs, Hc, Hx, SS, ST, Hb, HxB, NB, SB, PB, KB, HBs, HBr, AC, BK, Os, Oc, CC,
    lF, lP, lH, lC, sA, sA0, rA, sR, rR, sP, rP, sG, rG, sGh, rGh, sH, rH, sS, rS, sB, rB, sO, rO, sN, rN, OV, sV,
):
    dp = lax.axis_index("dp")
    rr = lax.axis_index("rows")
    c = lax.rem(dp, 2)
    z = lax.div(dp, 2)
    x = lax.rem(rr, NX)
    y = lax.div(rr, NX)
    X = lax.div(z, 2)
    mine_y = x == X
    mine_z = jnp.logical_and(x == X, y == z)

    def remote(src, dst, ss, rs, target):
        return pltpu.make_async_remote_copy(
            src_ref=src, dst_ref=dst, send_sem=ss, recv_sem=rs, device_id=target,
            device_id_type=MESH,
        )

    def local_wait(ref, sem):
        pltpu.make_async_copy(ref, ref, sem).wait()

    Hb[...] = jnp.zeros_like(Hb)
    bar = pltpu.get_barrier_semaphore()

    def here(target):
        pl.semaphore_signal(bar, inc=1, device_id=target, device_id_type=MESH)

    for b in range(2):
        zs = 2 * x + lax.rem(z + b, 2)
        for k in range(NX):
            xs = lax.rem(x + k, NX)
            if b == 0 and k == 0:
                @pl.when(jnp.logical_not(mine_y))
                def _():
                    here(dev(xs, y, zs, c))

                @pl.when(jnp.logical_not(mine_z))
                def _():
                    here(dev(xs, z, zs, c))
            else:
                here(dev(xs, y, zs, c))
                here(dev(xs, z, zs, c))
    for k in range(1, NX):
        here(dev(lax.rem(x + k, NX), y, z, c))
    for k in range(1, NY):
        here(dev(x, lax.rem(y + k, NY), z, c))
    for k in (1, 2, NZ - 2, NZ - 1):
        here(dev(x, y, lax.rem(z + k, NZ), c))
    here(dev(x, y, z, 1 - c))

    loads = [pltpu.make_async_copy(r, FV.at[f], lF.at[f]) for f, r in enumerate((f1, f2))]
    loads += [pltpu.make_async_copy(r, HV.at[a], lH.at[a]) for a, r in enumerate((hid, lat))]
    loads += [
        pltpu.make_async_copy(r, PV[a], lP.at[a]) for a, r in enumerate((g2, s2, g1, s1))
    ]
    own_cot = pltpu.make_async_copy(cot, G.at[x], lC)
    for load in loads[1::-1] + loads[2:]:
        load.start()
    own_cot.start()
    WB[...] = jnp.zeros_like(WB)

    def own_block(f):
        loads[f].wait()
        for a in range(3):
            taps = [FV[f, 3 * a + b].astype(F32) for b in range(3)]
            WB[f, 0:20, 128 * a : 128 * a + 128] = jnp.concatenate(
                taps + [jnp.zeros((20, 8), F32)], axis=1
            ).astype(BF16)

    own_block(1)

    pl.semaphore_wait(
        bar, 31 - mine_y.astype(jnp.int32) - mine_z.astype(jnp.int32)
    )

    slot = lax.rem(z, 2) * 4 + x
    along_y = {f: lax.rem(f + c, 2) == 1 for f in (1, 0)}
    mine = {f: jnp.where(along_y[f], mine_y.astype(jnp.int32), mine_z.astype(jnp.int32)) == 1 for f in (1, 0)}
    place = {f: jnp.where(along_y[f], y, z) for f in (1, 0)}

    def first_stage(f):
        for k in FAR_FIRST + (0,):
            y_ = jnp.where(along_y[f], y, lax.rem(y + k, NY))
            z_ = jnp.where(along_y[f], lax.rem(z + k, NZ), y)
            target = dev(X, y_, z_, c)
            if k == 0:
                @pl.when(mine[f])
                def _():
                    pltpu.make_async_copy(WB.at[f], RA.at[f, slot], rA.at[f]).start()

                @pl.when(jnp.logical_not(mine[f]))
                def _():
                    remote(WB.at[f], RA.at[f, slot], sA0.at[f], rA.at[f], target).start()
            else:
                remote(WB.at[f], RA.at[f, slot], sA.at[f], rA.at[f], target).start()

    first_stage(1)
    for a in range(2):
        loads[2 + a].wait()
    v = [HV[a].astype(F32) for a in range(2)]
    for k in range(NX):
        Hs[k] = jnp.concatenate(
            [v[a][:, BLK * k : BLK * k + BLK] for a in range(2)] + [jnp.zeros((PX, 64), F32)],
            axis=1,
        ).astype(BF16)
    own_cot.wait()
    for k in range(1, NX):
        t = lax.rem(x + k, NX)
        remote(Hs.at[t], Hc.at[x], sH, rH, dev(t, y, z, c)).start()
    for k in range(1, NX):
        t = lax.rem(x + k, NX)
        remote(G.at[x], G.at[x], sG, rG, dev(t, y, z, c)).start()
    Hc[x] = Hs[x]
    own_block(0)
    params = []
    for a in range(4):
        loads[4 + a].wait()
        whole = PV[a][...].reshape(1, CH)
        p = jnp.zeros((1, BLK), F32)
        for k in range(NX):
            p = jnp.where(x == k, whole[:, BLK * k : BLK * k + BLK], p)
        params.append(jnp.concatenate([p, jnp.zeros((1, 256 - BLK), F32)], axis=1))

    def region(f, cc, a, o):
        return W.at[f, cc, a, pl.ds(pl.multiple_of(80 * o, 16), 80), :]

    om = iota((80, 96), 0)
    mm_ = iota((80, 96), 1)
    hit = jnp.zeros((80, 96), jnp.bool_)
    for k in range(4):
        hit = jnp.logical_or(
            hit,
            jnp.logical_and(
                jnp.logical_and(mm_ >= 24 * k, mm_ < 24 * k + 20), om == mm_ - 4 * k
            ),
        )
    join = hit.astype(F32).astype(BF16)

    def at(f, p):
        return dev(x, jnp.where(along_y[f], p, y), jnp.where(along_y[f], z, p), c)

    def ring(f, way, step, a, hops):
        p = place[f]
        sign = 1 if way == 0 else -1
        o = lax.rem(p - sign * (step + 1 - hops) + 8, 8)
        return remote(
            region(f, c, a, o), region(f, c, a, o), sR.at[f], rR.at[f, way, step, a],
            at(f, lax.rem(p + sign * hops + 8, 8)),
        )

    def share(f, a, o):
        o = lax.rem(o + 8, 8)
        remote(
            region(f, c, a, o), region(f, c, a, o), sP.at[f], rP.at[f], dev(x, y, z, 1 - c)
        ).start()

    def start_ring(f):
        local_wait(RA.at[f], rA.at[f])
        for b in range(2):
            piece = dot(join, RA[f, 4 * b : 4 * b + 4].reshape(96, 384)).astype(BF16)
            for a in range(3):
                W[
                    f, c, a, pl.ds(pl.multiple_of(80 * place[f], 16), 80),
                    128 * b : 128 * b + 128,
                ] = piece[:, 128 * a : 128 * a + 128]
        for hops in (2, 1):
            for a in range(3):
                for way in range(2):
                    ring(f, way, hops - 1, a, hops).start()
        for a in range(3):
            share(f, a, place[f])

    def ring_step(f, s):
        step = (1, 0, 2, 3)[s]
        for a in range(3):
            for way in range(2):
                if step == 3 and way != a % 2:
                    continue
                ring(f, way, step, a, 0).wait_recv()
                if step == 1:
                    ring(f, way, 2, a, 1).start()
                    if way == a % 2:
                        ring(f, way, 3, a, 2).start()
                share(f, a, place[f] - (step + 1) * (1 if way == 0 else -1))

    start_ring(1)
    first_stage(0)
    for s in range(2):
        ring_step(1, s)

    row8 = iota((8, 256), 0)
    local_wait(Hc.at[0:3], rH)
    zero = jnp.zeros((64, 256 - BLK), F32)
    sums = jnp.zeros((8, 256), F32)
    for img in range(2):
        tot = [jnp.zeros((1, 256), F32)] * 2
        sq = [jnp.zeros((1, 256), F32)] * 2
        for t in range(NX):
            both = Hc[t, 64 * img : 64 * img + 64, :].astype(F32)
            for a in range(2):
                v = jnp.concatenate([both[:, BLK * a : BLK * a + BLK], zero], axis=1)
                Hx[a, t, 64 * img : 64 * img + 64, :] = v
                tot[a] = tot[a] + jnp.sum(v, axis=0, keepdims=True)
                sq[a] = sq[a] + jnp.sum(v * v, axis=0, keepdims=True)
        for a in range(2):
            sums = jnp.where(row8 == 4 * a + img, tot[a], sums)
            sums = jnp.where(row8 == 4 * a + 2 + img, sq[a], sums)

    gi = group_of(iota((256, 256), 0))
    gj = group_of(iota((256, 256), 1))
    same = jnp.logical_and(gi == gj, gi < 4).astype(F32).astype(BF16)

    def group_totals(v):
        high = v.astype(BF16)
        left = v - high.astype(F32)
        mid = left.astype(BF16)
        low = (left - mid.astype(F32)).astype(BF16)
        terms = jnp.concatenate([high.astype(F32), mid.astype(F32), low.astype(F32)], axis=0).astype(BF16)
        got = dot(terms, same[:, 0:128])
        return got[0:8] + got[8:16] + got[16:24]

    def send_sums(p, value):
        value = group_totals(value)
        SS[p] = value
        ST[p, y] = value
        for k in FAR_FIRST:
            remote(
                SS.at[p], ST.at[p, y], sS.at[p], rS.at[p], dev(x, lax.rem(y + k, NY), z, c)
            ).start()

    def take_sums(p):
        local_wait(ST.at[p, 0:7], rS.at[p])
        tot = ST[p, 0]
        for k in range(1, NY):
            tot = tot + ST[p, k]
        tot = tot * (1.0 / NUMBER)
        last = jnp.where(iota((8, 128), 1) < 32, tot[:, 127:128], 0.0)
        return jnp.concatenate([tot, last], axis=1)

    send_sums(0, sums)
    @pl.when(y < NY - 1)
    def _():
        remote(Hc.at[3], Hb.at[0], sN.at[0], rN.at[0], dev(x, lax.rem(y + 1, 8), z, c)).start()

    @pl.when(y > 0)
    def _():
        remote(Hc.at[0], Hb.at[1], sN.at[1], rN.at[1], dev(x, lax.rem(y + 7, 8), z, c)).start()

    ring_step(1, 2)
    @pl.when(c == 1)
    def _():
        start_ring(0)

    ring_step(1, 3)

    @pl.when(c == 0)
    def _():
        start_ring(0)


    ln128 = iota((16, 128), 1)

    def pack(v):
        fold = v[0:16, 128:256]
        for g in range(1, 4):
            fold = fold + pltpu.roll(v[16 * g : 16 * g + 16, 128:256], 32 * g, 1)
        return jnp.concatenate([v[:, 0:128], fold], axis=0)

    def unpack(m):
        fold = m[64:80]
        rest = [jnp.where(ln128 < 32, fold, 0.0)]
        for g in range(1, 4):
            rest.append(jnp.where(ln128 < 32, pltpu.roll(fold, 128 - 32 * g, 1), 0.0))
        return jnp.concatenate([m[0:64], jnp.concatenate(rest, axis=0)], axis=1)

    def combine(accs):
        rows = accs[0].shape[0]
        q = jnp.bitwise_and(iota((rows, 128), 0), 63)
        ln = iota((rows, 128), 1)
        t0 = jnp.zeros((rows, 128), F32)
        t1 = jnp.zeros((rows, 128), F32)
        for p in range(3):
            r = []
            for j in range(4):
                b = j // 2
                blk = accs[j % 2][:, 128 * b : 128 * b + 128]
                shift = (40 * j - 40 * p) % 128
                r.append(pltpu.roll(blk, shift, 1) if shift else blk)
            u0 = jnp.where(ln < 40, r[0], jnp.where(ln < 80, r[1], jnp.where(ln < 120, r[2], r[3])))
            u1 = jnp.where(ln < 32, r[3], 0.0)
            if p == 0:
                u0, u1 = (jnp.where(q == 63, 0.0, pltpu.roll(u, rows - 1, 0)) for u in (u0, u1))
            if p == 2:
                u0, u1 = (jnp.where(q == 0, 0.0, pltpu.roll(u, 1, 0)) for u in (u0, u1))
            t0 = t0 + u0
            t1 = t1 + u1
        return jnp.concatenate([t0, t1], axis=1)

    def conv(n, img, mul):
        for cc in range(2):
            AC[cc, 256:384] = jnp.zeros((128, 256), F32)
            AC[cc, 0:256] = mul(img, cc, 0)
            AC[cc, 64:320] += mul(img, cc, 1)
            AC[cc, 128:384] += mul(img, cc, 2)
        back = combine([AC[0], AC[1]])
        BK[img] = back[64:320]
        for e in range(2):
            PB[img, e] = back[320 * e : 320 * e + 64]
            HBs[n, img, e] = pack(back[320 * e : 320 * e + 64])

    def send_halo(n, img):
        @pl.when(y > 0)
        def _():
            remote(
                HBs.at[n, img, 0], HBr.at[n, img, 0], sB.at[n, img, 0], rB.at[n, img, 0],
                dev(x, lax.rem(y + 7, 8), z, c),
            ).start()

        @pl.when(y < NY - 1)
        def _():
            remote(
                HBs.at[n, img, 1], HBr.at[n, img, 1], sB.at[n, img, 1], rB.at[n, img, 1],
                dev(x, lax.rem(y + 1, 8), z, c),
            ).start()

    def take_halo(n, img, e):
        @pl.when(y < NY - 1 if e == 0 else y > 0)
        def _():
            local_wait(HBr.at[n, img, e], rB.at[n, img, e])
            px = slice(192, 256) if e == 0 else slice(0, 64)
            BK[img, px] += unpack(HBr[n, img, e]) * KB[img, 1 - e]

    def mul_cot(img, cc, ai):
        return dot(G[:, 64 * img : 64 * img + 64, :].reshape(NX * 64, CH), W[1, cc, ai])

    def mul_grad(img, cc, ai):
        return dot(L[img], W1[cc, ai])

    def slopes(a, img):
        avg, inv = (v[img : img + 1] for v in stats[a])
        gain, shift = params[2 * a], params[2 * a + 1]
        q = slice(64 * img, 64 * img + 64)
        for t in range(6):
            v = Hx[a, t, q, :] if t < 4 else HxB[a, t - 4, q, :]
            normed = (v - avg) * inv
            linear = normed * gain + shift
            s = jax.nn.sigmoid(linear)
            NB[img, t] = normed
            SB[img, t] = s * (1.0 + linear * (1.0 - s)) * gain

    def norm_sums(n, img):
        first = jnp.zeros((1, 256), F32)
        second = jnp.zeros((1, 256), F32)
        for t in range(6):
            slope = SB[img, t]
            if t < 4:
                px = slice(64 * t, 64 * t + 64)
                scaled = BK[img, px, :] * slope
                BK[img, px, :] = scaled
                if t in (0, 3):
                    KB[img, t // 3] = slope
            else:
                valid = y > 0 if t == 4 else y < NY - 1
                scaled = jnp.where(valid, PB[img, t - 4] * slope, 0.0)
            first = first + jnp.sum(scaled, axis=0, keepdims=True)
            second = second + jnp.sum(scaled * NB[img, t], axis=0, keepdims=True)
        value = jnp.where(row8 == 0, first, jnp.where(row8 == 1, second, 0.0))
        send_sums(2 * n + 1 + img, value)
        send_halo(n, img)

    def norm_finish(n, img):
        take_halo(n, img, 1)
        take_halo(n, img, 0)
        got = take_sums(2 * n + 1 + img)
        inv = stats[n][1][img : img + 1]
        first, second = got[0:1], got[1:2]
        return [
            inv * (BK[img, 64 * t : 64 * t + 64, :] - first - NB[img, t] * second) for t in range(NX)
        ]

    local_wait(G.at[0:3], rG)
    local_wait(W.at[1, 1 - c], rP.at[1])
    conv(0, 0, mul_cot)
    mean = take_sums(0)
    stats = []
    for a in range(2):
        avg = mean[4 * a : 4 * a + 2]
        inv = lax.rsqrt(mean[4 * a + 2 : 4 * a + 4] - avg * avg + 1e-05)
        stats.append((avg, inv))
    @pl.when(y > 0)
    def _():
        local_wait(Hb.at[0], rN.at[0])

    @pl.when(y < NY - 1)
    def _():
        local_wait(Hb.at[1], rN.at[1])

    for e in range(2):
        both = Hb[e].astype(F32)
        for a in range(2):
            HxB[a, e] = jnp.concatenate(
                [both[:, BLK * a : BLK * a + BLK], jnp.zeros((PX, 256 - BLK), F32)], axis=1
            )
    slopes(0, 0)
    norm_sums(0, 0)
    slopes(0, 1)
    conv(0, 1, mul_cot)
    norm_sums(0, 1)
    ring_step(0, 0)
    pick = (iota((CH, 256), 0) == iota((CH, 256), 1) + BLK * x) & (iota((CH, 256), 1) < BLK)
    pick = pick.astype(F32).astype(BF16)
    for t in range(NX):
        CC[t] = dot(G[t], pick)
    for img in range(2):
        rest = jnp.zeros((64, 128), F32)
        for t, v in enumerate(norm_finish(0, img)):
            Gh[img, x, 64 * t : 64 * t + 64, :] = v[:, 0:128].astype(BF16)
            rest = rest + (pltpu.roll(v[:, 128:256], 32 * t, 1) if t else v[:, 128:256])
        Gh[img, x, 256:320, :] = rest.astype(BF16)
        for k in (2, 1, 3):
            remote(
                Gh.at[img, x], Gh.at[img, x], sGh.at[img], rGh.at[img],
                dev(lax.rem(x + k, NX), y, z, c),
            ).start()
    for s in range(1, 4):
        ring_step(0, s)
    local_wait(W.at[0, 1 - c], rP.at[0])
    for k in range(NX):
        W1[:, :, 128 * k : 128 * k + 128, :] = W[0, :, :, BLK * k : BLK * k + 128, :]
        W1[:, :, 512 + 32 * k : 544 + 32 * k, :] = W[0, :, :, BLK * k + 128 : BLK * k + BLK, :]
    for img in range(2):
        slopes(1, img)
    lane = iota((64, 128), 1)
    for img in range(2):
        local_wait(Gh.at[img, 0:3], rGh.at[img])
        rests = [Gh[img, k, 256:320, :].astype(F32) for k in range(NX)]
        for k in range(NX):
            L[img, :, 128 * k : 128 * k + 128] = Gh[img, k, 0:256, :]
        for t in range(NX):
            v = jnp.zeros((64, 128), F32)
            for k in range(NX):
                w = pltpu.roll(rests[k], (32 * (k - t)) % 128, 1) if k != t else rests[k]
                v = jnp.where((lane >= 32 * k) & (lane < 32 * k + 32), w, v)
            L[img, 64 * t : 64 * t + 64, 512:640] = v.astype(BF16)
        conv(1, img, mul_grad)
        norm_sums(1, img)
    for img in range(2):
        for t, v in enumerate(norm_finish(1, img)):
            Os[img, t] = pack(CC[t, 64 * img : 64 * img + 64, :] + v).astype(BF16)
        for k in (2, 1, 3):
            t = lax.rem(x + k, NX)
            remote(
                Os.at[img, t], Oc.at[img, x], sO.at[img], rO.at[img], dev(t, y, z, c)
            ).start()
        Oc[img, x] = Os[img, x]

    for f in (1, 0):
        local_wait(RA.at[f, 0:7], sA.at[f])

        @pl.when(jnp.logical_not(mine[f]))
        def _():
            local_wait(RA.at[f, 0], sA0.at[f])

        local_wait(W.at[f, 0, :, 0:560, :], sR.at[f])
        local_wait(W.at[f, 0], sP.at[f])
    local_wait(G.at[0:3], sG)
    for img in range(2):
        local_wait(Gh.at[img, 0:3], sGh.at[img])
    local_wait(Hc.at[0:3], sH)

    @pl.when(y < NY - 1)
    def _():
        local_wait(Hc.at[3], sN.at[0])

    @pl.when(y > 0)
    def _():
        local_wait(Hc.at[0], sN.at[1])

    for p in range(5):
        local_wait(ST.at[p, 0:7], sS.at[p])
    for n, img in ((0, 0), (0, 1), (1, 0), (1, 1)):
        @pl.when(y > 0)
        def _():
            local_wait(HBs.at[n, img, 0], sB.at[n, img, 0])

        @pl.when(y < NY - 1)
        def _():
            local_wait(HBs.at[n, img, 1], sB.at[n, img, 1])

    for img in range(2):
        local_wait(Oc.at[img, 0:3], rO.at[img])
        OV[64 * img : 64 * img + 64, :] = jnp.concatenate(
            [unpack(Oc[img, k].astype(F32))[:, 0:BLK] for k in range(NX)], axis=1
        ).astype(BF16)
        pltpu.make_async_copy(OV.at[pl.ds(64 * img, 64), :], out.at[pl.ds(64 * img, 64), :], sV.at[img]).start()
    for img in range(2):
        local_wait(Oc.at[img, 0:3], sO.at[img])
        local_wait(OV.at[pl.ds(64 * img, 64), :], sV.at[img])


def body(latent, hidden, cotangent, filter_one, filter_two, gain_one, shift_one, gain_two, shift_two):
    filters = [jnp.transpose(a, (0, 2, 1)) for a in (filter_one, filter_two)]
    rows = [a.reshape(PX, CH) for a in (cotangent, hidden, latent)]
    params = (gain_two, shift_two, gain_one, shift_one)
    vmem = pl.BlockSpec(memory_space=pltpu.VMEM)
    anywhere = pl.BlockSpec(memory_space=pl.ANY)
    dma = pltpu.SemaphoreType.DMA
    out = pl.pallas_call(
        kernel,
        out_shape=jax.ShapeDtypeStruct((PX, CH), BF16),
        in_specs=[anywhere] * 9,
        out_specs=pl.BlockSpec(memory_space=pltpu.HBM),
        scratch_shapes=[
            pltpu.VMEM((2, 9, 20, 40), BF16),
            [pltpu.VMEM((CH,), F32)] * 4,
            pltpu.VMEM((2, PX, CH), BF16),
            pltpu.VMEM((2, 24, 384), BF16),
            pltpu.VMEM((2, 2, 3, CH, 256), BF16),
            pltpu.VMEM((2, 3, CH, 256), BF16),
            pltpu.VMEM((2, 8, 24, 384), BF16),
            pltpu.VMEM((NX, PX, CH), BF16),
            pltpu.VMEM((2, NX, 320, 128), BF16),
            pltpu.VMEM((2, NX * 64, CH), BF16),
            pltpu.VMEM((NX, PX, 384), BF16),
            pltpu.VMEM((NX, PX, 384), BF16),
            pltpu.VMEM((2, NX, PX, 256), F32),
            pltpu.VMEM((5, 8, 128), F32),
            pltpu.VMEM((5, NY, 8, 128), F32),
            pltpu.VMEM((2, PX, 384), BF16),
            pltpu.VMEM((2, 2, PX, 256), F32),
            pltpu.VMEM((2, 6, 64, 256), F32),
            pltpu.VMEM((2, 6, 64, 256), F32),
            pltpu.VMEM((2, 2, 64, 256), F32),
            pltpu.VMEM((2, 2, 64, 256), F32),
            pltpu.VMEM((2, 2, 2, 80, 128), F32),
            pltpu.VMEM((2, 2, 2, 80, 128), F32),
            pltpu.VMEM((2, 384, 256), F32),
            pltpu.VMEM((2, NX * 64, 256), F32),
            pltpu.VMEM((2, NX, 80, 128), BF16),
            pltpu.VMEM((2, NX, 80, 128), BF16),
            pltpu.VMEM((NX, PX, 256), F32),
            dma((2,)), dma((4,)), dma((2,)), dma,
            dma((2,)), dma((2,)), dma((2,)),
            dma((2,)), dma((2, 2, 4, 3)),
            dma((2,)), dma((2,)),
            dma, dma, dma((2,)), dma((2,)), dma, dma,
            dma((5,)), dma((5,)),
            dma((2, 2, 2)), dma((2, 2, 2)),
            dma((2,)), dma((2,)),
            dma((2,)), dma((2,)),
            pltpu.VMEM((PX, CH), BF16), dma((2,)),
        ],
        compiler_params=pltpu.CompilerParams(
            collective_id=0, has_side_effects=True, vmem_limit_bytes=62 * 1024 * 1024
        ),
        name="block_backward",
    )(*filters, *rows, *params)
    return out.reshape(latent.shape)


def solution(mesh):
    in_specs = (
        P("dp", "rows", None, None),
        P("dp", "rows", None, None),
        P("dp", "rows", None, None),
        P(None, "dp", "rows"),
        P(None, "dp", "rows"),
        P(),
        P(),
        P(),
        P(),
    )
    out_specs = P("dp", "rows", None, None)
    return jax.shard_map(body, mesh=mesh, in_specs=in_specs, out_specs=out_specs, check_vma=False)
```
